256 devices in a mesh: gx: 16 (over y, x), gy: 16 (over z, core).
Axes of the slice: x: 4, y: 4, z: 8, core: 2. Of those that a mesh axis runs over, the one named last changes fastest.
Arguments:
- right_side: float32 [9, 512, 2048], P(None, 'gx', 'gy'), may hold values from -16 to 16
- diag_blocks: float32 [9, 9, 512, 2048], P(None, None, 'gx', 'gy'), may hold values from -0.3 to 6, as said below
- couple_blocks: float32 [9, 9, 512, 2048], P(None, None, 'gx', 'gy'), may hold values from -0.15 to 1.5, as said below
- transmissibility: float32 [4, 512, 2048], P(None, 'gx', 'gy'), may hold values from 0.1 to 0.8
- pressure_weights: float32 [9, 512, 2048], P(None, 'gx', 'gy'), may hold values from 0.2 to 1
- well_mask: int32 [512, 2048], P('gx', 'gy'), may hold values 0 or 1
Outputs:
- solution: float32 [9, 512, 2048], P(None, 'gx', 'gy')
- estimate: float32 [], replicated
The draws below stay inside these ranges and needn't reach their ends.
Inputs may be any that keep to these rules, and one draw needn't show every extreme that they name: `diag_blocks`: outside the first column, each block has diagonal entries from 4 to 6 and other entries within 0.3 in magnitude (within 0.05 in the first row); the first column is positive. `couple_blocks`: each block has first-column entries from 0.5 to 1.5, other diagonal entries from 0.6 to 1.2, and other entries within 0.15 in magnitude.
All inputs are finite; a program needn't handle non-finite values. No bound on the sum of `well_mask` on one device may be relied on, other than what follows from the above.
Results may differ from the reference program's by a relative error of at most 0.0003.
Values sent between devices are 32-bit elements; how exact they have to be, the bound alone decides.
No kernel may reach another device: no remote copies, remote signals or barrier semaphores. Data moves between devices by JAX's collectives and lax.ppermute only.
A program may use at most 64 MiB of HBM per device.

```python
import math
import jax
import jax.numpy as jnp
from jax import lax

NC = 9
GSTEPS = 2
LEVELS = 3
COARSE_SWEEPS = 6
NX = 512
NY = 2048


def block_pattern(key, diag_low, diag_high, column_low, column_high, spread, column_first):
    array_shape = (NC, NC, NX, NY)
    key_off, key_column, key_diag = jax.random.split(key, 3)
    off_values = jax.random.uniform(key_off, array_shape, jnp.float32, -spread, spread)
    column_values = jax.random.uniform(key_column, array_shape, jnp.float32, column_low, column_high)
    diag_values = jax.random.uniform(key_diag, array_shape, jnp.float32, diag_low, diag_high)
    rows_iota = lax.broadcasted_iota(jnp.int32, array_shape, 0)
    cols_iota = lax.broadcasted_iota(jnp.int32, array_shape, 1)
    if column_first:
        return jnp.where(cols_iota == 0, column_values, jnp.where(rows_iota == cols_iota, diag_values, off_values))
    return jnp.where(rows_iota == cols_iota, diag_values, jnp.where(cols_iota == 0, column_values, off_values))


def flux_parts(key):
    trans_key = jax.random.fold_in(key, 101)
    log_values = jax.random.uniform(trans_key, (4, NX, NY), jnp.float32, math.log(0.1), math.log(0.8))
    face_trans = jnp.exp(log_values)
    couple = block_pattern(jax.random.fold_in(key, 23), 0.6, 1.2, 0.5, 1.5, 0.15, True)
    return (face_trans, couple)


def draw_transmissibility(key, part):
    return flux_parts(key)[0]


def draw_couple_blocks(key, part):
    return flux_parts(key)[1]


def draw_diag_blocks(key, part):
    face_trans, couple = flux_parts(key)
    array_shape = (NC, NC, NX, NY)
    key_off, key_diag, key_accum = jax.random.split(jax.random.fold_in(key, 11), 3)
    rows_iota = lax.broadcasted_iota(jnp.int32, array_shape, 0)
    cols_iota = lax.broadcasted_iota(jnp.int32, array_shape, 1)
    off_values = jax.random.uniform(key_off, array_shape, jnp.float32, -0.3, 0.3)
    off_values = jnp.where(rows_iota == 0, off_values / 6.0, off_values)
    diag_values = jax.random.uniform(key_diag, array_shape, jnp.float32, 4.0, 6.0)
    padded = jnp.pad(couple[:, 0], ((0, 0), (1, 1), (1, 1)))
    inflow = face_trans[0] * padded[:, 2:, 1:-1] + face_trans[1] * padded[:, :-2, 1:-1] + face_trans[2] * padded[:, 1:-1, 2:] + face_trans[3] * padded[:, 1:-1, :-2]
    accumulation = jax.random.uniform(key_accum, (NC, NX, NY), jnp.float32, 0.05, 0.15)
    first_column = (accumulation + inflow)[:, None]
    return jnp.where(cols_iota == 0, first_column, jnp.where(rows_iota == cols_iota, diag_values, off_values))


def draw_right_side(key, part):
    array_shape = (NC, NX, NY)
    key_rough = jax.random.fold_in(jax.random.fold_in(key, 37), 0)
    return jnp.clip(4.0 * jax.random.normal(key_rough, array_shape, jnp.float32), -16.0, 16.0)


def touch_ends(drawn, key, least, high):
    shape = drawn.shape
    spot = [jax.random.randint(jax.random.fold_in(key, axis), (), 0, shape[axis]) for axis in range(len(shape))]
    drawn = drawn.at[tuple(spot)].set(least)
    longest = shape.index(max(shape))
    spot[longest] = (spot[longest] + 1) % shape[longest]
    return drawn.at[tuple(spot)].set(high)


def block_scale(own_key, shape, pieces, smallest, top_value):
    factor_of = 1.0
    for position, parts in pieces:
        heights = jax.random.uniform(jax.random.fold_in(jax.random.fold_in(own_key, 6), position), (parts,), jnp.float32, smallest / len(pieces), top_value / len(pieces))
        factor_of = factor_of * jnp.repeat(jnp.exp(heights), shape[position] // parts).reshape((-1,) + (1,) * (len(shape) - 1 - position))
    return factor_of


def setup_inputs(seed: int = 0) -> dict:
    arg_keys = jax.random.split(jax.random.key(seed), 7)
    right_side = draw_right_side(jax.random.fold_in(arg_keys[6], 71), 0)
    diag_blocks = draw_diag_blocks(jax.random.fold_in(arg_keys[6], 71), 0)
    couple_blocks = draw_couple_blocks(jax.random.fold_in(arg_keys[6], 71), 0)
    transmissibility = draw_transmissibility(jax.random.fold_in(arg_keys[6], 71), 0)
    pressure_weights = jnp.clip(0.2 + 0.8 * jax.random.uniform(arg_keys[4], (NC, NX, NY), jnp.float32) ** block_scale(arg_keys[4], (NC, NX, NY), ((1, 16), (2, 16)), -0.2, 0.2), 0.2, 1.0)
    well_mask = touch_ends((jax.random.randint(arg_keys[5], (NX, NY), 0, 16) < 1).astype(jnp.int32), jax.random.fold_in(arg_keys[5], 1), 0, 1)
    return dict(right_side=right_side, diag_blocks=diag_blocks, couple_blocks=couple_blocks, transmissibility=transmissibility, pressure_weights=pressure_weights, well_mask=well_mask)


relax_factor = 0.8
well_boost = 8.0

def pad_cells(values):
    widths = [(0, 0)] * (values.ndim - 2) + [(1, 1), (1, 1)]
    return jnp.pad(values, widths)

def four_sides(padded):
    return (padded[..., 2:, 1:-1], padded[..., :-2, 1:-1], padded[..., 1:-1, 2:], padded[..., 1:-1, :-2])

def apply_blocks(vector, eff_diag, couple_blocks, face_trans, padder):
    product = lax.optimization_barrier(jnp.sum(couple_blocks * vector[None], axis=1))
    east_side, west_side, north_side, south_side = four_sides(padder(product))
    own_term = lax.optimization_barrier(jnp.sum(eff_diag * vector[None], axis=1))
    return own_term - (face_trans[0] * east_side + face_trans[1] * west_side + face_trans[2] * north_side + face_trans[3] * south_side)

def level_apply(values, coeffs, padder):
    east_side, west_side, north_side, south_side = four_sides(padder(values))
    return coeffs[0] * values + (coeffs[1] * east_side + coeffs[2] * west_side + coeffs[3] * north_side + coeffs[4] * south_side)

def jacobi_sweep(iterate, source, coeffs, padder):
    return iterate + relax_factor * (source - level_apply(iterate, coeffs, padder)) / coeffs[0]

def coarse_sweeps(source, coeffs, padder):
    iterate = relax_factor * source / coeffs[0]
    for sweep_no in range(COARSE_SWEEPS - 1):
        iterate = jacobi_sweep(iterate, source, coeffs, padder)
    return iterate

def coarsen(coeffs):
    extent_x, extent_y = (coeffs.shape[1], coeffs.shape[2])
    grouped = coeffs.reshape(5, extent_x // 2, 2, extent_y // 2, 2)
    center_fine, east_fine, west_fine, north_fine, south_fine = (grouped[0], grouped[1], grouped[2], grouped[3], grouped[4])
    center = center_fine.sum(axis=(1, 3)) + east_fine[:, 0].sum(axis=2) + west_fine[:, 1].sum(axis=2) + north_fine[:, :, :, 0].sum(axis=1) + south_fine[:, :, :, 1].sum(axis=1)
    east_link = east_fine[:, 1].sum(axis=2)
    west_link = west_fine[:, 0].sum(axis=2)
    north_link = north_fine[:, :, :, 1].sum(axis=1)
    south_link = south_fine[:, :, :, 0].sum(axis=1)
    return jnp.stack([center, east_link, west_link, north_link, south_link])

def restrict(values):
    extent_x, extent_y = values.shape
    return values.reshape(extent_x // 2, 2, extent_y // 2, 2).sum(axis=(1, 3))

def prolong(values):
    return jnp.repeat(jnp.repeat(values, 2, axis=0), 2, axis=1)

def vcycle(source, hierarchy, padder, coarse_solve):
    if len(hierarchy) == 1:
        return coarse_solve(source, hierarchy[0])
    coeffs = hierarchy[0]
    iterate = relax_factor * source / coeffs[0]
    residue = source - level_apply(iterate, coeffs, padder)
    correction = vcycle(restrict(residue), hierarchy[1:], padder, coarse_solve)
    iterate = iterate + prolong(correction)
    return jacobi_sweep(iterate, source, coeffs, padder)

def block_inverse(matrix):
    extent = matrix.shape[0]
    identity = jnp.eye(extent, dtype=matrix.dtype)[:, :, None, None] * jnp.ones_like(matrix[0, 0])
    left_part, right_part = (matrix, identity)
    for pivot_row in range(extent):
        pivot_value = left_part[pivot_row, pivot_row]
        scaled_left = left_part[pivot_row] / pivot_value
        scaled_right = right_part[pivot_row] / pivot_value
        factor = left_part[:, pivot_row]
        left_part = left_part - factor[:, None] * scaled_left[None]
        right_part = right_part - factor[:, None] * scaled_right[None]
        left_part = left_part.at[pivot_row].set(scaled_left)
        right_part = right_part.at[pivot_row].set(scaled_right)
    return right_part

def pressure_coeffs(eff_diag, weights, face_trans, ghosts):

    def weighed(side_values):
        return lax.optimization_barrier(jnp.sum(weights * side_values, axis=0))
    center = lax.optimization_barrier(jnp.sum(weights * eff_diag[:, 0], axis=0))
    return jnp.stack([center, -face_trans[0] * weighed(ghosts[0]), -face_trans[1] * weighed(ghosts[1]), -face_trans[2] * weighed(ghosts[2]), -face_trans[3] * weighed(ghosts[3])])

def least_squares(start_norm, columns):
    steps_count = len(columns)
    rhs_list = [start_norm] + [jnp.zeros_like(start_norm)] * steps_count
    cosine_values, sine_values, upper_columns = ([], [], [])
    for column_no in range(steps_count):
        column = list(columns[column_no])
        for earlier in range(column_no):
            first_entry = column[earlier]
            second_entry = column[earlier + 1]
            column[earlier] = cosine_values[earlier] * first_entry + sine_values[earlier] * second_entry
            column[earlier + 1] = -sine_values[earlier] * first_entry + cosine_values[earlier] * second_entry
        radius = jnp.sqrt(column[column_no] * column[column_no] + column[column_no + 1] * column[column_no + 1])
        cosine_value = column[column_no] / radius
        sine_value = column[column_no + 1] / radius
        column[column_no] = radius
        rhs_list[column_no + 1] = -sine_value * rhs_list[column_no]
        rhs_list[column_no] = cosine_value * rhs_list[column_no]
        cosine_values.append(cosine_value)
        sine_values.append(sine_value)
        upper_columns.append(column)
    coefficients = [None] * steps_count
    for row_no in reversed(range(steps_count)):
        running = rhs_list[row_no]
        for later_no in range(row_no + 1, steps_count):
            running = running - upper_columns[later_no][row_no] * coefficients[later_no]
        coefficients[row_no] = running / upper_columns[row_no][row_no]
    return (coefficients, jnp.abs(rhs_list[steps_count]))

def reference(right_side, diag_blocks, couple_blocks, transmissibility, pressure_weights, well_mask):
    identity = jnp.eye(NC, dtype=diag_blocks.dtype)[:, :, None, None]
    eff_diag = diag_blocks + well_boost * well_mask.astype(diag_blocks.dtype)[None, None] * identity
    inverse = block_inverse(eff_diag)
    ghosts = four_sides(pad_cells(couple_blocks[:, 0]))
    hierarchy = [pressure_coeffs(eff_diag, pressure_weights, transmissibility, ghosts)]
    for level_no in range(LEVELS - 1):
        hierarchy.append(coarsen(hierarchy[-1]))

    def coarse_solve(source, coeffs):
        return coarse_sweeps(source, coeffs, pad_cells)

    def apply_full(vector):
        return apply_blocks(vector, eff_diag, couple_blocks, transmissibility, pad_cells)

    def precondition(vector):
        pressure_rhs = lax.optimization_barrier(jnp.sum(pressure_weights * vector, axis=0))
        pressure = vcycle(pressure_rhs, hierarchy, pad_cells, coarse_solve)
        lifted = jnp.concatenate([pressure[None], jnp.zeros((NC - 1,) + pressure.shape, pressure.dtype)])
        second = vector - apply_full(lifted)
        return lifted + lax.optimization_barrier(jnp.sum(inverse * second[None], axis=1))
    start_norm = jnp.sqrt(jnp.sum(right_side * right_side))
    krylov_basis = [right_side / start_norm]
    directions, columns = ([], [])
    for step_no in range(GSTEPS):
        direction = precondition(krylov_basis[step_no])
        directions.append(direction)
        mapped = apply_full(direction)
        projections = [jnp.sum(mapped * member) for member in krylov_basis]
        remainder = mapped
        for projection, member in zip(projections, krylov_basis):
            remainder = remainder - projection * member
        length = jnp.sqrt(jnp.sum(remainder * remainder))
        krylov_basis.append(remainder / length)
        columns.append(projections + [length])
    coefficients, estimate = least_squares(start_norm, columns)
    solution = coefficients[0] * directions[0]
    for step_no in range(1, GSTEPS):
        solution = solution + coefficients[step_no] * directions[step_no]
    return (solution, estimate)
```

```python
import functools

import jax
import jax.numpy as jnp
from jax import lax
from jax.experimental import pallas as pl
from jax.experimental.pallas import tpu as pltpu
from jax.sharding import PartitionSpec as P

NC = 9
COARSE_SWEEPS = 6
RELAX = 0.8
WELL_BOOST = 8.0

R, L = 32, 128
HALO = 32
EX, EY = 3 * R, 2 * L

AX_EDGE = 6 * R
AX_COL = AX_EDGE + 24
AX_ROWS = AX_COL + R
AY_ROWS = 2 * EX
BX_EDGE = R
BX_COL = BX_EDGE + 16
BX_ROWS = BX_COL + R

CENTER, EAST, WEST, NORTH, SOUTH, SCALE = range(6)


def iotas(shape):
    return (lax.broadcasted_iota(jnp.int32, shape, 0), lax.broadcasted_iota(jnp.int32, shape, 1))


def shifted(values, axis, step):
    return pltpu.roll(values, (-step) % values.shape[axis], axis)


def lane_roll(values, shift):
    shift = shift % values.shape[1]
    return values if shift == 0 else pltpu.roll(values, shift, 1)


def even_mask(par_ref, which, shape):
    return jnp.full(shape, par_ref[which], jnp.int32) == 0


def put(par_ref, which, first, second, rows, up, down):
    even = even_mask(par_ref, which, up.shape)
    first[rows, :] = jnp.where(even, up, down)
    second[rows, :] = jnp.where(even, down, up)


def take(par_ref, which, first, second, rows):
    one, two = (first[rows, :], second[rows, :])
    even = even_mask(par_ref, which, one.shape)
    return (jnp.where(even, one, two), jnp.where(even, two, one))


def pack_columns(parts):
    shape = parts[0][0].shape
    lanes = iotas(shape)[1]
    packed = jnp.zeros(shape, jnp.float32)
    for values, lane, target in parts:
        packed = jnp.where(lanes == target, lane_roll(values, target - lane), packed)
    return packed


def setup_kernel(par, rhs, diag0, couple0, trans, weights, wells, msg1, msg2, own, cols):
    rows, lanes = iotas((R, L))
    center = WELL_BOOST * wells[...].astype(jnp.float32) * weights[0]
    pressure = jnp.zeros((R, L), jnp.float32)
    links = [jnp.zeros((R, L), jnp.float32) for _ in range(4)]
    for c in range(NC):
        w, col = (weights[c], couple0[c, 0])
        center = center + w * diag0[c, 0]
        pressure = pressure + w * rhs[c]
        for d, (axis, step) in enumerate(((0, 1), (0, -1), (1, 1), (1, -1))):
            links[d] = links[d] + w * shifted(col, axis, step)
    inside = (rows != R - 1, rows != 0, lanes != L - 1, lanes != 0)
    fields = [center]
    for d in range(4):
        fields.append(jnp.where(inside[d], -trans[d] * links[d], 0.0))
    fields.append(pressure)
    for k, field in enumerate(fields):
        span = pl.ds(k * R, R)
        own[span, :] = field
        msg1[span, :] = field
        msg2[span, :] = field
    t_up, t_down = (trans[0, R - 1 : R, :], trans[1, 0:1, :])
    t_right, t_left = (trans[2], trans[3])
    for c in range(NC):
        put(par, 0, msg1, msg2, pl.ds(AX_EDGE + c, 1), couple0[c, 0, R - 1 : R, :], couple0[c, 0, 0:1, :])
        put(par, 0, msg1, msg2, pl.ds(AX_EDGE + NC + c, 1), t_up * weights[c, R - 1 : R, :], t_down * weights[c, 0:1, :])
    blank = jnp.zeros((24 - 2 * NC, L), jnp.float32)
    msg1[pl.ds(AX_EDGE + 2 * NC, 24 - 2 * NC), :] = blank
    msg2[pl.ds(AX_EDGE + 2 * NC, 24 - 2 * NC), :] = blank
    parts = []
    for c in range(NC):
        col, w = (couple0[c, 0], weights[c])
        parts += [(col, 0, c), (t_left * w, 0, NC + c), (col, L - 1, 2 * NC + c), (t_right * w, L - 1, 3 * NC + c)]
    packed = pack_columns(parts)
    cols[...] = packed
    msg1[pl.ds(AX_COL, R), :] = packed
    msg2[pl.ds(AX_COL, R), :] = packed


def inverse_kernel(diag, wells, out):
    boost = WELL_BOOST * wells[...].astype(jnp.float32)
    a = [[diag[i, j] + boost if i == j else diag[i, j] for j in range(NC)] for i in range(NC)]
    for k in range(NC):
        inv = 1.0 / a[k][k]
        a[k] = [inv if j == k else a[k][j] * inv for j in range(NC)]
        for i in range(NC):
            if i != k:
                factor = a[i][k]
                a[i] = [-factor * inv if j == k else a[i][j] - factor * a[k][j] for j in range(NC)]
    for i in range(NC):
        for j in range(NC):
            out[i, j] = a[i][j]


def setup_middle_kernel(par, got1, got2, own, cols, couple0, trans, weights, msg1, msg2, ext, ext_cols, edges):
    rows, lanes = iotas((EX, L))

    def dots(span_of):
        total = jnp.zeros((1, L), jnp.float32)
        for c in range(NC):
            total = total + span_of(c)
        return -total

    ups, downs, tw_ups, tw_downs = ([], [], [], [])
    for c in range(NC):
        up, down = take(par, 0, got1, got2, pl.ds(AX_EDGE + c, 1))
        ups.append(up)
        downs.append(down)
        up, down = take(par, 0, got1, got2, pl.ds(AX_EDGE + NC + c, 1))
        tw_ups.append(up)
        tw_downs.append(down)
        edges[pl.ds(c, 1), :] = ups[c]
        edges[pl.ds(NC + c, 1), :] = downs[c]
        edges[pl.ds(2 * NC + c, 1), :] = tw_ups[c]
        edges[pl.ds(3 * NC + c, 1), :] = tw_downs[c]
    t_up, t_down = (trans[0, R - 1 : R, :], trans[1, 0:1, :])
    east_own = dots(lambda c: t_up * weights[c, R - 1 : R, :] * ups[c])
    west_own = dots(lambda c: t_down * weights[c, 0:1, :] * downs[c])
    west_up = dots(lambda c: tw_ups[c] * couple0[c, 0, R - 1 : R, :])
    east_down = dots(lambda c: tw_downs[c] * couple0[c, 0, 0:1, :])
    fields = []
    for k in range(6):
        up, down = take(par, 0, got1, got2, pl.ds(k * R, R))
        field = jnp.concatenate([own[pl.ds(k * R, R), :], up, down], axis=0)
        if k == CENTER:
            field = jnp.where(field == 0.0, 1.0, field)
        if k == EAST:
            field = jnp.where(rows == R - 1, east_own, jnp.where(rows == EX - 1, east_down, field))
        if k == WEST:
            field = jnp.where(rows == 0, west_own, jnp.where(rows == R, west_up, field))
        ext[k] = field
        fields.append(field)
    up, down = take(par, 0, got1, got2, pl.ds(AX_COL, R))
    packed = jnp.concatenate([cols[...], up, down], axis=0)
    ext_cols[...] = packed
    to_right = [lane_roll(f, HALO * (k % 4) + HALO) for k, f in enumerate(fields)]
    to_left = [lane_roll(f, HALO * (k % 4)) for k, f in enumerate(fields)]
    group = lanes // HALO

    def quad(parts):
        result = parts[-1]
        for g in range(len(parts) - 2, -1, -1):
            result = jnp.where(group == g, parts[g], result)
        return result

    put(par, 1, msg1, msg2, pl.ds(0, EX), quad(to_right[:4]), quad(to_left[:4]))
    put(
        par,
        1,
        msg1,
        msg2,
        pl.ds(EX, EX),
        quad(to_right[4:] + [lane_roll(packed, 64 - 2 * NC)]),
        quad(to_left[4:] + [lane_roll(packed, 64)]),
    )


def lane_sum(product, start):
    lanes = iotas(product.shape)[1]
    keep = jnp.logical_and(lanes >= start, lanes < start + NC)
    return jnp.sum(jnp.where(keep, product, 0.0), axis=1, keepdims=True)


def pair_sums(values, step):
    rows, lanes = iotas(values.shape)
    values = values + jnp.where((rows // step) % 2 == 0, shifted(values, 0, step), shifted(values, 0, -step))
    return values + jnp.where((lanes // step) % 2 == 0, shifted(values, 1, step), shifted(values, 1, -step))


def coarsen_into(coeffs, level):
    step = 2**level
    base, out = (6 * level, 6 * level + 6)
    rows, lanes = iotas((EX, EY))
    row_even = (rows // step) % 2 == 0
    lane_even = (lanes // step) % 2 == 0
    east, west, north, south = (coeffs[base + d] for d in (EAST, WEST, NORTH, SOUTH))
    center = coeffs[base] + (jnp.where(row_even, east, west) + jnp.where(lane_even, north, south))
    center = pair_sums(center, step)
    coeffs[out + CENTER] = center
    coeffs[out + SCALE] = RELAX / center
    coeffs[out + EAST] = pair_sums(jnp.where(row_even, 0.0, east), step)
    coeffs[out + WEST] = pair_sums(jnp.where(row_even, west, 0.0), step)
    coeffs[out + NORTH] = pair_sums(jnp.where(lane_even, 0.0, north), step)
    coeffs[out + SOUTH] = pair_sums(jnp.where(lane_even, south, 0.0), step)


def level_apply(values, coeffs, level):
    step = 2**level
    base = 6 * level
    return coeffs[base + CENTER] * values + (
        coeffs[base + EAST] * shifted(values, 0, step)
        + coeffs[base + WEST] * shifted(values, 0, -step)
        + coeffs[base + NORTH] * shifted(values, 1, step)
        + coeffs[base + SOUTH] * shifted(values, 1, -step)
    )


def sweep(values, source, coeffs, level):
    return values + coeffs[6 * level + SCALE] * (source - level_apply(values, coeffs, level))


def vcycle(source, coeffs):
    values0 = coeffs[SCALE] * source
    source1 = pair_sums(source - level_apply(values0, coeffs, 0), 1)
    values1 = coeffs[6 + SCALE] * source1
    source2 = pair_sums(source1 - level_apply(values1, coeffs, 1), 2)
    values2 = coeffs[12 + SCALE] * source2
    for _ in range(COARSE_SWEEPS - 1):
        values2 = sweep(values2, source2, coeffs, 2)
    values1 = sweep(values1 + values2, source1, coeffs, 1)
    return sweep(values0 + values1, source, coeffs, 0)


def ghost_column(packed, start, to_lane, lane):
    return lane_roll(packed, to_lane - (start + lane))


def neighbour_sum(values, trans, up_row, down_row, right_col, left_col):
    rows, lanes = iotas((R, L))
    east = jnp.where(rows == R - 1, up_row, shifted(values, 0, 1))
    west = jnp.where(rows == 0, down_row, shifted(values, 0, -1))
    north = jnp.where(lanes == L - 1, right_col, shifted(values, 1, 1))
    south = jnp.where(lanes == 0, left_col, shifted(values, 1, -1))
    return trans[0] * east + trans[1] * west + trans[2] * north + trans[3] * south


def ghost_sum(trans, up_row, down_row, right_col, left_col):
    rows, lanes = iotas((R, L))
    return (
        jnp.where(rows == R - 1, trans[0] * up_row, 0.0)
        + jnp.where(rows == 0, trans[1] * down_row, 0.0)
        + jnp.where(lanes == L - 1, trans[2] * right_col, 0.0)
        + jnp.where(lanes == 0, trans[3] * left_col, 0.0)
    )


def one_step(pressure, vector, edges, col_right, col_left, diag, inverse, couple, trans, boost, z_out, product_out):
    p = pressure[0:R, 0:L]
    up_row, down_row = (pressure[R : R + 1, 0:L], pressure[EX - 1 : EX, 0:L])
    far = pressure[0:R, L:EY]
    right_p, left_p = (lane_roll(far, L - 1), lane_roll(far, 1))
    second = []
    for c in range(NC):
        own = diag[c, 0] * p
        if c == 0:
            own = own + boost * p
        around = neighbour_sum(
            couple[c, 0] * p,
            trans,
            edges[pl.ds(c, 1), :] * up_row,
            edges[pl.ds(NC + c, 1), :] * down_row,
            ghost_column(col_right, 64, L - 1, c) * right_p,
            ghost_column(col_left, 64, 0, c) * left_p,
        )
        second.append(vector[c] - (own - around))
    z = []
    for c in range(NC):
        total = inverse[c, 0] * second[0]
        for k in range(1, NC):
            total = total + inverse[c, k] * second[k]
        if c == 0:
            total = total + p
        z_out[c] = total
        z.append(total)
    result = []
    for c in range(NC):
        product = couple[c, 0] * z[0]
        own = diag[c, 0] * z[0]
        for k in range(1, NC):
            product = product + couple[c, k] * z[k]
            own = own + diag[c, k] * z[k]
        product_out[c] = product
        own = own + boost * z[c]
        zero = jnp.zeros((1, L), jnp.float32)
        around = neighbour_sum(product, trans, zero, zero, 0.0, 0.0)
        result.append(own - around - vector[c])
    return result


def load_blocks(sources, targets, sems):
    copies = [pltpu.make_async_copy(s, t, sems.at[i]) for i, (s, t) in enumerate(zip(sources, targets))]
    for copy in copies:
        copy.start()
    return copies


def first_step_kernel(
    par, got1, got2, ext, ext_cols, edges, rhs, trans, weights, wells, diag_hbm, inverse_hbm, couple_hbm,
    msg1, msg2, z_out, partial, product, coeffs, cols_right, cols_left, pressure_part, product_cols,
    diag, inverse, couple, sems,
):
    copies = load_blocks((diag_hbm, inverse_hbm, couple_hbm), (diag, inverse, couple), sems)
    rows, lanes = iotas((EX, L))
    right, left = take(par, 1, got1, got2, pl.ds(EX, EX))
    cols_right[...] = right
    cols_left[...] = left
    packed = ext_cols[...]
    north_own = -lane_sum(lane_roll(packed, 64 - 3 * NC) * right, 64)
    south_right = -lane_sum(lane_roll(packed, 64 - NC) * right, 64 + NC)
    south_own = -lane_sum(lane_roll(packed, 64 - NC) * left, 64)
    north_left = -lane_sum(lane_roll(packed, 64 + NC) * left, 64 + NC)
    right_four, left_four = take(par, 1, got1, got2, pl.ds(0, EX))
    source = None
    for k in range(6):
        from_right = lane_roll(right_four if k < 4 else right, -HALO * (k % 4))
        from_left = lane_roll(left_four if k < 4 else left, L - HALO - HALO * (k % 4))
        near = ext[k]
        far = jnp.where(lanes < HALO, from_right, jnp.where(lanes >= L - HALO, from_left, 0.0))
        if k == CENTER:
            far = jnp.where(far == 0.0, 1.0, far)
        if k == NORTH:
            near = jnp.where(lanes == L - 1, north_own, near)
            far = jnp.where(lanes == L - 1, north_left, far)
        if k == SOUTH:
            near = jnp.where(lanes == 0, south_own, near)
            far = jnp.where(lanes == 0, south_right, far)
        field = jnp.concatenate([near, far], axis=1)
        if k == 5:
            source = field
        else:
            coeffs[k] = field
    coeffs[SCALE] = RELAX / coeffs[CENTER]
    coarsen_into(coeffs, 0)
    coarsen_into(coeffs, 1)
    pressure = vcycle(source, coeffs)
    for copy in copies:
        copy.wait()
    boost = WELL_BOOST * wells[...].astype(jnp.float32)
    vector = [rhs[c] for c in range(NC)]
    result = one_step(
        pressure, vector, edges, right[0:R], left[0:R], diag, inverse, couple, trans, boost, z_out, product
    )
    weighed = jnp.zeros((R, L), jnp.float32)
    parts = []
    for c in range(NC):
        partial[c] = result[c]
        weighed = weighed + weights[c] * result[c]
        put(par, 0, msg1, msg2, pl.ds(BX_EDGE + c, 1), product[c, R - 1 : R, :], product[c, 0:1, :])
        parts += [(product[c], 0, c), (product[c], L - 1, NC + c)]
    blank = jnp.zeros((16 - NC, L), jnp.float32)
    columns = pack_columns(parts)
    pressure_part[...] = weighed
    product_cols[...] = columns
    for msg in (msg1, msg2):
        msg[pl.ds(0, R), :] = weighed
        msg[pl.ds(BX_EDGE + NC, 16 - NC), :] = blank
        msg[pl.ds(BX_COL, R), :] = columns


def between_kernel(par, got1, got2, pressure_part, product_cols, product, edges, trans, weights, msg1, msg2, ext, ext_cols, rows_out):
    rows, lanes = iotas((EX, L))
    t_up, t_down = (trans[0, R - 1 : R, :], trans[1, 0:1, :])
    own_up, own_down, far_up, far_down = (jnp.zeros((1, L), jnp.float32) for _ in range(4))
    for c in range(NC):
        up, down = take(par, 0, got1, got2, pl.ds(BX_EDGE + c, 1))
        rows_out[pl.ds(c, 1), :] = up
        rows_out[pl.ds(NC + c, 1), :] = down
        own_up = own_up + t_up * weights[c, R - 1 : R, :] * up
        own_down = own_down + t_down * weights[c, 0:1, :] * down
        far_up = far_up + edges[pl.ds(2 * NC + c, 1), :] * product[c, R - 1 : R, :]
        far_down = far_down + edges[pl.ds(3 * NC + c, 1), :] * product[c, 0:1, :]
    up, down = take(par, 0, got1, got2, pl.ds(0, R))
    field = jnp.concatenate([pressure_part[...], up, down], axis=0)
    edge = jnp.where(rows == R - 1, own_up, 0.0) + jnp.where(rows == 0, own_down, 0.0)
    edge = edge + jnp.where(rows == R, far_up, 0.0) + jnp.where(rows == EX - 1, far_down, 0.0)
    field = field - edge
    ext[...] = field
    up, down = take(par, 0, got1, got2, pl.ds(BX_COL, R))
    packed = jnp.concatenate([product_cols[...], up, down], axis=0)
    ext_cols[...] = packed
    near = lanes < HALO
    put(
        par, 1, msg1, msg2, pl.ds(0, EX),
        jnp.where(near, lane_roll(field, HALO), lane_roll(packed, HALO - NC)),
        jnp.where(near, field, lane_roll(packed, HALO)),
    )


def second_step_kernel(
    par, got1, got2, ext, ext_cols, rows_in, setup_cols, cols_right, cols_left, edges, coeffs, partial, trans, wells,
    diag_hbm, inverse_hbm, couple_hbm,
    msgx1, msgx2, msgy1, msgy2, z_out, vector_out, remainder, product,
    diag, inverse, couple, sems,
):
    copies = load_blocks((diag_hbm, inverse_hbm, couple_hbm), (diag, inverse, couple), sems)
    rows, lanes = iotas((EX, L))
    right, left = take(par, 1, got1, got2, pl.ds(0, EX))
    packed, tw = (ext_cols[...], setup_cols[...])
    old_right, old_left = (cols_right[...], cols_left[...])
    own_right = lane_sum(lane_roll(tw, HALO - 3 * NC) * right, HALO)
    own_left = lane_sum(lane_roll(tw, HALO - NC) * left, HALO)
    far_right = lane_sum(old_right * lane_roll(packed, 64), 64 + NC)
    far_left = lane_sum(old_left * lane_roll(packed, 64 + NC), 64 + NC)
    near = ext[...] - jnp.where(lanes == L - 1, own_right, 0.0) - jnp.where(lanes == 0, own_left, 0.0)
    far = jnp.where(
        lanes < HALO, right, jnp.where(lanes >= L - HALO, lane_roll(left, L - HALO), 0.0)
    )
    far = far - jnp.where(lanes == 0, far_right, 0.0) - jnp.where(lanes == L - 1, far_left, 0.0)
    pressure = vcycle(jnp.concatenate([near, far], axis=1), coeffs)
    vector = []
    for c in range(NC):
        ghosts = ghost_sum(
            trans,
            rows_in[pl.ds(c, 1), :],
            rows_in[pl.ds(NC + c, 1), :],
            ghost_column(right[0:R], HALO, L - 1, c),
            ghost_column(left[0:R], HALO, 0, c),
        )
        value = partial[c] - ghosts
        vector_out[c] = value
        vector.append(value)
    for copy in copies:
        copy.wait()
    boost = WELL_BOOST * wells[...].astype(jnp.float32)
    result = one_step(
        pressure, vector, edges, old_right[0:R], old_left[0:R], diag, inverse, couple, trans, boost, z_out, product
    )
    to_right, to_left = ([], [])
    for c in range(NC):
        remainder[c] = result[c]
        put(par, 0, msgx1, msgx2, pl.ds(c, 1), product[c, R - 1 : R, :], product[c, 0:1, :])
        to_right.append((product[c], L - 1, c))
        to_left.append((product[c], 0, c))
    blank = jnp.zeros((16 - NC, L), jnp.float32)
    msgx1[pl.ds(NC, 16 - NC), :] = blank
    msgx2[pl.ds(NC, 16 - NC), :] = blank
    put(par, 1, msgy1, msgy2, pl.ds(0, R), pack_columns(to_right), pack_columns(to_left))


def dots_kernel(par, gotx1, gotx2, goty1, goty2, rhs, vector, remainder, trans, out):
    right, left = take(par, 1, goty1, goty2, pl.ds(0, R))
    sums = [jnp.zeros((R, L), jnp.float32) for _ in range(6)]
    for c in range(NC):
        up, down = take(par, 0, gotx1, gotx2, pl.ds(c, 1))
        ghosts = ghost_sum(trans, up, down, ghost_column(right, 0, L - 1, c), ghost_column(left, 0, 0, c))
        two = remainder[c] - ghosts
        zero, one = (rhs[c], vector[c])
        for k, (a, b) in enumerate(((zero, zero), (zero, one), (one, one), (zero, two), (one, two), (two, two))):
            sums[k] = sums[k] + a * b
    lanes = iotas((1, L))[1]
    row = jnp.zeros((1, L), jnp.float32)
    for k, total in enumerate(sums):
        row = jnp.where(lanes == k, jnp.sum(total, keepdims=True), row)
    out[...] = jnp.broadcast_to(row, out.shape)


def finish_kernel(gathered, z_one, z_two, out, estimate):
    row = jnp.sum(gathered[...], axis=0, keepdims=True)
    lanes = iotas((1, L))[1]
    g00, g01, g11, g02, g12, g22 = (
        jnp.sum(jnp.where(lanes == k, row, 0.0), axis=1, keepdims=True) for k in range(6)
    )
    beta = jnp.sqrt(g00)
    shift = g01 / g00
    h00 = 1.0 + shift
    length2 = g11 - shift * g01
    length = jnp.sqrt(length2)
    h10 = length / beta
    h01 = (g02 - shift * g01) / (beta * length)
    above = (g12 - shift * g02 - shift * (g11 - shift * g01)) / length2
    h11 = 1.0 + above
    h21 = jnp.sqrt((g22 - 2.0 * shift * g12 + shift * shift * g11) / length2 - h01 * h01 - above * above)
    radius0 = jnp.sqrt(h00 * h00 + h10 * h10)
    cos0, sin0 = (h00 / radius0, h10 / radius0)
    r01 = cos0 * h01 + sin0 * h11
    mid = cos0 * h11 - sin0 * h01
    radius1 = jnp.sqrt(mid * mid + h21 * h21)
    cos1, sin1 = (mid / radius1, h21 / radius1)
    rhs0, rhs1 = (cos0 * beta, -sin0 * beta)
    estimate[...] = jnp.abs(sin1 * rhs1)
    y1 = cos1 * rhs1 / radius1
    y0 = (rhs0 - r01 * y1) / radius0
    weight1 = y1 / length
    weight0 = y0 / beta - weight1 * shift
    for c in range(NC):
        out[c] = weight0 * z_one[c] + weight1 * z_two[c]


VMEM = functools.partial(pl.BlockSpec, memory_space=pltpu.VMEM)
SMEM = functools.partial(pl.BlockSpec, memory_space=pltpu.SMEM)
ANY = functools.partial(pl.BlockSpec, memory_space=pl.ANY)


def shape(*dims):
    return jax.ShapeDtypeStruct(dims, jnp.float32)


def call(kernel, in_specs, outs, scratch=(), cost=20_000_000):
    return pl.pallas_call(
        kernel,
        in_specs=list(in_specs),
        out_specs=[VMEM()] * len(outs),
        out_shape=list(outs),
        scratch_shapes=list(scratch),
        cost_estimate=pl.CostEstimate(flops=cost, bytes_accessed=1_000_000, transcendentals=0),
        compiler_params=pltpu.CompilerParams(vmem_limit_bytes=30 * 1024 * 1024),
    )


def swap(first, second, axis):
    peers = lax.axis_size(axis)
    pairs = [(i, i ^ 1) for i in range(peers) if i ^ 1 < peers]
    others = [(i, ((i + 1) ^ 1) - 1) for i in range(1, peers) if ((i + 1) ^ 1) - 1 < peers]
    return (lax.ppermute(first, axis, pairs), lax.ppermute(second, axis, others))


def on_device(right_side, diag_blocks, couple_blocks, transmissibility, pressure_weights, well_mask):
    par = jnp.stack([lax.axis_index("gx") % 2, lax.axis_index("gy") % 2]).astype(jnp.int32)
    column = pl.BlockSpec((NC, 1, R, L), lambda i: (0, 0, 0, 0))

    def whole(*dims):
        return pl.BlockSpec(dims, lambda i: (0,) * len(dims))

    msg_a1, msg_a2, own, cols = pl.pallas_call(
        setup_kernel,
        grid=(1,),
        in_specs=[
            SMEM(), whole(NC, R, L), column, column, whole(4, R, L), whole(NC, R, L), whole(R, L),
        ],
        out_specs=[whole(AX_ROWS, L), whole(AX_ROWS, L), whole(6 * R, L), whole(R, L)],
        out_shape=[shape(AX_ROWS, L), shape(AX_ROWS, L), shape(6 * R, L), shape(R, L)],
        compiler_params=pltpu.CompilerParams(vmem_limit_bytes=30 * 1024 * 1024),
    )(par, right_side, diag_blocks, couple_blocks, transmissibility, pressure_weights, well_mask)

    got_a1, got_a2 = swap(msg_a1, msg_a2, "gx")

    slab = pl.BlockSpec((NC, NC, 8, L), lambda i: (0, 0, i, 0))
    inverse = pl.pallas_call(
        inverse_kernel,
        grid=(R // 8,),
        in_specs=[slab, pl.BlockSpec((8, L), lambda i: (i, 0))],
        out_specs=slab,
        out_shape=shape(NC, NC, R, L),
        cost_estimate=pl.CostEstimate(flops=20_000_000, bytes_accessed=2_700_000, transcendentals=0),
        compiler_params=pltpu.CompilerParams(vmem_limit_bytes=30 * 1024 * 1024),
    )(diag_blocks, well_mask)

    msg_y1, msg_y2, ext, ext_cols, edges = pl.pallas_call(
        setup_middle_kernel,
        grid=(1,),
        in_specs=[
            SMEM(), whole(AX_ROWS, L), whole(AX_ROWS, L), whole(6 * R, L), whole(R, L), column,
            whole(4, R, L), whole(NC, R, L),
        ],
        out_specs=[whole(AY_ROWS, L), whole(AY_ROWS, L), whole(6, EX, L), whole(EX, L), whole(4 * NC, L)],
        out_shape=[shape(AY_ROWS, L), shape(AY_ROWS, L), shape(6, EX, L), shape(EX, L), shape(4 * NC, L)],
        compiler_params=pltpu.CompilerParams(vmem_limit_bytes=30 * 1024 * 1024),
    )(par, got_a1, got_a2, own, cols, couple_blocks, transmissibility, pressure_weights)

    got_y1, got_y2 = swap(msg_y1, msg_y2, "gy")

    blocks = [pltpu.VMEM((NC, NC, R, L), jnp.float32)] * 3 + [pltpu.SemaphoreType.DMA((3,))]
    fields = shape(NC, R, L)
    msg_b1, msg_b2, z_one, partial, product, coeffs, cols_right, cols_left, pressure_part, product_cols = call(
        first_step_kernel,
        [SMEM()] + [VMEM()] * 9 + [ANY()] * 3,
        [
            shape(BX_ROWS, L), shape(BX_ROWS, L), fields, fields, fields, shape(18, EX, EY),
            shape(EX, L), shape(EX, L), shape(R, L), shape(R, L),
        ],
        blocks,
    )(
        par, got_y1, got_y2, ext, ext_cols, edges, right_side, transmissibility, pressure_weights, well_mask,
        diag_blocks, inverse, couple_blocks,
    )

    got_b1, got_b2 = swap(msg_b1, msg_b2, "gx")
    msg_c1, msg_c2, ext_b, ext_cols_b, rows_b = call(
        between_kernel,
        [SMEM()] + [VMEM()] * 8,
        [shape(EX, L), shape(EX, L), shape(EX, L), shape(EX, L), shape(2 * NC, L)],
    )(par, got_b1, got_b2, pressure_part, product_cols, product, edges, transmissibility, pressure_weights)
    got_c1, got_c2 = swap(msg_c1, msg_c2, "gy")

    msg_x1, msg_x2, msg_z1, msg_z2, z_two, vector, remainder, _ = call(
        second_step_kernel,
        [SMEM()] + [VMEM()] * 13 + [ANY()] * 3,
        [shape(16, L), shape(16, L), shape(R, L), shape(R, L), fields, fields, fields, fields],
        blocks,
    )(
        par, got_c1, got_c2, ext_b, ext_cols_b, rows_b, ext_cols, cols_right, cols_left, edges, coeffs, partial,
        transmissibility, well_mask, diag_blocks, inverse, couple_blocks,
    )
    got_x1, got_x2 = swap(msg_x1, msg_x2, "gx")
    got_z1, got_z2 = swap(msg_z1, msg_z2, "gy")
    devices = lax.axis_size("gx") * lax.axis_size("gy")
    (local,) = call(dots_kernel, [SMEM()] + [VMEM()] * 8, [shape(devices, L)])(
        par, got_x1, got_x2, got_z1, got_z2, right_side, vector, remainder, transmissibility
    )
    gathered = lax.all_to_all(local, ("gx", "gy"), 0, 0, tiled=True)
    answer, estimate = call(finish_kernel, [VMEM()] * 3, [fields, shape(1, 1)])(gathered, z_one, z_two)
    return (answer, estimate.reshape(()))


def solution(mesh):
    return jax.shard_map(
        on_device,
        mesh=mesh,
        in_specs=(
            P(None, "gx", "gy"),
            P(None, None, "gx", "gy"),
            P(None, None, "gx", "gy"),
            P(None, "gx", "gy"),
            P(None, "gx", "gy"),
            P("gx", "gy"),
        ),
        out_specs=(P(None, "gx", "gy"), P()),
        check_vma=False,
    )
```

```python
import functools

import jax
import jax.numpy as jnp
from jax import lax
from jax.experimental import pallas as pl
from jax.experimental.pallas import tpu as pltpu
from jax.sharding import PartitionSpec as P

NC = 9
COARSE_SWEEPS = 6
RELAX = 0.8
WELL_BOOST = 8.0

R, L = 32, 128
HALO = 32
EX, EY = 3 * R, 2 * L

AX_EDGE = 6 * R
AX_COL = AX_EDGE + 24
AX_ROWS = AX_COL + R
AY_ROWS = 2 * EX
BX_EDGE = R
BX_COL = BX_EDGE + 16
BX_ROWS = BX_COL + R

CENTER, EAST, WEST, NORTH, SOUTH, SCALE = range(6)


def iotas(shape):
    return (lax.broadcasted_iota(jnp.int32, shape, 0), lax.broadcasted_iota(jnp.int32, shape, 1))


def shifted(values, axis, step):
    return pltpu.roll(values, (-step) % values.shape[axis], axis)


def lane_roll(values, shift):
    shift = shift % values.shape[1]
    return values if shift == 0 else pltpu.roll(values, shift, 1)


def even_mask(par_ref, which, shape):
    return jnp.full(shape, par_ref[which], jnp.int32) == 0


def put(par_ref, which, first, second, rows, up, down):
    even = even_mask(par_ref, which, up.shape)
    first[rows, :] = jnp.where(even, up, down)
    second[rows, :] = jnp.where(even, down, up)


def take(par_ref, which, first, second, rows):
    one, two = (first[rows, :], second[rows, :])
    even = even_mask(par_ref, which, one.shape)
    return (jnp.where(even, one, two), jnp.where(even, two, one))


def pack_columns(parts):
    shape = parts[0][0].shape
    lanes = iotas(shape)[1]
    packed = jnp.zeros(shape, jnp.float32)
    for values, lane, target in parts:
        packed = jnp.where(lanes == target, lane_roll(values, target - lane), packed)
    return packed


def setup_kernel(
    par, rhs_hbm, diag_hbm, couple_hbm, trans_hbm, weights_hbm, wells_hbm, msg1, msg2, own, cols,
    rhs, diag0, couple0, trans, weights, wells, sems,
):
    pairs = (
        (weights_hbm, weights),
        (couple_hbm.at[:, 0:1], couple0),
        (diag_hbm.at[:, 0:1], diag0),
        (trans_hbm, trans),
        (rhs_hbm, rhs),
        (wells_hbm, wells),
    )
    copies = [pltpu.make_async_copy(a, b, sems.at[i]) for i, (a, b) in enumerate(pairs)]
    for copy in copies:
        copy.start()
    for copy in copies:
        copy.wait()
    rows, lanes = iotas((R, L))
    center = WELL_BOOST * wells[...].astype(jnp.float32) * weights[0]
    pressure = jnp.zeros((R, L), jnp.float32)
    links = [jnp.zeros((R, L), jnp.float32) for _ in range(4)]
    for c in range(NC):
        w, col = (weights[c], couple0[c, 0])
        center = center + w * diag0[c, 0]
        pressure = pressure + w * rhs[c]
        for d, (axis, step) in enumerate(((0, 1), (0, -1), (1, 1), (1, -1))):
            links[d] = links[d] + w * shifted(col, axis, step)
    inside = (rows != R - 1, rows != 0, lanes != L - 1, lanes != 0)
    fields = [center]
    for d in range(4):
        fields.append(jnp.where(inside[d], -trans[d] * links[d], 0.0))
    fields.append(pressure)
    for k, field in enumerate(fields):
        span = pl.ds(k * R, R)
        own[span, :] = field
        msg1[span, :] = field
        msg2[span, :] = field
    t_up, t_down = (trans[0, R - 1 : R, :], trans[1, 0:1, :])
    t_right, t_left = (trans[2], trans[3])
    for c in range(NC):
        put(par, 0, msg1, msg2, pl.ds(AX_EDGE + c, 1), couple0[c, 0, R - 1 : R, :], couple0[c, 0, 0:1, :])
        put(par, 0, msg1, msg2, pl.ds(AX_EDGE + NC + c, 1), t_up * weights[c, R - 1 : R, :], t_down * weights[c, 0:1, :])
    blank = jnp.zeros((24 - 2 * NC, L), jnp.float32)
    msg1[pl.ds(AX_EDGE + 2 * NC, 24 - 2 * NC), :] = blank
    msg2[pl.ds(AX_EDGE + 2 * NC, 24 - 2 * NC), :] = blank
    parts = []
    for c in range(NC):
        col, w = (couple0[c, 0], weights[c])
        parts += [(col, 0, c), (t_left * w, 0, NC + c), (col, L - 1, 2 * NC + c), (t_right * w, L - 1, 3 * NC + c)]
    packed = pack_columns(parts)
    cols[...] = packed
    msg1[pl.ds(AX_COL, R), :] = packed
    msg2[pl.ds(AX_COL, R), :] = packed


def inverse_kernel(diag, wells, out):
    boost = WELL_BOOST * wells[...].astype(jnp.float32)
    a = [[diag[i, j] + boost if i == j else diag[i, j] for j in range(NC)] for i in range(NC)]
    for k in range(NC):
        inv = 1.0 / a[k][k]
        a[k] = [inv if j == k else a[k][j] * inv for j in range(NC)]
        for i in range(NC):
            if i != k:
                factor = a[i][k]
                a[i] = [-factor * inv if j == k else a[i][j] - factor * a[k][j] for j in range(NC)]
    for i in range(NC):
        for j in range(NC):
            out[i, j] = a[i][j]


def setup_middle_kernel(par, got1, got2, own, cols, couple0, trans, weights, msg1, msg2, ext, ext_cols, edges):
    rows, lanes = iotas((EX, L))

    def dots(span_of):
        total = jnp.zeros((1, L), jnp.float32)
        for c in range(NC):
            total = total + span_of(c)
        return -total

    ups, downs, tw_ups, tw_downs = ([], [], [], [])
    for c in range(NC):
        up, down = take(par, 0, got1, got2, pl.ds(AX_EDGE + c, 1))
        ups.append(up)
        downs.append(down)
        up, down = take(par, 0, got1, got2, pl.ds(AX_EDGE + NC + c, 1))
        tw_ups.append(up)
        tw_downs.append(down)
        edges[pl.ds(c, 1), :] = ups[c]
        edges[pl.ds(NC + c, 1), :] = downs[c]
        edges[pl.ds(2 * NC + c, 1), :] = tw_ups[c]
        edges[pl.ds(3 * NC + c, 1), :] = tw_downs[c]
    t_up, t_down = (trans[0, R - 1 : R, :], trans[1, 0:1, :])
    east_own = dots(lambda c: t_up * weights[c, R - 1 : R, :] * ups[c])
    west_own = dots(lambda c: t_down * weights[c, 0:1, :] * downs[c])
    west_up = dots(lambda c: tw_ups[c] * couple0[c, 0, R - 1 : R, :])
    east_down = dots(lambda c: tw_downs[c] * couple0[c, 0, 0:1, :])
    fields = []
    for k in range(6):
        up, down = take(par, 0, got1, got2, pl.ds(k * R, R))
        field = jnp.concatenate([own[pl.ds(k * R, R), :], up, down], axis=0)
        if k == CENTER:
            field = jnp.where(field == 0.0, 1.0, field)
        if k == EAST:
            field = jnp.where(rows == R - 1, east_own, jnp.where(rows == EX - 1, east_down, field))
        if k == WEST:
            field = jnp.where(rows == 0, west_own, jnp.where(rows == R, west_up, field))
        ext[k] = field
        fields.append(field)
    up, down = take(par, 0, got1, got2, pl.ds(AX_COL, R))
    packed = jnp.concatenate([cols[...], up, down], axis=0)
    ext_cols[...] = packed
    to_right = [lane_roll(f, HALO * (k % 4) + HALO) for k, f in enumerate(fields)]
    to_left = [lane_roll(f, HALO * (k % 4)) for k, f in enumerate(fields)]
    group = lanes // HALO

    def quad(parts):
        result = parts[-1]
        for g in range(len(parts) - 2, -1, -1):
            result = jnp.where(group == g, parts[g], result)
        return result

    put(par, 1, msg1, msg2, pl.ds(0, EX), quad(to_right[:4]), quad(to_left[:4]))
    put(
        par,
        1,
        msg1,
        msg2,
        pl.ds(EX, EX),
        quad(to_right[4:] + [lane_roll(packed, 64 - 2 * NC)]),
        quad(to_left[4:] + [lane_roll(packed, 64)]),
    )


def lane_sum(product, start):
    lanes = iotas(product.shape)[1]
    keep = jnp.logical_and(lanes >= start, lanes < start + NC)
    return jnp.sum(jnp.where(keep, product, 0.0), axis=1, keepdims=True)


def pair_sums(values, step):
    rows, lanes = iotas(values.shape)
    values = values + jnp.where((rows // step) % 2 == 0, shifted(values, 0, step), shifted(values, 0, -step))
    return values + jnp.where((lanes // step) % 2 == 0, shifted(values, 1, step), shifted(values, 1, -step))


def coarsen_into(coeffs, level):
    step = 2**level
    base, out = (6 * level, 6 * level + 6)
    rows, lanes = iotas((EX, EY))
    row_even = (rows // step) % 2 == 0
    lane_even = (lanes // step) % 2 == 0
    east, west, north, south = (coeffs[base + d] for d in (EAST, WEST, NORTH, SOUTH))
    center = coeffs[base] + (jnp.where(row_even, east, west) + jnp.where(lane_even, north, south))
    center = pair_sums(center, step)
    coeffs[out + CENTER] = center
    coeffs[out + SCALE] = RELAX / center
    coeffs[out + EAST] = pair_sums(jnp.where(row_even, 0.0, east), step)
    coeffs[out + WEST] = pair_sums(jnp.where(row_even, west, 0.0), step)
    coeffs[out + NORTH] = pair_sums(jnp.where(lane_even, 0.0, north), step)
    coeffs[out + SOUTH] = pair_sums(jnp.where(lane_even, south, 0.0), step)


def level_apply(values, coeffs, level):
    step = 2**level
    base = 6 * level
    return coeffs[base + CENTER] * values + (
        coeffs[base + EAST] * shifted(values, 0, step)
        + coeffs[base + WEST] * shifted(values, 0, -step)
        + coeffs[base + NORTH] * shifted(values, 1, step)
        + coeffs[base + SOUTH] * shifted(values, 1, -step)
    )


def sweep(values, source, coeffs, level):
    return values + coeffs[6 * level + SCALE] * (source - level_apply(values, coeffs, level))


def vcycle(source, coeffs):
    values0 = coeffs[SCALE] * source
    source1 = pair_sums(source - level_apply(values0, coeffs, 0), 1)
    values1 = coeffs[6 + SCALE] * source1
    source2 = pair_sums(source1 - level_apply(values1, coeffs, 1), 2)
    values2 = coeffs[12 + SCALE] * source2
    for _ in range(COARSE_SWEEPS - 1):
        values2 = sweep(values2, source2, coeffs, 2)
    values1 = sweep(values1 + values2, source1, coeffs, 1)
    return sweep(values0 + values1, source, coeffs, 0)


def ghost_column(packed, start, to_lane, lane):
    return lane_roll(packed, to_lane - (start + lane))


def neighbour_sum(values, trans, up_row, down_row, right_col, left_col):
    rows, lanes = iotas((R, L))
    east = jnp.where(rows == R - 1, up_row, shifted(values, 0, 1))
    west = jnp.where(rows == 0, down_row, shifted(values, 0, -1))
    north = jnp.where(lanes == L - 1, right_col, shifted(values, 1, 1))
    south = jnp.where(lanes == 0, left_col, shifted(values, 1, -1))
    return trans[0] * east + trans[1] * west + trans[2] * north + trans[3] * south


def ghost_sum(trans, up_row, down_row, right_col, left_col):
    rows, lanes = iotas((R, L))
    return (
        jnp.where(rows == R - 1, trans[0] * up_row, 0.0)
        + jnp.where(rows == 0, trans[1] * down_row, 0.0)
        + jnp.where(lanes == L - 1, trans[2] * right_col, 0.0)
        + jnp.where(lanes == 0, trans[3] * left_col, 0.0)
    )


def one_step(pressure, vector, edges, col_right, col_left, diag, inverse, couple, trans, boost, z_out, product_out):
    p = pressure[0:R, 0:L]
    up_row, down_row = (pressure[R : R + 1, 0:L], pressure[EX - 1 : EX, 0:L])
    far = pressure[0:R, L:EY]
    right_p, left_p = (lane_roll(far, L - 1), lane_roll(far, 1))
    second = []
    for c in range(NC):
        own = diag[c, 0] * p
        if c == 0:
            own = own + boost * p
        around = neighbour_sum(
            couple[c, 0] * p,
            trans,
            edges[pl.ds(c, 1), :] * up_row,
            edges[pl.ds(NC + c, 1), :] * down_row,
            ghost_column(col_right, 64, L - 1, c) * right_p,
            ghost_column(col_left, 64, 0, c) * left_p,
        )
        second.append(vector[c] - (own - around))
    z = []
    for c in range(NC):
        total = inverse[c, 0] * second[0]
        for k in range(1, NC):
            total = total + inverse[c, k] * second[k]
        if c == 0:
            total = total + p
        z_out[c] = total
        z.append(total)
    result = []
    for c in range(NC):
        product = couple[c, 0] * z[0]
        own = diag[c, 0] * z[0]
        for k in range(1, NC):
            product = product + couple[c, k] * z[k]
            own = own + diag[c, k] * z[k]
        product_out[c] = product
        own = own + boost * z[c]
        zero = jnp.zeros((1, L), jnp.float32)
        around = neighbour_sum(product, trans, zero, zero, 0.0, 0.0)
        result.append(own - around - vector[c])
    return result


def first_step_kernel(
    par, got1, got2, ext, ext_cols, edges, rhs, trans, weights, wells, diag, inverse, couple,
    msg1, msg2, z_out, partial, product, coeffs, cols_right, cols_left, pressure_part, product_cols,
):
    rows, lanes = iotas((EX, L))
    right, left = take(par, 1, got1, got2, pl.ds(EX, EX))
    cols_right[...] = right
    cols_left[...] = left
    packed = ext_cols[...]
    north_own = -lane_sum(lane_roll(packed, 64 - 3 * NC) * right, 64)
    south_right = -lane_sum(lane_roll(packed, 64 - NC) * right, 64 + NC)
    south_own = -lane_sum(lane_roll(packed, 64 - NC) * left, 64)
    north_left = -lane_sum(lane_roll(packed, 64 + NC) * left, 64 + NC)
    right_four, left_four = take(par, 1, got1, got2, pl.ds(0, EX))
    source = None
    for k in range(6):
        from_right = lane_roll(right_four if k < 4 else right, -HALO * (k % 4))
        from_left = lane_roll(left_four if k < 4 else left, L - HALO - HALO * (k % 4))
        near = ext[k]
        far = jnp.where(lanes < HALO, from_right, jnp.where(lanes >= L - HALO, from_left, 0.0))
        if k == CENTER:
            far = jnp.where(far == 0.0, 1.0, far)
        if k == NORTH:
            near = jnp.where(lanes == L - 1, north_own, near)
            far = jnp.where(lanes == L - 1, north_left, far)
        if k == SOUTH:
            near = jnp.where(lanes == 0, south_own, near)
            far = jnp.where(lanes == 0, south_right, far)
        field = jnp.concatenate([near, far], axis=1)
        if k == 5:
            source = field
        else:
            coeffs[k] = field
    coeffs[SCALE] = RELAX / coeffs[CENTER]
    coarsen_into(coeffs, 0)
    coarsen_into(coeffs, 1)
    pressure = vcycle(source, coeffs)
    boost = WELL_BOOST * wells[...].astype(jnp.float32)
    vector = [rhs[c] for c in range(NC)]
    result = one_step(
        pressure, vector, edges, right[0:R], left[0:R], diag, inverse, couple, trans, boost, z_out, product
    )
    weighed = jnp.zeros((R, L), jnp.float32)
    parts = []
    for c in range(NC):
        partial[c] = result[c]
        weighed = weighed + weights[c] * result[c]
        put(par, 0, msg1, msg2, pl.ds(BX_EDGE + c, 1), product[c, R - 1 : R, :], product[c, 0:1, :])
        parts += [(product[c], 0, c), (product[c], L - 1, NC + c)]
    blank = jnp.zeros((16 - NC, L), jnp.float32)
    columns = pack_columns(parts)
    pressure_part[...] = weighed
    product_cols[...] = columns
    for msg in (msg1, msg2):
        msg[pl.ds(0, R), :] = weighed
        msg[pl.ds(BX_EDGE + NC, 16 - NC), :] = blank
        msg[pl.ds(BX_COL, R), :] = columns


def between_kernel(par, got1, got2, pressure_part, product_cols, product, edges, trans, weights, msg1, msg2, ext, ext_cols, rows_out):
    rows, lanes = iotas((EX, L))
    t_up, t_down = (trans[0, R - 1 : R, :], trans[1, 0:1, :])
    own_up, own_down, far_up, far_down = (jnp.zeros((1, L), jnp.float32) for _ in range(4))
    for c in range(NC):
        up, down = take(par, 0, got1, got2, pl.ds(BX_EDGE + c, 1))
        rows_out[pl.ds(c, 1), :] = up
        rows_out[pl.ds(NC + c, 1), :] = down
        own_up = own_up + t_up * weights[c, R - 1 : R, :] * up
        own_down = own_down + t_down * weights[c, 0:1, :] * down
        far_up = far_up + edges[pl.ds(2 * NC + c, 1), :] * product[c, R - 1 : R, :]
        far_down = far_down + edges[pl.ds(3 * NC + c, 1), :] * product[c, 0:1, :]
    up, down = take(par, 0, got1, got2, pl.ds(0, R))
    field = jnp.concatenate([pressure_part[...], up, down], axis=0)
    edge = jnp.where(rows == R - 1, own_up, 0.0) + jnp.where(rows == 0, own_down, 0.0)
    edge = edge + jnp.where(rows == R, far_up, 0.0) + jnp.where(rows == EX - 1, far_down, 0.0)
    field = field - edge
    ext[...] = field
    up, down = take(par, 0, got1, got2, pl.ds(BX_COL, R))
    packed = jnp.concatenate([product_cols[...], up, down], axis=0)
    ext_cols[...] = packed
    near = lanes < HALO
    put(
        par, 1, msg1, msg2, pl.ds(0, EX),
        jnp.where(near, lane_roll(field, HALO), lane_roll(packed, HALO - NC)),
        jnp.where(near, field, lane_roll(packed, HALO)),
    )


def second_step_kernel(
    par, got1, got2, ext, ext_cols, rows_in, setup_cols, cols_right, cols_left, edges, coeffs, partial, trans, wells,
    diag, inverse, couple,
    msgx1, msgx2, msgy1, msgy2, z_out, vector_out, remainder, product,
):
    rows, lanes = iotas((EX, L))
    right, left = take(par, 1, got1, got2, pl.ds(0, EX))
    packed, tw = (ext_cols[...], setup_cols[...])
    old_right, old_left = (cols_right[...], cols_left[...])
    own_right = lane_sum(lane_roll(tw, HALO - 3 * NC) * right, HALO)
    own_left = lane_sum(lane_roll(tw, HALO - NC) * left, HALO)
    far_right = lane_sum(old_right * lane_roll(packed, 64), 64 + NC)
    far_left = lane_sum(old_left * lane_roll(packed, 64 + NC), 64 + NC)
    near = ext[...] - jnp.where(lanes == L - 1, own_right, 0.0) - jnp.where(lanes == 0, own_left, 0.0)
    far = jnp.where(
        lanes < HALO, right, jnp.where(lanes >= L - HALO, lane_roll(left, L - HALO), 0.0)
    )
    far = far - jnp.where(lanes == 0, far_right, 0.0) - jnp.where(lanes == L - 1, far_left, 0.0)
    pressure = vcycle(jnp.concatenate([near, far], axis=1), coeffs)
    vector = []
    for c in range(NC):
        ghosts = ghost_sum(
            trans,
            rows_in[pl.ds(c, 1), :],
            rows_in[pl.ds(NC + c, 1), :],
            ghost_column(right[0:R], HALO, L - 1, c),
            ghost_column(left[0:R], HALO, 0, c),
        )
        value = partial[c] - ghosts
        vector_out[c] = value
        vector.append(value)
    boost = WELL_BOOST * wells[...].astype(jnp.float32)
    result = one_step(
        pressure, vector, edges, old_right[0:R], old_left[0:R], diag, inverse, couple, trans, boost, z_out, product
    )
    to_right, to_left = ([], [])
    for c in range(NC):
        remainder[c] = result[c]
        put(par, 0, msgx1, msgx2, pl.ds(c, 1), product[c, R - 1 : R, :], product[c, 0:1, :])
        to_right.append((product[c], L - 1, c))
        to_left.append((product[c], 0, c))
    blank = jnp.zeros((16 - NC, L), jnp.float32)
    msgx1[pl.ds(NC, 16 - NC), :] = blank
    msgx2[pl.ds(NC, 16 - NC), :] = blank
    put(par, 1, msgy1, msgy2, pl.ds(0, R), pack_columns(to_right), pack_columns(to_left))


def dots_kernel(par, gotx1, gotx2, goty1, goty2, rhs, vector, remainder, trans, out):
    right, left = take(par, 1, goty1, goty2, pl.ds(0, R))
    sums = [jnp.zeros((R, L), jnp.float32) for _ in range(6)]
    for c in range(NC):
        up, down = take(par, 0, gotx1, gotx2, pl.ds(c, 1))
        ghosts = ghost_sum(trans, up, down, ghost_column(right, 0, L - 1, c), ghost_column(left, 0, 0, c))
        two = remainder[c] - ghosts
        zero, one = (rhs[c], vector[c])
        for k, (a, b) in enumerate(((zero, zero), (zero, one), (one, one), (zero, two), (one, two), (two, two))):
            sums[k] = sums[k] + a * b
    lanes = iotas((1, L))[1]
    row = jnp.zeros((1, L), jnp.float32)
    for k, total in enumerate(sums):
        row = jnp.where(lanes == k, jnp.sum(total, keepdims=True), row)
    out[...] = jnp.broadcast_to(row, out.shape)


def finish_kernel(gathered, z_one, z_two, out, estimate):
    row = jnp.sum(gathered[...], axis=0, keepdims=True)
    lanes = iotas((1, L))[1]
    g00, g01, g11, g02, g12, g22 = (
        jnp.sum(jnp.where(lanes == k, row, 0.0), axis=1, keepdims=True) for k in range(6)
    )
    beta = jnp.sqrt(g00)
    shift = g01 / g00
    h00 = 1.0 + shift
    length2 = g11 - shift * g01
    length = jnp.sqrt(length2)
    h10 = length / beta
    h01 = (g02 - shift * g01) / (beta * length)
    above = (g12 - shift * g02 - shift * (g11 - shift * g01)) / length2
    h11 = 1.0 + above
    h21 = jnp.sqrt((g22 - 2.0 * shift * g12 + shift * shift * g11) / length2 - h01 * h01 - above * above)
    radius0 = jnp.sqrt(h00 * h00 + h10 * h10)
    cos0, sin0 = (h00 / radius0, h10 / radius0)
    r01 = cos0 * h01 + sin0 * h11
    mid = cos0 * h11 - sin0 * h01
    radius1 = jnp.sqrt(mid * mid + h21 * h21)
    cos1, sin1 = (mid / radius1, h21 / radius1)
    rhs0, rhs1 = (cos0 * beta, -sin0 * beta)
    estimate[...] = jnp.abs(sin1 * rhs1)
    y1 = cos1 * rhs1 / radius1
    y0 = (rhs0 - r01 * y1) / radius0
    weight1 = y1 / length
    weight0 = y0 / beta - weight1 * shift
    for c in range(NC):
        out[c] = weight0 * z_one[c] + weight1 * z_two[c]


VMEM = functools.partial(pl.BlockSpec, memory_space=pltpu.VMEM)
SMEM = functools.partial(pl.BlockSpec, memory_space=pltpu.SMEM)
HBM = functools.partial(pl.BlockSpec, memory_space=pltpu.HBM)


def shape(*dims):
    return jax.ShapeDtypeStruct(dims, jnp.float32)


def call(kernel, in_specs, outs, scratch=(), cost=20_000_000):
    return pl.pallas_call(
        kernel,
        in_specs=list(in_specs),
        out_specs=[VMEM()] * len(outs),
        out_shape=list(outs),
        scratch_shapes=list(scratch),
        cost_estimate=pl.CostEstimate(flops=cost, bytes_accessed=1_000_000, transcendentals=0),
        compiler_params=pltpu.CompilerParams(vmem_limit_bytes=30 * 1024 * 1024),
    )


def swap(first, second, axis):
    peers = lax.axis_size(axis)
    pairs = [(i, i ^ 1) for i in range(peers) if i ^ 1 < peers]
    others = [(i, ((i + 1) ^ 1) - 1) for i in range(1, peers) if ((i + 1) ^ 1) - 1 < peers]
    return (lax.ppermute(first, axis, pairs), lax.ppermute(second, axis, others))


def on_device(right_side, diag_blocks, couple_blocks, transmissibility, pressure_weights, well_mask):
    par = jnp.stack([lax.axis_index("gx") & 1, lax.axis_index("gy") & 1]).astype(jnp.int32)
    column = pl.BlockSpec((NC, 1, R, L), lambda i: (0, 0, 0, 0))

    def whole(*dims):
        return pl.BlockSpec(dims, lambda i: (0,) * len(dims))

    msg_a1, msg_a2, own, cols = call(
        setup_kernel,
        [SMEM()] + [HBM()] * 6,
        [shape(AX_ROWS, L), shape(AX_ROWS, L), shape(6 * R, L), shape(R, L)],
        [
            pltpu.VMEM((NC, R, L), jnp.float32),
            pltpu.VMEM((NC, 1, R, L), jnp.float32),
            pltpu.VMEM((NC, 1, R, L), jnp.float32),
            pltpu.VMEM((4, R, L), jnp.float32),
            pltpu.VMEM((NC, R, L), jnp.float32),
            pltpu.VMEM((R, L), jnp.int32),
            pltpu.SemaphoreType.DMA((6,)),
        ],
    )(
        par,
        *(
            pltpu.with_memory_space_constraint(x, pltpu.HBM)
            for x in (right_side, diag_blocks, couple_blocks, transmissibility, pressure_weights, well_mask)
        ),
    )

    got_a1, got_a2 = swap(msg_a1, msg_a2, "gx")

    slab = pl.BlockSpec((NC, NC, 8, L), lambda i: (0, 0, i, 0))
    inverse = pl.pallas_call(
        inverse_kernel,
        grid=(R // 8,),
        in_specs=[slab, pl.BlockSpec((8, L), lambda i: (i, 0))],
        out_specs=slab,
        out_shape=shape(NC, NC, R, L),
        cost_estimate=pl.CostEstimate(flops=20_000_000, bytes_accessed=2_700_000, transcendentals=0),
        compiler_params=pltpu.CompilerParams(vmem_limit_bytes=30 * 1024 * 1024),
    )(diag_blocks, well_mask)

    msg_y1, msg_y2, ext, ext_cols, edges = pl.pallas_call(
        setup_middle_kernel,
        grid=(1,),
        in_specs=[
            SMEM(), whole(AX_ROWS, L), whole(AX_ROWS, L), whole(6 * R, L), whole(R, L), column,
            whole(4, R, L), whole(NC, R, L),
        ],
        out_specs=[whole(AY_ROWS, L), whole(AY_ROWS, L), whole(6, EX, L), whole(EX, L), whole(4 * NC, L)],
        out_shape=[shape(AY_ROWS, L), shape(AY_ROWS, L), shape(6, EX, L), shape(EX, L), shape(4 * NC, L)],
        compiler_params=pltpu.CompilerParams(vmem_limit_bytes=30 * 1024 * 1024),
    )(par, got_a1, got_a2, own, cols, couple_blocks, transmissibility, pressure_weights)

    got_y1, got_y2 = swap(msg_y1, msg_y2, "gy")

    fields = shape(NC, R, L)
    msg_b1, msg_b2, z_one, partial, product, coeffs, cols_right, cols_left, pressure_part, product_cols = call(
        first_step_kernel,
        [SMEM()] + [VMEM()] * 12,
        [
            shape(BX_ROWS, L), shape(BX_ROWS, L), fields, fields, fields, shape(18, EX, EY),
            shape(EX, L), shape(EX, L), shape(R, L), shape(R, L),
        ],
    )(
        par, got_y1, got_y2, ext, ext_cols, edges, right_side, transmissibility, pressure_weights, well_mask,
        diag_blocks, inverse, couple_blocks,
    )

    got_b1, got_b2 = swap(msg_b1, msg_b2, "gx")
    msg_c1, msg_c2, ext_b, ext_cols_b, rows_b = call(
        between_kernel,
        [SMEM()] + [VMEM()] * 8,
        [shape(EX, L), shape(EX, L), shape(EX, L), shape(EX, L), shape(2 * NC, L)],
    )(par, got_b1, got_b2, pressure_part, product_cols, product, edges, transmissibility, pressure_weights)
    got_c1, got_c2 = swap(msg_c1, msg_c2, "gy")

    msg_x1, msg_x2, msg_z1, msg_z2, z_two, vector, remainder, _ = call(
        second_step_kernel,
        [SMEM()] + [VMEM()] * 16,
        [shape(16, L), shape(16, L), shape(R, L), shape(R, L), fields, fields, fields, fields],
    )(
        par, got_c1, got_c2, ext_b, ext_cols_b, rows_b, ext_cols, cols_right, cols_left, edges, coeffs, partial,
        transmissibility, well_mask, diag_blocks, inverse, couple_blocks,
    )
    got_x1, got_x2 = swap(msg_x1, msg_x2, "gx")
    got_z1, got_z2 = swap(msg_z1, msg_z2, "gy")
    devices = lax.axis_size("gx") * lax.axis_size("gy")
    (local,) = call(dots_kernel, [SMEM()] + [VMEM()] * 8, [shape(devices, L)])(
        par, got_x1, got_x2, got_z1, got_z2, right_side, vector, remainder, transmissibility
    )
    gathered = lax.all_to_all(local, ("gx", "gy"), 0, 0, tiled=True)
    answer, estimate = call(finish_kernel, [VMEM()] * 3, [fields, shape(1, 1)])(gathered, z_one, z_two)
    return (answer, estimate.reshape(()))


def solution(mesh):
    return jax.shard_map(
        on_device,
        mesh=mesh,
        in_specs=(
            P(None, "gx", "gy"),
            P(None, None, "gx", "gy"),
            P(None, None, "gx", "gy"),
            P(None, "gx", "gy"),
            P(None, "gx", "gy"),
            P("gx", "gy"),
        ),
        out_specs=(P(None, "gx", "gy"), P()),
        check_vma=False,
    )
```

```python
import functools

import jax
import jax.numpy as jnp
from jax import lax
from jax.experimental import pallas as pl
from jax.experimental.pallas import tpu as pltpu
from jax.sharding import PartitionSpec as P

NC = 9
COARSE_SWEEPS = 6
RELAX = 0.8
WELL_BOOST = 8.0

R, L = 32, 128
HALO = 32
EX, EY = 3 * R, 2 * L

AX_EDGE = 6 * R
AX_COL = AX_EDGE + 24
AX_ROWS = AX_COL + R
AY_ROWS = 2 * EX
BX_EDGE = R
BX_COL = BX_EDGE + 16
BX_RING = BX_COL + R
BX_ROWS = BX_RING + 112
RING_EFF, RING_NEXT, RING_TRANS, RING_VECTOR, RING_STATIC = 81, 90, 99, 103, 104

CENTER, EAST, WEST, NORTH, SOUTH, SCALE = range(6)


def iotas(shape):
    return (lax.broadcasted_iota(jnp.int32, shape, 0), lax.broadcasted_iota(jnp.int32, shape, 1))


def shifted(values, axis, step):
    return pltpu.roll(values, (-step) % values.shape[axis], axis)


def lane_roll(values, shift):
    shift = shift % values.shape[1]
    return values if shift == 0 else pltpu.roll(values, shift, 1)


def even_mask(par_ref, which, shape):
    return jnp.full(shape, par_ref[which], jnp.int32) == 0


def put(par_ref, which, first, second, rows, up, down):
    even = even_mask(par_ref, which, up.shape)
    first[rows, :] = jnp.where(even, up, down)
    second[rows, :] = jnp.where(even, down, up)


def take(par_ref, which, first, second, rows):
    one, two = (first[rows, :], second[rows, :])
    even = even_mask(par_ref, which, one.shape)
    return (jnp.where(even, one, two), jnp.where(even, two, one))


def pack_columns(parts):
    shape = parts[0][0].shape
    lanes = iotas(shape)[1]
    packed = jnp.zeros(shape, jnp.float32)
    for values, lane, target in parts:
        packed = jnp.where(lanes == target, lane_roll(values, target - lane), packed)
    return packed


def setup_kernel(
    par, rhs_hbm, diag_hbm, couple_hbm, trans_hbm, weights_hbm, wells_hbm, msg1, msg2, own, cols,
    rhs, diag0, couple0, trans, weights, wells, sems,
):
    pairs = (
        (weights_hbm, weights),
        (couple_hbm.at[:, 0:1], couple0),
        (diag_hbm.at[:, 0:1], diag0),
        (trans_hbm, trans),
        (rhs_hbm, rhs),
        (wells_hbm, wells),
    )
    copies = [pltpu.make_async_copy(a, b, sems.at[i]) for i, (a, b) in enumerate(pairs)]
    for copy in copies:
        copy.start()
    for copy in copies:
        copy.wait()
    rows, lanes = iotas((R, L))
    center = WELL_BOOST * wells[...].astype(jnp.float32) * weights[0]
    pressure = jnp.zeros((R, L), jnp.float32)
    links = [jnp.zeros((R, L), jnp.float32) for _ in range(4)]
    for c in range(NC):
        w, col = (weights[c], couple0[c, 0])
        center = center + w * diag0[c, 0]
        pressure = pressure + w * rhs[c]
        for d, (axis, step) in enumerate(((0, 1), (0, -1), (1, 1), (1, -1))):
            links[d] = links[d] + w * shifted(col, axis, step)
    inside = (rows != R - 1, rows != 0, lanes != L - 1, lanes != 0)
    fields = [center]
    for d in range(4):
        fields.append(jnp.where(inside[d], -trans[d] * links[d], 0.0))
    fields.append(pressure)
    for k, field in enumerate(fields):
        span = pl.ds(k * R, R)
        own[span, :] = field
        msg1[span, :] = field
        msg2[span, :] = field
    t_up, t_down = (trans[0, R - 1 : R, :], trans[1, 0:1, :])
    t_right, t_left = (trans[2], trans[3])
    for c in range(NC):
        put(par, 0, msg1, msg2, pl.ds(AX_EDGE + c, 1), couple0[c, 0, R - 1 : R, :], couple0[c, 0, 0:1, :])
        put(par, 0, msg1, msg2, pl.ds(AX_EDGE + NC + c, 1), t_up * weights[c, R - 1 : R, :], t_down * weights[c, 0:1, :])
    blank = jnp.zeros((24 - 2 * NC, L), jnp.float32)
    msg1[pl.ds(AX_EDGE + 2 * NC, 24 - 2 * NC), :] = blank
    msg2[pl.ds(AX_EDGE + 2 * NC, 24 - 2 * NC), :] = blank
    parts = []
    for c in range(NC):
        col, w = (couple0[c, 0], weights[c])
        parts += [(col, 0, c), (t_left * w, 0, NC + c), (col, L - 1, 2 * NC + c), (t_right * w, L - 1, 3 * NC + c)]
    packed = pack_columns(parts)
    cols[...] = packed
    msg1[pl.ds(AX_COL, R), :] = packed
    msg2[pl.ds(AX_COL, R), :] = packed


def inverse_kernel(diag, couple, trans, wells, out, pack_left, pack_right, rows_up, rows_down):
    boost = WELL_BOOST * wells[...].astype(jnp.float32)
    a = [[diag[i, j] + boost if i == j else diag[i, j] for j in range(NC)] for i in range(NC)]
    for k in range(NC):
        inv = 1.0 / a[k][k]
        a[k] = [inv if j == k else a[k][j] * inv for j in range(NC)]
        for i in range(NC):
            if i != k:
                factor = a[i][k]
                a[i] = [-factor * inv if j == k else a[i][j] - factor * a[k][j] for j in range(NC)]
    for i in range(NC):
        for j in range(NC):
            out[i, j] = a[i][j]
    entries = []
    for k in range(NC):
        for c in range(NC):
            total = couple[c, 0] * a[0][k]
            for m in range(1, NC):
                total = total + couple[c, m] * a[m][k]
            entries.append((total, 0, NC * k + c))
    for c in range(NC):
        entries.append((diag[c, 0] + boost if c == 0 else diag[c, 0], 0, RING_EFF + c))
        entries.append((couple[c, 0], 1, RING_NEXT + c))
    for d in range(4):
        entries.append((trans[d], 0, RING_TRANS + d))
    pack_left[...] = pack_columns([(v, inward, place) for v, inward, place in entries])
    pack_right[...] = pack_columns([(v, L - 1 - inward, place) for v, inward, place in entries])
    zero = jnp.zeros((1, L), jnp.float32)

    @pl.when(pl.program_id(0) == 0)
    def _():
        rows_down[pl.ds(RING_STATIC - 1, 1), :] = zero
        for v, inward, place in entries:
            rows_down[pl.ds(place, 1), :] = v[inward : inward + 1, :]

    @pl.when(pl.program_id(0) == R // 8 - 1)
    def _():
        rows_up[pl.ds(RING_STATIC - 1, 1), :] = zero
        for v, inward, place in entries:
            rows_up[pl.ds(place, 1), :] = v[7 - inward : 8 - inward, :]


def setup_middle_kernel(par, got1, got2, own, cols, couple0, trans, weights, msg1, msg2, ext, ext_cols, edges):
    rows, lanes = iotas((EX, L))

    def dots(span_of):
        total = jnp.zeros((1, L), jnp.float32)
        for c in range(NC):
            total = total + span_of(c)
        return -total

    ups, downs, tw_ups, tw_downs = ([], [], [], [])
    for c in range(NC):
        up, down = take(par, 0, got1, got2, pl.ds(AX_EDGE + c, 1))
        ups.append(up)
        downs.append(down)
        up, down = take(par, 0, got1, got2, pl.ds(AX_EDGE + NC + c, 1))
        tw_ups.append(up)
        tw_downs.append(down)
        edges[pl.ds(c, 1), :] = ups[c]
        edges[pl.ds(NC + c, 1), :] = downs[c]
        edges[pl.ds(2 * NC + c, 1), :] = tw_ups[c]
        edges[pl.ds(3 * NC + c, 1), :] = tw_downs[c]
    t_up, t_down = (trans[0, R - 1 : R, :], trans[1, 0:1, :])
    east_own = dots(lambda c: t_up * weights[c, R - 1 : R, :] * ups[c])
    west_own = dots(lambda c: t_down * weights[c, 0:1, :] * downs[c])
    west_up = dots(lambda c: tw_ups[c] * couple0[c, 0, R - 1 : R, :])
    east_down = dots(lambda c: tw_downs[c] * couple0[c, 0, 0:1, :])
    fields = []
    for k in range(6):
        up, down = take(par, 0, got1, got2, pl.ds(k * R, R))
        field = jnp.concatenate([own[pl.ds(k * R, R), :], up, down], axis=0)
        if k == CENTER:
            field = jnp.where(field == 0.0, 1.0, field)
        if k == EAST:
            field = jnp.where(rows == R - 1, east_own, jnp.where(rows == EX - 1, east_down, field))
        if k == WEST:
            field = jnp.where(rows == 0, west_own, jnp.where(rows == R, west_up, field))
        ext[k] = field
        fields.append(field)
    up, down = take(par, 0, got1, got2, pl.ds(AX_COL, R))
    packed = jnp.concatenate([cols[...], up, down], axis=0)
    ext_cols[...] = packed
    to_right = [lane_roll(f, HALO * (k % 4) + HALO) for k, f in enumerate(fields)]
    to_left = [lane_roll(f, HALO * (k % 4)) for k, f in enumerate(fields)]
    group = lanes // HALO

    def quad(parts):
        result = parts[-1]
        for g in range(len(parts) - 2, -1, -1):
            result = jnp.where(group == g, parts[g], result)
        return result

    put(par, 1, msg1, msg2, pl.ds(0, EX), quad(to_right[:4]), quad(to_left[:4]))
    put(
        par,
        1,
        msg1,
        msg2,
        pl.ds(EX, EX),
        quad(to_right[4:] + [lane_roll(packed, 64 - 2 * NC)]),
        quad(to_left[4:] + [lane_roll(packed, 64)]),
    )


def lane_sum(product, start):
    lanes = iotas(product.shape)[1]
    keep = jnp.logical_and(lanes >= start, lanes < start + NC)
    return jnp.sum(jnp.where(keep, product, 0.0), axis=1, keepdims=True)


def pair_sums(values, step):
    rows, lanes = iotas(values.shape)
    values = values + jnp.where((rows // step) % 2 == 0, shifted(values, 0, step), shifted(values, 0, -step))
    return values + jnp.where((lanes // step) % 2 == 0, shifted(values, 1, step), shifted(values, 1, -step))


def coarsen_into(coeffs, level):
    step = 2**level
    base, out = (6 * level, 6 * level + 6)
    rows, lanes = iotas((EX, EY))
    row_even = (rows // step) % 2 == 0
    lane_even = (lanes // step) % 2 == 0
    east, west, north, south = (coeffs[base + d] for d in (EAST, WEST, NORTH, SOUTH))
    center = coeffs[base] + (jnp.where(row_even, east, west) + jnp.where(lane_even, north, south))
    center = pair_sums(center, step)
    coeffs[out + CENTER] = center
    coeffs[out + SCALE] = RELAX / center
    coeffs[out + EAST] = pair_sums(jnp.where(row_even, 0.0, east), step)
    coeffs[out + WEST] = pair_sums(jnp.where(row_even, west, 0.0), step)
    coeffs[out + NORTH] = pair_sums(jnp.where(lane_even, 0.0, north), step)
    coeffs[out + SOUTH] = pair_sums(jnp.where(lane_even, south, 0.0), step)


def level_apply(values, coeffs, level):
    step = 2**level
    base = 6 * level
    return coeffs[base + CENTER] * values + (
        coeffs[base + EAST] * shifted(values, 0, step)
        + coeffs[base + WEST] * shifted(values, 0, -step)
        + coeffs[base + NORTH] * shifted(values, 1, step)
        + coeffs[base + SOUTH] * shifted(values, 1, -step)
    )


def sweep(values, source, coeffs, level):
    return values + coeffs[6 * level + SCALE] * (source - level_apply(values, coeffs, level))


def vcycle(source, coeffs):
    values0 = coeffs[SCALE] * source
    source1 = pair_sums(source - level_apply(values0, coeffs, 0), 1)
    values1 = coeffs[6 + SCALE] * source1
    source2 = pair_sums(source1 - level_apply(values1, coeffs, 1), 2)
    values2 = coeffs[12 + SCALE] * source2
    for _ in range(COARSE_SWEEPS - 1):
        values2 = sweep(values2, source2, coeffs, 2)
    values1 = sweep(values1 + values2, source1, coeffs, 1)
    return sweep(values0 + values1, source, coeffs, 0)


def ghost_column(packed, start, to_lane, lane):
    return lane_roll(packed, to_lane - (start + lane))


def neighbour_sum(values, trans, up_row, down_row, right_col, left_col):
    rows, lanes = iotas((R, L))
    east = jnp.where(rows == R - 1, up_row, shifted(values, 0, 1))
    west = jnp.where(rows == 0, down_row, shifted(values, 0, -1))
    north = jnp.where(lanes == L - 1, right_col, shifted(values, 1, 1))
    south = jnp.where(lanes == 0, left_col, shifted(values, 1, -1))
    return trans[0] * east + trans[1] * west + trans[2] * north + trans[3] * south


def ghost_rows(trans, up_row, down_row):
    rows, _ = iotas((R, L))
    return jnp.where(rows == R - 1, trans[0] * up_row, 0.0) + jnp.where(rows == 0, trans[1] * down_row, 0.0)


def ghost_columns(trans, right_col, left_col):
    _, lanes = iotas((R, L))
    return jnp.where(lanes == L - 1, trans[2] * right_col, 0.0) + jnp.where(lanes == 0, trans[3] * left_col, 0.0)


def one_step(pressure, vector, edges, col_right, col_left, diag, inverse, couple, trans, boost, z_out):
    p = pressure[0:R, 0:L]
    up_row, down_row = (pressure[R : R + 1, 0:L], pressure[EX - 1 : EX, 0:L])
    far = pressure[0:R, L:EY]
    right_p, left_p = (lane_roll(far, L - 1), lane_roll(far, 1))
    second = []
    for c in range(NC):
        own = diag[c, 0] * p
        if c == 0:
            own = own + boost * p
        around = neighbour_sum(
            couple[c, 0] * p,
            trans,
            edges[pl.ds(c, 1), :] * up_row,
            edges[pl.ds(NC + c, 1), :] * down_row,
            ghost_column(col_right, 64, L - 1, c) * right_p,
            ghost_column(col_left, 64, 0, c) * left_p,
        )
        second.append(vector[c] - (own - around))
    rest = []
    for c in range(NC):
        total = inverse[c, 0] * second[0]
        for k in range(1, NC):
            total = total + inverse[c, k] * second[k]
        rest.append(total)
        z_out[c] = total + p if c == 0 else total
    products = []
    for c in range(NC):
        product = couple[c, 0] * rest[0]
        for k in range(1, NC):
            product = product + couple[c, k] * rest[k]
        products.append(product)
    return products


def first_step_kernel(
    par, got1, got2, ext, ext_cols, edges, rhs, trans, weights, wells, diag, inverse, couple, rows_up, rows_down,
    msg1, msg2, z_out, partial, product, coeffs, cols_right, cols_left, pressure_part, product_cols,
):
    rows, lanes = iotas((EX, L))
    right, left = take(par, 1, got1, got2, pl.ds(EX, EX))
    cols_right[...] = right
    cols_left[...] = left
    packed = ext_cols[...]
    north_own = -lane_sum(lane_roll(packed, 64 - 3 * NC) * right, 64)
    south_right = -lane_sum(lane_roll(packed, 64 - NC) * right, 64 + NC)
    south_own = -lane_sum(lane_roll(packed, 64 - NC) * left, 64)
    north_left = -lane_sum(lane_roll(packed, 64 + NC) * left, 64 + NC)
    right_four, left_four = take(par, 1, got1, got2, pl.ds(0, EX))
    source = None
    for k in range(6):
        from_right = lane_roll(right_four if k < 4 else right, -HALO * (k % 4))
        from_left = lane_roll(left_four if k < 4 else left, L - HALO - HALO * (k % 4))
        near = ext[k]
        far = jnp.where(lanes < HALO, from_right, jnp.where(lanes >= L - HALO, from_left, 0.0))
        if k == CENTER:
            far = jnp.where(far == 0.0, 1.0, far)
        if k == NORTH:
            near = jnp.where(lanes == L - 1, north_own, near)
            far = jnp.where(lanes == L - 1, north_left, far)
        if k == SOUTH:
            near = jnp.where(lanes == 0, south_own, near)
            far = jnp.where(lanes == 0, south_right, far)
        field = jnp.concatenate([near, far], axis=1)
        if k == 5:
            source = field
        else:
            coeffs[k] = field
    coeffs[SCALE] = RELAX / coeffs[CENTER]
    coarsen_into(coeffs, 0)
    coarsen_into(coeffs, 1)
    pressure = vcycle(source, coeffs)
    boost = WELL_BOOST * wells[...].astype(jnp.float32)
    vector = [rhs[c] for c in range(NC)]
    products = one_step(
        pressure, vector, edges, right[0:R], left[0:R], diag, inverse, couple, trans, boost, z_out
    )
    put(par, 0, msg1, msg2, pl.ds(BX_RING, RING_STATIC), rows_up[...], rows_down[...])
    weighed = jnp.zeros((R, L), jnp.float32)
    zero = jnp.zeros((1, L), jnp.float32)
    parts = []
    for c in range(NC):
        product[c] = products[c]
        value = -neighbour_sum(products[c], trans, zero, zero, 0.0, 0.0)
        partial[c] = value
        weighed = weighed + weights[c] * value
        last, first = (slice(R - 1, R), slice(0, 1))
        put(par, 0, msg1, msg2, pl.ds(BX_EDGE + c, 1), products[c][last], products[c][first])
        put(par, 0, msg1, msg2, pl.ds(BX_RING + RING_VECTOR + c, 1), value[last], value[first])
        parts += [(products[c], 0, c), (products[c], L - 1, NC + c)]
    blank = jnp.zeros((16 - NC, L), jnp.float32)
    columns = pack_columns(parts)
    pressure_part[...] = weighed
    product_cols[...] = columns
    for msg in (msg1, msg2):
        msg[pl.ds(0, R), :] = weighed
        msg[pl.ds(BX_EDGE + NC, 16 - NC), :] = blank
        msg[pl.ds(BX_COL, R), :] = columns


def between_kernel(
    par, got1, got2, pressure_part, product_cols, product, edges, trans, weights, partial, pack_left, pack_right,
    msg1, msg2, ext, ext_cols, rows_out, vector_out,
):
    rows, lanes = iotas((EX, L))
    t_up, t_down = (trans[0, R - 1 : R, :], trans[1, 0:1, :])
    own_up, own_down, far_up, far_down = (jnp.zeros((1, L), jnp.float32) for _ in range(4))
    to_right, to_left = ([], [])
    for c in range(NC):
        up, down = take(par, 0, got1, got2, pl.ds(BX_EDGE + c, 1))
        rows_out[pl.ds(c, 1), :] = up
        rows_out[pl.ds(NC + c, 1), :] = down
        own_up = own_up + t_up * weights[c, R - 1 : R, :] * up
        own_down = own_down + t_down * weights[c, 0:1, :] * down
        far_up = far_up + edges[pl.ds(2 * NC + c, 1), :] * product[c, R - 1 : R, :]
        far_down = far_down + edges[pl.ds(3 * NC + c, 1), :] * product[c, 0:1, :]
        value = partial[c] - ghost_rows(trans, up, down)
        vector_out[c] = value
        to_right.append((value, L - 1, RING_VECTOR + c))
        to_left.append((value, 0, RING_VECTOR + c))
    up, down = take(par, 0, got1, got2, pl.ds(0, R))
    field = jnp.concatenate([pressure_part[...], up, down], axis=0)
    edge = jnp.where(rows == R - 1, own_up, 0.0) + jnp.where(rows == 0, own_down, 0.0)
    edge = edge + jnp.where(rows == R, far_up, 0.0) + jnp.where(rows == EX - 1, far_down, 0.0)
    field = field - edge
    ext[...] = field
    up, down = take(par, 0, got1, got2, pl.ds(BX_COL, R))
    packed = jnp.concatenate([product_cols[...], up, down], axis=0)
    ext_cols[...] = packed
    near = lanes < HALO
    put(
        par, 1, msg1, msg2, pl.ds(0, EX),
        jnp.where(near, lane_roll(field, HALO), lane_roll(packed, HALO - NC)),
        jnp.where(near, field, lane_roll(packed, HALO)),
    )
    fixed = iotas((R, L))[1] < RING_VECTOR
    put(
        par, 1, msg1, msg2, pl.ds(EX, R),
        jnp.where(fixed, pack_right[...], pack_columns(to_right)),
        jnp.where(fixed, pack_left[...], pack_columns(to_left)),
    )


def row_ring(ring, outward, inward, pressure, row, out_row, own_row, edge_cols, product_row, couple_row, corners, old_corners):
    lanes = iotas((1, L))[1]
    line = pressure[row : row + 1, :]
    p = line[:, 0:L]
    p_right, p_left = (line[:, L : L + 1], line[:, EY - 1 : EY])
    p_out, p_own = (pressure[out_row : out_row + 1, 0:L], pressure[own_row : own_row + 1, 0:L])
    t_out, t_in = (ring(RING_TRANS + outward), ring(RING_TRANS + inward))
    t_right, t_left = (ring(RING_TRANS + 2), ring(RING_TRANS + 3))
    second = []
    for c in range(NC):
        beside = edge_cols(c) * p
        old_right, old_left = (ghost_column(old_corners[0], 64, L - 1, c), ghost_column(old_corners[1], 64, 0, c))
        new_right, new_left = (ghost_column(corners[0], HALO, L - 1, c), ghost_column(corners[1], HALO, 0, c))
        north = jnp.where(lanes == L - 1, old_right * p_right, shifted(beside, 1, 1))
        south = jnp.where(lanes == 0, old_left * p_left, shifted(beside, 1, -1))
        value = ring(RING_VECTOR + c) - t_in * product_row(c)
        value = value - jnp.where(lanes == L - 1, t_right * new_right, 0.0)
        value = value - jnp.where(lanes == 0, t_left * new_left, 0.0)
        second.append(
            value
            - ring(RING_EFF + c) * p
            + t_out * (ring(RING_NEXT + c) * p_out)
            + t_in * (couple_row(c) * p_own)
            + t_right * north
            + t_left * south
        )
    return second


def column_ring(pack, outward, inward, p, p_out, p_own, p_up, p_down, own_couple, own_product, beside_up, beside_down):
    lanes = iotas((R, L))[1]

    def trans(d):
        return pack[:, RING_TRANS + d : RING_TRANS + d + 1]

    second = (
        lane_roll(pack, -RING_VECTOR)
        - trans(inward) * own_product
        - lane_roll(pack, -RING_EFF) * p
        + trans(outward) * (lane_roll(pack, -RING_NEXT) * p_out)
        + trans(inward) * (own_couple * p_own)
        + trans(0) * (beside_up * p_up)
        + trans(1) * (beside_down * p_down)
    )
    spread = jnp.zeros((R, L), jnp.float32)
    for k in range(NC):
        within = jnp.logical_and(lanes >= NC * k, lanes < NC * k + NC)
        spread = jnp.where(within, second[:, k : k + 1], spread)
    terms = pack * spread
    total = terms
    for k in range(1, NC):
        total = total + lane_roll(terms, -NC * k)
    return total


def second_step_kernel(
    par, got1, got2, gotx1, gotx2, ext, ext_cols, rows_in, setup_cols, cols_right, cols_left, edges, coeffs, partial,
    product, rhs, trans, wells, diag, inverse, couple,
    z_out, dots, ring_up, ring_down,
):
    rows, lanes = iotas((EX, L))
    right, left = take(par, 1, got1, got2, pl.ds(0, EX))
    packed, tw = (ext_cols[...], setup_cols[...])
    old_right, old_left = (cols_right[...], cols_left[...])
    own_right = lane_sum(lane_roll(tw, HALO - 3 * NC) * right, HALO)
    own_left = lane_sum(lane_roll(tw, HALO - NC) * left, HALO)
    far_right = lane_sum(old_right * lane_roll(packed, 64), 64 + NC)
    far_left = lane_sum(old_left * lane_roll(packed, 64 + NC), 64 + NC)
    near = ext[...] - jnp.where(lanes == L - 1, own_right, 0.0) - jnp.where(lanes == 0, own_left, 0.0)
    far = jnp.where(
        lanes < HALO, right, jnp.where(lanes >= L - HALO, lane_roll(left, L - HALO), 0.0)
    )
    far = far - jnp.where(lanes == 0, far_right, 0.0) - jnp.where(lanes == L - 1, far_left, 0.0)
    pressure = vcycle(jnp.concatenate([near, far], axis=1), coeffs)
    vector = []
    for c in range(NC):
        columns = ghost_columns(
            trans, ghost_column(right[0:R], HALO, L - 1, c), ghost_column(left[0:R], HALO, 0, c)
        )
        vector.append(partial[c] - columns)
    boost = WELL_BOOST * wells[...].astype(jnp.float32)
    products = one_step(
        pressure, vector, edges, old_right[0:R], old_left[0:R], diag, inverse, couple, trans, boost, z_out
    )
    up, down = take(par, 0, gotx1, gotx2, pl.ds(BX_RING, 112))
    ring_up[...] = up
    ring_down[...] = down
    second_up = row_ring(
        lambda i: ring_up[pl.ds(i, 1), :], 0, 1, pressure, R, R + 1, R - 1,
        lambda c: edges[pl.ds(c, 1), :], lambda c: product[c, R - 1 : R, :], lambda c: couple[c, 0, R - 1 : R, :],
        (right[R : R + 1], left[R : R + 1]), (old_right[R : R + 1], old_left[R : R + 1]),
    )
    second_down = row_ring(
        lambda i: ring_down[pl.ds(i, 1), :], 1, 0, pressure, EX - 1, EX - 2, 0,
        lambda c: edges[pl.ds(NC + c, 1), :], lambda c: product[c, 0:1, :], lambda c: couple[c, 0, 0:1, :],
        (right[EX - 1 : EX], left[EX - 1 : EX]), (old_right[EX - 1 : EX], old_left[EX - 1 : EX]),
    )
    product_up = ring_up[pl.ds(0, NC), :] * second_up[0]
    product_down = ring_down[pl.ds(0, NC), :] * second_down[0]
    for k in range(1, NC):
        product_up = product_up + ring_up[pl.ds(NC * k, NC), :] * second_up[k]
        product_down = product_down + ring_down[pl.ds(NC * k, NC), :] * second_down[k]
    pack_right, pack_left = take(par, 1, got1, got2, pl.ds(EX, R))
    far_p = pressure[:, L:EY]
    far_up, far_down = (shifted(far_p, 0, 1)[0:R], shifted(far_p, 0, -1)[0:R])
    far_p, near_p = (far_p[0:R], pressure[0:R, 0:L])
    right_cols = column_ring(
        pack_right, 2, 3, far_p[:, 0:1], far_p[:, 1:2], near_p[:, L - 1 : L], far_up[:, 0:1], far_down[:, 0:1],
        lane_roll(tw[0:R], -2 * NC), lane_roll(packed[0:R], -NC),
        lane_roll(shifted(old_right, 0, 1)[0:R], -64), lane_roll(shifted(old_right, 0, -1)[0:R], -64),
    )
    left_cols = column_ring(
        pack_left, 3, 2, far_p[:, L - 1 : L], far_p[:, L - 2 : L - 1], near_p[:, 0:1], far_up[:, L - 1 : L],
        far_down[:, L - 1 : L], tw[0:R], packed[0:R],
        lane_roll(shifted(old_left, 0, 1)[0:R], -64), lane_roll(shifted(old_left, 0, -1)[0:R], -64),
    )
    sums = [jnp.zeros((R, L), jnp.float32) for _ in range(6)]
    for c in range(NC):
        two = -neighbour_sum(
            products[c], trans, product_up[c : c + 1], product_down[c : c + 1],
            ghost_column(right_cols, 0, L - 1, c), ghost_column(left_cols, 0, 0, c),
        )
        zero, one = (rhs[c], vector[c])
        for k, (a, b) in enumerate(((zero, zero), (zero, one), (one, one), (zero, two), (one, two), (two, two))):
            sums[k] = sums[k] + a * b
    lane = iotas((1, L))[1]
    row = jnp.zeros((1, L), jnp.float32)
    for k, total in enumerate(sums):
        row = jnp.where(lane == k, jnp.sum(total, keepdims=True), row)
    dots[...] = jnp.broadcast_to(row, dots.shape)


def finish_kernel(gathered, z_one, z_two, out, estimate):
    row = jnp.sum(gathered[...], axis=0, keepdims=True)
    lanes = iotas((1, L))[1]
    g00, g01, g11, g02, g12, g22 = (
        jnp.sum(jnp.where(lanes == k, row, 0.0), axis=1, keepdims=True) for k in range(6)
    )
    beta = jnp.sqrt(g00)
    shift = g01 / g00
    h00 = 1.0 + shift
    length2 = g11 - shift * g01
    length = jnp.sqrt(length2)
    h10 = length / beta
    h01 = (g02 - shift * g01) / (beta * length)
    above = (g12 - shift * g02 - shift * (g11 - shift * g01)) / length2
    h11 = 1.0 + above
    h21 = jnp.sqrt((g22 - 2.0 * shift * g12 + shift * shift * g11) / length2 - h01 * h01 - above * above)
    radius0 = jnp.sqrt(h00 * h00 + h10 * h10)
    cos0, sin0 = (h00 / radius0, h10 / radius0)
    r01 = cos0 * h01 + sin0 * h11
    mid = cos0 * h11 - sin0 * h01
    radius1 = jnp.sqrt(mid * mid + h21 * h21)
    cos1, sin1 = (mid / radius1, h21 / radius1)
    rhs0, rhs1 = (cos0 * beta, -sin0 * beta)
    estimate[...] = jnp.abs(sin1 * rhs1)
    y1 = cos1 * rhs1 / radius1
    y0 = (rhs0 - r01 * y1) / radius0
    weight1 = y1 / length
    weight0 = y0 / beta - weight1 * shift
    for c in range(NC):
        out[c] = weight0 * z_one[c] + weight1 * z_two[c]


VMEM = functools.partial(pl.BlockSpec, memory_space=pltpu.VMEM)
SMEM = functools.partial(pl.BlockSpec, memory_space=pltpu.SMEM)
HBM = functools.partial(pl.BlockSpec, memory_space=pltpu.HBM)


def shape(*dims):
    return jax.ShapeDtypeStruct(dims, jnp.float32)


def call(kernel, in_specs, outs, scratch=(), cost=20_000_000):
    return pl.pallas_call(
        kernel,
        in_specs=list(in_specs),
        out_specs=[VMEM()] * len(outs),
        out_shape=list(outs),
        scratch_shapes=list(scratch),
        cost_estimate=pl.CostEstimate(flops=cost, bytes_accessed=1_000_000, transcendentals=0),
        compiler_params=pltpu.CompilerParams(vmem_limit_bytes=30 * 1024 * 1024),
    )


def swap(first, second, axis):
    peers = lax.axis_size(axis)
    pairs = [(i, i ^ 1) for i in range(peers) if i ^ 1 < peers]
    others = [(i, ((i + 1) ^ 1) - 1) for i in range(1, peers) if ((i + 1) ^ 1) - 1 < peers]
    return (lax.ppermute(first, axis, pairs), lax.ppermute(second, axis, others))


def on_device(right_side, diag_blocks, couple_blocks, transmissibility, pressure_weights, well_mask):
    par = jnp.stack([lax.axis_index("gx") & 1, lax.axis_index("gy") & 1]).astype(jnp.int32)
    column = pl.BlockSpec((NC, 1, R, L), lambda i: (0, 0, 0, 0))

    def whole(*dims):
        return pl.BlockSpec(dims, lambda i: (0,) * len(dims))

    msg_a1, msg_a2, own, cols = call(
        setup_kernel,
        [SMEM()] + [HBM()] * 6,
        [shape(AX_ROWS, L), shape(AX_ROWS, L), shape(6 * R, L), shape(R, L)],
        [
            pltpu.VMEM((NC, R, L), jnp.float32),
            pltpu.VMEM((NC, 1, R, L), jnp.float32),
            pltpu.VMEM((NC, 1, R, L), jnp.float32),
            pltpu.VMEM((4, R, L), jnp.float32),
            pltpu.VMEM((NC, R, L), jnp.float32),
            pltpu.VMEM((R, L), jnp.int32),
            pltpu.SemaphoreType.DMA((6,)),
        ],
    )(
        par,
        *(
            pltpu.with_memory_space_constraint(x, pltpu.HBM)
            for x in (right_side, diag_blocks, couple_blocks, transmissibility, pressure_weights, well_mask)
        ),
    )

    got_a1, got_a2 = swap(msg_a1, msg_a2, "gx")

    slab = pl.BlockSpec((NC, NC, 8, L), lambda i: (0, 0, i, 0))
    strip = pl.BlockSpec((8, L), lambda i: (i, 0))
    inverse, pack_left, pack_right, rows_up, rows_down = pl.pallas_call(
        inverse_kernel,
        grid=(R // 8,),
        in_specs=[slab, slab, pl.BlockSpec((4, 8, L), lambda i: (0, i, 0)), strip],
        out_specs=[slab, strip, strip, whole(RING_STATIC, L), whole(RING_STATIC, L)],
        out_shape=[shape(NC, NC, R, L), shape(R, L), shape(R, L), shape(RING_STATIC, L), shape(RING_STATIC, L)],
        cost_estimate=pl.CostEstimate(flops=20_000_000, bytes_accessed=2_700_000, transcendentals=0),
        compiler_params=pltpu.CompilerParams(vmem_limit_bytes=30 * 1024 * 1024),
    )(diag_blocks, couple_blocks, transmissibility, well_mask)

    msg_y1, msg_y2, ext, ext_cols, edges = pl.pallas_call(
        setup_middle_kernel,
        grid=(1,),
        in_specs=[
            SMEM(), whole(AX_ROWS, L), whole(AX_ROWS, L), whole(6 * R, L), whole(R, L), column,
            whole(4, R, L), whole(NC, R, L),
        ],
        out_specs=[whole(AY_ROWS, L), whole(AY_ROWS, L), whole(6, EX, L), whole(EX, L), whole(4 * NC, L)],
        out_shape=[shape(AY_ROWS, L), shape(AY_ROWS, L), shape(6, EX, L), shape(EX, L), shape(4 * NC, L)],
        compiler_params=pltpu.CompilerParams(vmem_limit_bytes=30 * 1024 * 1024),
    )(par, got_a1, got_a2, own, cols, couple_blocks, transmissibility, pressure_weights)

    got_y1, got_y2 = swap(msg_y1, msg_y2, "gy")

    fields = shape(NC, R, L)
    msg_b1, msg_b2, z_one, partial, product, coeffs, cols_right, cols_left, pressure_part, product_cols = call(
        first_step_kernel,
        [SMEM()] + [VMEM()] * 14,
        [
            shape(BX_ROWS, L), shape(BX_ROWS, L), fields, fields, fields, shape(18, EX, EY),
            shape(EX, L), shape(EX, L), shape(R, L), shape(R, L),
        ],
    )(
        par, got_y1, got_y2, ext, ext_cols, edges, right_side, transmissibility, pressure_weights, well_mask,
        diag_blocks, inverse, couple_blocks, rows_up, rows_down,
    )

    got_b1, got_b2 = swap(msg_b1, msg_b2, "gx")
    msg_c1, msg_c2, ext_b, ext_cols_b, rows_b, vector_b = call(
        between_kernel,
        [SMEM()] + [VMEM()] * 11,
        [shape(EX + R, L), shape(EX + R, L), shape(EX, L), shape(EX, L), shape(2 * NC, L), fields],
    )(
        par, got_b1, got_b2, pressure_part, product_cols, product, edges, transmissibility, pressure_weights,
        partial, pack_left, pack_right,
    )
    got_c1, got_c2 = swap(msg_c1, msg_c2, "gy")

    devices = lax.axis_size("gx") * lax.axis_size("gy")
    z_two, local = call(
        second_step_kernel,
        [SMEM()] + [VMEM()] * 20,
        [fields, shape(devices, L)],
        [pltpu.VMEM((112, L), jnp.float32), pltpu.VMEM((112, L), jnp.float32)],
    )(
        par, got_c1, got_c2, got_b1, got_b2, ext_b, ext_cols_b, rows_b, ext_cols, cols_right, cols_left, edges, coeffs,
        vector_b, product, right_side, transmissibility, well_mask, diag_blocks, inverse, couple_blocks,
    )
    gathered = lax.all_to_all(local, ("gx", "gy"), 0, 0, tiled=True)
    answer, estimate = call(finish_kernel, [VMEM()] * 3, [fields, shape(1, 1)])(gathered, z_one, z_two)
    return (answer, estimate.reshape(()))


def solution(mesh):
    return jax.shard_map(
        on_device,
        mesh=mesh,
        in_specs=(
            P(None, "gx", "gy"),
            P(None, None, "gx", "gy"),
            P(None, None, "gx", "gy"),
            P(None, "gx", "gy"),
            P(None, "gx", "gy"),
            P("gx", "gy"),
        ),
        out_specs=(P(None, "gx", "gy"), P()),
        check_vma=False,
    )
```

```python
import functools

import jax
import jax.numpy as jnp
from jax import lax
from jax.experimental import pallas as pl
from jax.experimental.pallas import tpu as pltpu
from jax.sharding import PartitionSpec as P

NC = 9
COARSE_SWEEPS = 6
RELAX = 0.8
WELL_BOOST = 8.0

R, L = 32, 128
HALO = 32
EX, EY = 3 * R, 2 * L

AX_EDGE = 6 * R
AX_COL = AX_EDGE + 24
AX_ROWS = AX_COL + R
AY_ROWS = 2 * EX
BX_EDGE = R
BX_COL = BX_EDGE + 16
BX_RING = BX_COL + R
BX_ROWS = BX_RING + 112
RING_EFF, RING_NEXT, RING_TRANS, RING_VECTOR, RING_STATIC = 81, 90, 99, 103, 104

CENTER, EAST, WEST, NORTH, SOUTH, SCALE = range(6)


def iotas(shape):
    return (lax.broadcasted_iota(jnp.int32, shape, 0), lax.broadcasted_iota(jnp.int32, shape, 1))


def shifted(values, axis, step):
    return pltpu.roll(values, (-step) % values.shape[axis], axis)


def lane_roll(values, shift):
    shift = shift % values.shape[1]
    return values if shift == 0 else pltpu.roll(values, shift, 1)


def first_is_up(par_ref, which, shape):
    return jnp.broadcast_to(par_ref[which : which + 1, :], shape) == 0


def put(par_ref, which, first, second, rows, up, down):
    mask = first_is_up(par_ref, which, up.shape)
    first[rows, :] = jnp.where(mask, up, down)
    second[rows, :] = jnp.where(mask, down, up)


def take(par_ref, which, first, second, rows):
    one, two = (first[rows, :], second[rows, :])
    mask = first_is_up(par_ref, which, one.shape)
    return (jnp.where(mask, one, two), jnp.where(mask, two, one))


def pack_columns(parts):
    shape = parts[0][0].shape
    lanes = iotas(shape)[1]
    packed = jnp.zeros(shape, jnp.float32)
    for values, lane, target in parts:
        packed = jnp.where(lanes == target, lane_roll(values, target - lane), packed)
    return packed


def setup_kernel(
    par, rhs_hbm, diag_hbm, couple_hbm, trans_hbm, weights_hbm, wells_hbm, msg1, msg2, own, cols,
    rhs, diag0, couple0, trans, weights, wells, sems,
):
    pairs = (
        (weights_hbm, weights),
        (couple_hbm.at[:, 0:1], couple0),
        (diag_hbm.at[:, 0:1], diag0),
        (trans_hbm, trans),
        (rhs_hbm, rhs),
        (wells_hbm, wells),
    )
    copies = [pltpu.make_async_copy(a, b, sems.at[i]) for i, (a, b) in enumerate(pairs)]
    for copy in copies:
        copy.start()
    for copy in copies:
        copy.wait()
    rows, lanes = iotas((R, L))
    center = WELL_BOOST * wells[...].astype(jnp.float32) * weights[0]
    pressure = jnp.zeros((R, L), jnp.float32)
    links = [jnp.zeros((R, L), jnp.float32) for _ in range(4)]
    for c in range(NC):
        w, col = (weights[c], couple0[c, 0])
        center = center + w * diag0[c, 0]
        pressure = pressure + w * rhs[c]
        for d, (axis, step) in enumerate(((0, 1), (0, -1), (1, 1), (1, -1))):
            links[d] = links[d] + w * shifted(col, axis, step)
    inside = (rows != R - 1, rows != 0, lanes != L - 1, lanes != 0)
    fields = [center]
    for d in range(4):
        fields.append(jnp.where(inside[d], -trans[d] * links[d], 0.0))
    fields.append(pressure)
    for k, field in enumerate(fields):
        span = pl.ds(k * R, R)
        own[span, :] = field
        msg1[span, :] = field
        msg2[span, :] = field
    t_up, t_down = (trans[0, R - 1 : R, :], trans[1, 0:1, :])
    t_right, t_left = (trans[2], trans[3])
    for c in range(NC):
        put(par, 0, msg1, msg2, pl.ds(AX_EDGE + c, 1), couple0[c, 0, R - 1 : R, :], couple0[c, 0, 0:1, :])
        put(par, 0, msg1, msg2, pl.ds(AX_EDGE + NC + c, 1), t_up * weights[c, R - 1 : R, :], t_down * weights[c, 0:1, :])
    blank = jnp.zeros((24 - 2 * NC, L), jnp.float32)
    msg1[pl.ds(AX_EDGE + 2 * NC, 24 - 2 * NC), :] = blank
    msg2[pl.ds(AX_EDGE + 2 * NC, 24 - 2 * NC), :] = blank
    parts = []
    for c in range(NC):
        col, w = (couple0[c, 0], weights[c])
        parts += [(col, 0, c), (t_left * w, 0, NC + c), (col, L - 1, 2 * NC + c), (t_right * w, L - 1, 3 * NC + c)]
    packed = pack_columns(parts)
    cols[...] = packed
    msg1[pl.ds(AX_COL, R), :] = packed
    msg2[pl.ds(AX_COL, R), :] = packed


def inverse_kernel(diag, wells, out):
    boost = WELL_BOOST * wells[...].astype(jnp.float32)
    a = [[diag[i, j] + boost if i == j else diag[i, j] for j in range(NC)] for i in range(NC)]
    for k in range(NC):
        inv = 1.0 / a[k][k]
        a[k] = [inv if j == k else a[k][j] * inv for j in range(NC)]
        for i in range(NC):
            if i != k:
                factor = a[i][k]
                a[i] = [-factor * inv if j == k else a[i][j] - factor * a[k][j] for j in range(NC)]
    for i in range(NC):
        for j in range(NC):
            out[i, j] = a[i][j]


def ring_kernel(inverse, diag, couple, trans, wells, pack_left, pack_right, rows_up, rows_down):
    boost = WELL_BOOST * wells[...].astype(jnp.float32)
    entries = []
    for k in range(NC):
        for c in range(NC):
            total = couple[c, 0] * inverse[0, k]
            for m in range(1, NC):
                total = total + couple[c, m] * inverse[m, k]
            entries.append((total, 0, NC * k + c))
    for c in range(NC):
        entries.append((diag[c, 0] + boost if c == 0 else diag[c, 0], 0, RING_EFF + c))
        entries.append((couple[c, 0], 1, RING_NEXT + c))
    for d in range(4):
        entries.append((trans[d], 0, RING_TRANS + d))
    pack_left[...] = pack_columns([(v, inward, place) for v, inward, place in entries])
    pack_right[...] = pack_columns([(v, L - 1 - inward, place) for v, inward, place in entries])
    zero = jnp.zeros((1, L), jnp.float32)

    @pl.when(pl.program_id(0) == 0)
    def _():
        rows_down[pl.ds(RING_STATIC - 1, 1), :] = zero
        for v, inward, place in entries:
            rows_down[pl.ds(place, 1), :] = v[inward : inward + 1, :]

    @pl.when(pl.program_id(0) == R // 8 - 1)
    def _():
        rows_up[pl.ds(RING_STATIC - 1, 1), :] = zero
        for v, inward, place in entries:
            rows_up[pl.ds(place, 1), :] = v[7 - inward : 8 - inward, :]


def setup_middle_kernel(par, got1, got2, own, cols, couple0, trans, weights, _, msg1, msg2, ext, ext_cols, edges):
    rows, lanes = iotas((EX, L))

    def dots(span_of):
        total = jnp.zeros((1, L), jnp.float32)
        for c in range(NC):
            total = total + span_of(c)
        return -total

    ups, downs, tw_ups, tw_downs = ([], [], [], [])
    for c in range(NC):
        up, down = take(par, 0, got1, got2, pl.ds(AX_EDGE + c, 1))
        ups.append(up)
        downs.append(down)
        up, down = take(par, 0, got1, got2, pl.ds(AX_EDGE + NC + c, 1))
        tw_ups.append(up)
        tw_downs.append(down)
        edges[pl.ds(c, 1), :] = ups[c]
        edges[pl.ds(NC + c, 1), :] = downs[c]
        edges[pl.ds(2 * NC + c, 1), :] = tw_ups[c]
        edges[pl.ds(3 * NC + c, 1), :] = tw_downs[c]
    t_up, t_down = (trans[0, R - 1 : R, :], trans[1, 0:1, :])
    east_own = dots(lambda c: t_up * weights[c, R - 1 : R, :] * ups[c])
    west_own = dots(lambda c: t_down * weights[c, 0:1, :] * downs[c])
    west_up = dots(lambda c: tw_ups[c] * couple0[c, 0, R - 1 : R, :])
    east_down = dots(lambda c: tw_downs[c] * couple0[c, 0, 0:1, :])
    fields = []
    for k in range(6):
        up, down = take(par, 0, got1, got2, pl.ds(k * R, R))
        field = jnp.concatenate([own[pl.ds(k * R, R), :], up, down], axis=0)
        if k == CENTER:
            field = jnp.where(field == 0.0, 1.0, field)
        if k == EAST:
            field = jnp.where(rows == R - 1, east_own, jnp.where(rows == EX - 1, east_down, field))
        if k == WEST:
            field = jnp.where(rows == 0, west_own, jnp.where(rows == R, west_up, field))
        ext[k] = field
        fields.append(field)
    up, down = take(par, 0, got1, got2, pl.ds(AX_COL, R))
    packed = jnp.concatenate([cols[...], up, down], axis=0)
    ext_cols[...] = packed
    to_right = [lane_roll(f, HALO * (k % 4) + HALO) for k, f in enumerate(fields)]
    to_left = [lane_roll(f, HALO * (k % 4)) for k, f in enumerate(fields)]
    group = lanes // HALO

    def quad(parts):
        result = parts[-1]
        for g in range(len(parts) - 2, -1, -1):
            result = jnp.where(group == g, parts[g], result)
        return result

    put(par, 1, msg1, msg2, pl.ds(0, EX), quad(to_right[:4]), quad(to_left[:4]))
    put(
        par,
        1,
        msg1,
        msg2,
        pl.ds(EX, EX),
        quad(to_right[4:] + [lane_roll(packed, 64 - 2 * NC)]),
        quad(to_left[4:] + [lane_roll(packed, 64)]),
    )


def lane_sum(product, start):
    lanes = iotas(product.shape)[1]
    keep = jnp.logical_and(lanes >= start, lanes < start + NC)
    return jnp.sum(jnp.where(keep, product, 0.0), axis=1, keepdims=True)


def pair_sums(values, step):
    rows, lanes = iotas(values.shape)
    values = values + jnp.where((rows // step) % 2 == 0, shifted(values, 0, step), shifted(values, 0, -step))
    return values + jnp.where((lanes // step) % 2 == 0, shifted(values, 1, step), shifted(values, 1, -step))


def coarsen_into(coeffs, level):
    step = 2**level
    base, out = (6 * level, 6 * level + 6)
    rows, lanes = iotas((EX, EY))
    row_even = (rows // step) % 2 == 0
    lane_even = (lanes // step) % 2 == 0
    east, west, north, south = (coeffs[base + d] for d in (EAST, WEST, NORTH, SOUTH))
    center = coeffs[base] + (jnp.where(row_even, east, west) + jnp.where(lane_even, north, south))
    center = pair_sums(center, step)
    coeffs[out + CENTER] = center
    coeffs[out + SCALE] = RELAX / center
    coeffs[out + EAST] = pair_sums(jnp.where(row_even, 0.0, east), step)
    coeffs[out + WEST] = pair_sums(jnp.where(row_even, west, 0.0), step)
    coeffs[out + NORTH] = pair_sums(jnp.where(lane_even, 0.0, north), step)
    coeffs[out + SOUTH] = pair_sums(jnp.where(lane_even, south, 0.0), step)


def level_apply(values, coeffs, level):
    step = 2**level
    base = 6 * level
    return coeffs[base + CENTER] * values + (
        coeffs[base + EAST] * shifted(values, 0, step)
        + coeffs[base + WEST] * shifted(values, 0, -step)
        + coeffs[base + NORTH] * shifted(values, 1, step)
        + coeffs[base + SOUTH] * shifted(values, 1, -step)
    )


def sweep(values, source, coeffs, level):
    return values + coeffs[6 * level + SCALE] * (source - level_apply(values, coeffs, level))


def vcycle(source, coeffs):
    values0 = coeffs[SCALE] * source
    source1 = pair_sums(source - level_apply(values0, coeffs, 0), 1)
    values1 = coeffs[6 + SCALE] * source1
    source2 = pair_sums(source1 - level_apply(values1, coeffs, 1), 2)
    values2 = coeffs[12 + SCALE] * source2
    for _ in range(COARSE_SWEEPS - 1):
        values2 = sweep(values2, source2, coeffs, 2)
    values1 = sweep(values1 + values2, source1, coeffs, 1)
    return sweep(values0 + values1, source, coeffs, 0)


def ghost_column(packed, start, to_lane, lane):
    return lane_roll(packed, to_lane - (start + lane))


def neighbour_sum(values, trans, up_row, down_row, right_col, left_col):
    rows, lanes = iotas((R, L))
    east = jnp.where(rows == R - 1, up_row, shifted(values, 0, 1))
    west = jnp.where(rows == 0, down_row, shifted(values, 0, -1))
    north = jnp.where(lanes == L - 1, right_col, shifted(values, 1, 1))
    south = jnp.where(lanes == 0, left_col, shifted(values, 1, -1))
    return trans[0] * east + trans[1] * west + trans[2] * north + trans[3] * south


def ghost_rows(trans, up_row, down_row):
    rows, _ = iotas((R, L))
    return jnp.where(rows == R - 1, trans[0] * up_row, 0.0) + jnp.where(rows == 0, trans[1] * down_row, 0.0)


def ghost_columns(trans, right_col, left_col):
    _, lanes = iotas((R, L))
    return jnp.where(lanes == L - 1, trans[2] * right_col, 0.0) + jnp.where(lanes == 0, trans[3] * left_col, 0.0)


def one_step(pressure, vector, edges, col_right, col_left, diag, inverse, couple, trans, boost, z_out):
    p = pressure[0:R, 0:L]
    up_row, down_row = (pressure[R : R + 1, 0:L], pressure[EX - 1 : EX, 0:L])
    far = pressure[0:R, L:EY]
    right_p, left_p = (lane_roll(far, L - 1), lane_roll(far, 1))
    second = []
    for c in range(NC):
        own = diag[c, 0] * p
        if c == 0:
            own = own + boost * p
        around = neighbour_sum(
            couple[c, 0] * p,
            trans,
            edges[pl.ds(c, 1), :] * up_row,
            edges[pl.ds(NC + c, 1), :] * down_row,
            ghost_column(col_right, 64, L - 1, c) * right_p,
            ghost_column(col_left, 64, 0, c) * left_p,
        )
        second.append(vector[c] - (own - around))
    rest = []
    for c in range(NC):
        total = inverse[c, 0] * second[0]
        for k in range(1, NC):
            total = total + inverse[c, k] * second[k]
        rest.append(total)
        z_out[c] = total + p if c == 0 else total
    products = []
    for c in range(NC):
        product = couple[c, 0] * rest[0]
        for k in range(1, NC):
            product = product + couple[c, k] * rest[k]
        products.append(product)
    return products


def first_step_kernel(
    par, got1, got2, ext, ext_cols, edges, rhs, trans, weights, wells, diag, inverse, couple, rows_up, rows_down,
    msg1, msg2, z_out, partial, product, coeffs, cols_right, cols_left, pressure_part, product_cols,
):
    rows, lanes = iotas((EX, L))
    right, left = take(par, 1, got1, got2, pl.ds(EX, EX))
    cols_right[...] = right
    cols_left[...] = left
    packed = ext_cols[...]
    north_own = -lane_sum(lane_roll(packed, 64 - 3 * NC) * right, 64)
    south_right = -lane_sum(lane_roll(packed, 64 - NC) * right, 64 + NC)
    south_own = -lane_sum(lane_roll(packed, 64 - NC) * left, 64)
    north_left = -lane_sum(lane_roll(packed, 64 + NC) * left, 64 + NC)
    right_four, left_four = take(par, 1, got1, got2, pl.ds(0, EX))
    source = None
    for k in range(6):
        from_right = lane_roll(right_four if k < 4 else right, -HALO * (k % 4))
        from_left = lane_roll(left_four if k < 4 else left, L - HALO - HALO * (k % 4))
        near = ext[k]
        far = jnp.where(lanes < HALO, from_right, jnp.where(lanes >= L - HALO, from_left, 0.0))
        if k == CENTER:
            far = jnp.where(far == 0.0, 1.0, far)
        if k == NORTH:
            near = jnp.where(lanes == L - 1, north_own, near)
            far = jnp.where(lanes == L - 1, north_left, far)
        if k == SOUTH:
            near = jnp.where(lanes == 0, south_own, near)
            far = jnp.where(lanes == 0, south_right, far)
        field = jnp.concatenate([near, far], axis=1)
        if k == 5:
            source = field
        else:
            coeffs[k] = field
    coeffs[SCALE] = RELAX / coeffs[CENTER]
    coarsen_into(coeffs, 0)
    coarsen_into(coeffs, 1)
    pressure = vcycle(source, coeffs)
    boost = WELL_BOOST * wells[...].astype(jnp.float32)
    vector = [rhs[c] for c in range(NC)]
    products = one_step(
        pressure, vector, edges, right[0:R], left[0:R], diag, inverse, couple, trans, boost, z_out
    )
    put(par, 0, msg1, msg2, pl.ds(BX_RING, RING_STATIC), rows_up[...], rows_down[...])
    weighed = jnp.zeros((R, L), jnp.float32)
    zero = jnp.zeros((1, L), jnp.float32)
    parts = []
    for c in range(NC):
        product[c] = products[c]
        value = -neighbour_sum(products[c], trans, zero, zero, 0.0, 0.0)
        partial[c] = value
        weighed = weighed + weights[c] * value
        last, first = (slice(R - 1, R), slice(0, 1))
        put(par, 0, msg1, msg2, pl.ds(BX_EDGE + c, 1), products[c][last], products[c][first])
        put(par, 0, msg1, msg2, pl.ds(BX_RING + RING_VECTOR + c, 1), value[last], value[first])
        parts += [(products[c], 0, c), (products[c], L - 1, NC + c)]
    blank = jnp.zeros((16 - NC, L), jnp.float32)
    columns = pack_columns(parts)
    pressure_part[...] = weighed
    product_cols[...] = columns
    for msg in (msg1, msg2):
        msg[pl.ds(0, R), :] = weighed
        msg[pl.ds(BX_EDGE + NC, 16 - NC), :] = blank
        msg[pl.ds(BX_COL, R), :] = columns


def between_kernel(
    par, got1, got2, pressure_part, product_cols, product, edges, trans, weights, partial, pack_left, pack_right,
    msg1, msg2, ext, ext_cols, rows_out, vector_out,
):
    rows, lanes = iotas((EX, L))
    t_up, t_down = (trans[0, R - 1 : R, :], trans[1, 0:1, :])
    own_up, own_down, far_up, far_down = (jnp.zeros((1, L), jnp.float32) for _ in range(4))
    to_right, to_left = ([], [])
    for c in range(NC):
        up, down = take(par, 0, got1, got2, pl.ds(BX_EDGE + c, 1))
        rows_out[pl.ds(c, 1), :] = up
        rows_out[pl.ds(NC + c, 1), :] = down
        own_up = own_up + t_up * weights[c, R - 1 : R, :] * up
        own_down = own_down + t_down * weights[c, 0:1, :] * down
        far_up = far_up + edges[pl.ds(2 * NC + c, 1), :] * product[c, R - 1 : R, :]
        far_down = far_down + edges[pl.ds(3 * NC + c, 1), :] * product[c, 0:1, :]
        value = partial[c] - ghost_rows(trans, up, down)
        vector_out[c] = value
        to_right.append((value, L - 1, RING_VECTOR + c))
        to_left.append((value, 0, RING_VECTOR + c))
    up, down = take(par, 0, got1, got2, pl.ds(0, R))
    field = jnp.concatenate([pressure_part[...], up, down], axis=0)
    edge = jnp.where(rows == R - 1, own_up, 0.0) + jnp.where(rows == 0, own_down, 0.0)
    edge = edge + jnp.where(rows == R, far_up, 0.0) + jnp.where(rows == EX - 1, far_down, 0.0)
    field = field - edge
    ext[...] = field
    up, down = take(par, 0, got1, got2, pl.ds(BX_COL, R))
    packed = jnp.concatenate([product_cols[...], up, down], axis=0)
    ext_cols[...] = packed
    near = lanes < HALO
    put(
        par, 1, msg1, msg2, pl.ds(0, EX),
        jnp.where(near, lane_roll(field, HALO), lane_roll(packed, HALO - NC)),
        jnp.where(near, field, lane_roll(packed, HALO)),
    )
    fixed = iotas((R, L))[1] < RING_VECTOR
    put(
        par, 1, msg1, msg2, pl.ds(EX, R),
        jnp.where(fixed, pack_right[...], pack_columns(to_right)),
        jnp.where(fixed, pack_left[...], pack_columns(to_left)),
    )


def row_ring(ring, outward, inward, pressure, row, out_row, own_row, edge_cols, product_row, couple_row, corners, old_corners):
    lanes = iotas((1, L))[1]
    line = pressure[row : row + 1, :]
    p = line[:, 0:L]
    p_right, p_left = (line[:, L : L + 1], line[:, EY - 1 : EY])
    p_out, p_own = (pressure[out_row : out_row + 1, 0:L], pressure[own_row : own_row + 1, 0:L])
    t_out, t_in = (ring(RING_TRANS + outward), ring(RING_TRANS + inward))
    t_right, t_left = (ring(RING_TRANS + 2), ring(RING_TRANS + 3))
    second = []
    for c in range(NC):
        beside = edge_cols(c) * p
        old_right, old_left = (ghost_column(old_corners[0], 64, L - 1, c), ghost_column(old_corners[1], 64, 0, c))
        new_right, new_left = (ghost_column(corners[0], HALO, L - 1, c), ghost_column(corners[1], HALO, 0, c))
        north = jnp.where(lanes == L - 1, old_right * p_right, shifted(beside, 1, 1))
        south = jnp.where(lanes == 0, old_left * p_left, shifted(beside, 1, -1))
        value = ring(RING_VECTOR + c) - t_in * product_row(c)
        value = value - jnp.where(lanes == L - 1, t_right * new_right, 0.0)
        value = value - jnp.where(lanes == 0, t_left * new_left, 0.0)
        second.append(
            value
            - ring(RING_EFF + c) * p
            + t_out * (ring(RING_NEXT + c) * p_out)
            + t_in * (couple_row(c) * p_own)
            + t_right * north
            + t_left * south
        )
    return second


def column_ring(pack, outward, inward, p, p_out, p_own, p_up, p_down, own_couple, own_product, beside_up, beside_down):
    lanes = iotas((R, L))[1]

    def trans(d):
        return pack[:, RING_TRANS + d : RING_TRANS + d + 1]

    second = (
        lane_roll(pack, -RING_VECTOR)
        - trans(inward) * own_product
        - lane_roll(pack, -RING_EFF) * p
        + trans(outward) * (lane_roll(pack, -RING_NEXT) * p_out)
        + trans(inward) * (own_couple * p_own)
        + trans(0) * (beside_up * p_up)
        + trans(1) * (beside_down * p_down)
    )
    spread = jnp.zeros((R, L), jnp.float32)
    for k in range(NC):
        within = jnp.logical_and(lanes >= NC * k, lanes < NC * k + NC)
        spread = jnp.where(within, second[:, k : k + 1], spread)
    terms = pack * spread
    total = terms
    for k in range(1, NC):
        total = total + lane_roll(terms, -NC * k)
    return total


def second_step_kernel(
    par, got1, got2, gotx1, gotx2, ext, ext_cols, rows_in, setup_cols, cols_right, cols_left, edges, coeffs, partial,
    product, rhs, trans, wells, diag, inverse, couple,
    z_out, dots, ring_up, ring_down,
):
    rows, lanes = iotas((EX, L))
    right, left = take(par, 1, got1, got2, pl.ds(0, EX))
    packed, tw = (ext_cols[...], setup_cols[...])
    old_right, old_left = (cols_right[...], cols_left[...])
    own_right = lane_sum(lane_roll(tw, HALO - 3 * NC) * right, HALO)
    own_left = lane_sum(lane_roll(tw, HALO - NC) * left, HALO)
    far_right = lane_sum(old_right * lane_roll(packed, 64), 64 + NC)
    far_left = lane_sum(old_left * lane_roll(packed, 64 + NC), 64 + NC)
    near = ext[...] - jnp.where(lanes == L - 1, own_right, 0.0) - jnp.where(lanes == 0, own_left, 0.0)
    far = jnp.where(
        lanes < HALO, right, jnp.where(lanes >= L - HALO, lane_roll(left, L - HALO), 0.0)
    )
    far = far - jnp.where(lanes == 0, far_right, 0.0) - jnp.where(lanes == L - 1, far_left, 0.0)
    pressure = vcycle(jnp.concatenate([near, far], axis=1), coeffs)
    vector = []
    for c in range(NC):
        columns = ghost_columns(
            trans, ghost_column(right[0:R], HALO, L - 1, c), ghost_column(left[0:R], HALO, 0, c)
        )
        vector.append(partial[c] - columns)
    boost = WELL_BOOST * wells[...].astype(jnp.float32)
    products = one_step(
        pressure, vector, edges, old_right[0:R], old_left[0:R], diag, inverse, couple, trans, boost, z_out
    )
    up, down = take(par, 0, gotx1, gotx2, pl.ds(BX_RING, 112))
    ring_up[...] = up
    ring_down[...] = down
    second_up = row_ring(
        lambda i: ring_up[pl.ds(i, 1), :], 0, 1, pressure, R, R + 1, R - 1,
        lambda c: edges[pl.ds(c, 1), :], lambda c: product[c, R - 1 : R, :], lambda c: couple[c, 0, R - 1 : R, :],
        (right[R : R + 1], left[R : R + 1]), (old_right[R : R + 1], old_left[R : R + 1]),
    )
    second_down = row_ring(
        lambda i: ring_down[pl.ds(i, 1), :], 1, 0, pressure, EX - 1, EX - 2, 0,
        lambda c: edges[pl.ds(NC + c, 1), :], lambda c: product[c, 0:1, :], lambda c: couple[c, 0, 0:1, :],
        (right[EX - 1 : EX], left[EX - 1 : EX]), (old_right[EX - 1 : EX], old_left[EX - 1 : EX]),
    )
    product_up = ring_up[pl.ds(0, NC), :] * second_up[0]
    product_down = ring_down[pl.ds(0, NC), :] * second_down[0]
    for k in range(1, NC):
        product_up = product_up + ring_up[pl.ds(NC * k, NC), :] * second_up[k]
        product_down = product_down + ring_down[pl.ds(NC * k, NC), :] * second_down[k]
    pack_right, pack_left = take(par, 1, got1, got2, pl.ds(EX, R))
    far_p = pressure[:, L:EY]
    far_up, far_down = (shifted(far_p, 0, 1)[0:R], shifted(far_p, 0, -1)[0:R])
    far_p, near_p = (far_p[0:R], pressure[0:R, 0:L])
    right_cols = column_ring(
        pack_right, 2, 3, far_p[:, 0:1], far_p[:, 1:2], near_p[:, L - 1 : L], far_up[:, 0:1], far_down[:, 0:1],
        lane_roll(tw[0:R], -2 * NC), lane_roll(packed[0:R], -NC),
        lane_roll(shifted(old_right, 0, 1)[0:R], -64), lane_roll(shifted(old_right, 0, -1)[0:R], -64),
    )
    left_cols = column_ring(
        pack_left, 3, 2, far_p[:, L - 1 : L], far_p[:, L - 2 : L - 1], near_p[:, 0:1], far_up[:, L - 1 : L],
        far_down[:, L - 1 : L], tw[0:R], packed[0:R],
        lane_roll(shifted(old_left, 0, 1)[0:R], -64), lane_roll(shifted(old_left, 0, -1)[0:R], -64),
    )
    sums = [jnp.zeros((R, L), jnp.float32) for _ in range(6)]
    for c in range(NC):
        two = -neighbour_sum(
            products[c], trans, product_up[c : c + 1], product_down[c : c + 1],
            ghost_column(right_cols, 0, L - 1, c), ghost_column(left_cols, 0, 0, c),
        )
        zero, one = (rhs[c], vector[c])
        for k, (a, b) in enumerate(((zero, zero), (zero, one), (one, one), (zero, two), (one, two), (two, two))):
            sums[k] = sums[k] + a * b
    lane = iotas((1, L))[1]
    row = jnp.zeros((1, L), jnp.float32)
    for k, total in enumerate(sums):
        row = jnp.where(lane == k, jnp.sum(total, keepdims=True), row)
    dots[...] = jnp.broadcast_to(row, dots.shape)


def finish_kernel(gathered, z_one, z_two, out, estimate):
    row = jnp.sum(gathered[...], axis=0, keepdims=True)
    lanes = iotas((1, L))[1]
    g00, g01, g11, g02, g12, g22 = (
        jnp.sum(jnp.where(lanes == k, row, 0.0), axis=1, keepdims=True) for k in range(6)
    )
    beta = jnp.sqrt(g00)
    shift = g01 / g00
    h00 = 1.0 + shift
    length2 = g11 - shift * g01
    length = jnp.sqrt(length2)
    h10 = length / beta
    h01 = (g02 - shift * g01) / (beta * length)
    above = (g12 - shift * g02 - shift * (g11 - shift * g01)) / length2
    h11 = 1.0 + above
    h21 = jnp.sqrt((g22 - 2.0 * shift * g12 + shift * shift * g11) / length2 - h01 * h01 - above * above)
    radius0 = jnp.sqrt(h00 * h00 + h10 * h10)
    cos0, sin0 = (h00 / radius0, h10 / radius0)
    r01 = cos0 * h01 + sin0 * h11
    mid = cos0 * h11 - sin0 * h01
    radius1 = jnp.sqrt(mid * mid + h21 * h21)
    cos1, sin1 = (mid / radius1, h21 / radius1)
    rhs0, rhs1 = (cos0 * beta, -sin0 * beta)
    estimate[...] = jnp.abs(sin1 * rhs1)
    y1 = cos1 * rhs1 / radius1
    y0 = (rhs0 - r01 * y1) / radius0
    weight1 = y1 / length
    weight0 = y0 / beta - weight1 * shift
    for c in range(NC):
        out[c] = weight0 * z_one[c] + weight1 * z_two[c]


VMEM = functools.partial(pl.BlockSpec, memory_space=pltpu.VMEM)
HBM = functools.partial(pl.BlockSpec, memory_space=pltpu.HBM)
ANY = functools.partial(pl.BlockSpec, memory_space=pl.ANY)


def shape(*dims):
    return jax.ShapeDtypeStruct(dims, jnp.float32)


def call(kernel, in_specs, outs, scratch=(), cost=20_000_000):
    return pl.pallas_call(
        kernel,
        in_specs=list(in_specs),
        out_specs=[VMEM()] * len(outs),
        out_shape=list(outs),
        scratch_shapes=list(scratch),
        cost_estimate=pl.CostEstimate(flops=cost, bytes_accessed=1_000_000, transcendentals=0),
        compiler_params=pltpu.CompilerParams(vmem_limit_bytes=30 * 1024 * 1024),
    )


def swap(first, second, axis):
    peers = lax.axis_size(axis)
    pairs = [(i, i ^ 1) for i in range(peers) if i ^ 1 < peers]
    others = [(i, ((i + 1) ^ 1) - 1) for i in range(1, peers) if ((i + 1) ^ 1) - 1 < peers]
    return (lax.ppermute(first, axis, others), lax.ppermute(second, axis, pairs))


def on_device(right_side, diag_blocks, couple_blocks, transmissibility, pressure_weights, well_mask):
    par = jnp.stack([1 - (lax.axis_index("gx") & 1), 1 - (lax.axis_index("gy") & 1)]).astype(jnp.int32)
    par = jnp.broadcast_to(par[:, None], (2, L))
    column = pl.BlockSpec((NC, 1, R, L), lambda i: (0, 0, 0, 0))

    def whole(*dims):
        return pl.BlockSpec(dims, lambda i: (0,) * len(dims))

    msg_a1, msg_a2, own, cols = call(
        setup_kernel,
        [VMEM()] + [HBM()] * 6,
        [shape(AX_ROWS, L), shape(AX_ROWS, L), shape(6 * R, L), shape(R, L)],
        [
            pltpu.VMEM((NC, R, L), jnp.float32),
            pltpu.VMEM((NC, 1, R, L), jnp.float32),
            pltpu.VMEM((NC, 1, R, L), jnp.float32),
            pltpu.VMEM((4, R, L), jnp.float32),
            pltpu.VMEM((NC, R, L), jnp.float32),
            pltpu.VMEM((R, L), jnp.int32),
            pltpu.SemaphoreType.DMA((6,)),
        ],
    )(
        par,
        *(
            pltpu.with_memory_space_constraint(x, pltpu.HBM)
            for x in (right_side, diag_blocks, couple_blocks, transmissibility, pressure_weights, well_mask)
        ),
    )

    got_a1, got_a2 = swap(msg_a1, msg_a2, "gx")

    slab = pl.BlockSpec((NC, NC, 8, L), lambda i: (0, 0, i, 0))
    strip = pl.BlockSpec((8, L), lambda i: (i, 0))
    inverse = pl.pallas_call(
        inverse_kernel,
        grid=(R // 8,),
        in_specs=[slab, strip],
        out_specs=slab,
        out_shape=shape(NC, NC, R, L),
        cost_estimate=pl.CostEstimate(flops=20_000_000, bytes_accessed=2_700_000, transcendentals=0),
        compiler_params=pltpu.CompilerParams(vmem_limit_bytes=30 * 1024 * 1024),
    )(diag_blocks, well_mask)
    pack_left, pack_right, rows_up, rows_down = pl.pallas_call(
        ring_kernel,
        grid=(R // 8,),
        in_specs=[slab, slab, slab, pl.BlockSpec((4, 8, L), lambda i: (0, i, 0)), strip],
        out_specs=[strip, strip, whole(RING_STATIC, L), whole(RING_STATIC, L)],
        out_shape=[shape(R, L), shape(R, L), shape(RING_STATIC, L), shape(RING_STATIC, L)],
        cost_estimate=pl.CostEstimate(flops=20_000_000, bytes_accessed=2_700_000, transcendentals=0),
        compiler_params=pltpu.CompilerParams(vmem_limit_bytes=30 * 1024 * 1024),
    )(inverse, diag_blocks, couple_blocks, transmissibility, well_mask)

    msg_y1, msg_y2, ext, ext_cols, edges = pl.pallas_call(
        setup_middle_kernel,
        grid=(1,),
        in_specs=[
            VMEM(), whole(AX_ROWS, L), whole(AX_ROWS, L), whole(6 * R, L), whole(R, L), column,
            whole(4, R, L), whole(NC, R, L), ANY(),
        ],
        out_specs=[whole(AY_ROWS, L), whole(AY_ROWS, L), whole(6, EX, L), whole(EX, L), whole(4 * NC, L)],
        out_shape=[shape(AY_ROWS, L), shape(AY_ROWS, L), shape(6, EX, L), shape(EX, L), shape(4 * NC, L)],
        compiler_params=pltpu.CompilerParams(vmem_limit_bytes=30 * 1024 * 1024),
    )(par, got_a1, got_a2, own, cols, couple_blocks, transmissibility, pressure_weights, inverse)

    got_y1, got_y2 = swap(msg_y1, msg_y2, "gy")

    fields = shape(NC, R, L)
    msg_b1, msg_b2, z_one, partial, product, coeffs, cols_right, cols_left, pressure_part, product_cols = call(
        first_step_kernel,
        [VMEM()] + [VMEM()] * 14,
        [
            shape(BX_ROWS, L), shape(BX_ROWS, L), fields, fields, fields, shape(18, EX, EY),
            shape(EX, L), shape(EX, L), shape(R, L), shape(R, L),
        ],
    )(
        par, got_y1, got_y2, ext, ext_cols, edges, right_side, transmissibility, pressure_weights, well_mask,
        diag_blocks, inverse, couple_blocks, rows_up, rows_down,
    )

    got_b1, got_b2 = swap(msg_b1, msg_b2, "gx")
    msg_c1, msg_c2, ext_b, ext_cols_b, rows_b, vector_b = call(
        between_kernel,
        [VMEM()] + [VMEM()] * 11,
        [shape(EX + R, L), shape(EX + R, L), shape(EX, L), shape(EX, L), shape(2 * NC, L), fields],
    )(
        par, got_b1, got_b2, pressure_part, product_cols, product, edges, transmissibility, pressure_weights,
        partial, pack_left, pack_right,
    )
    got_c1, got_c2 = swap(msg_c1, msg_c2, "gy")

    devices = lax.axis_size("gx") * lax.axis_size("gy")
    z_two, local = call(
        second_step_kernel,
        [VMEM()] + [VMEM()] * 20,
        [fields, shape(devices, L)],
        [pltpu.VMEM((112, L), jnp.float32), pltpu.VMEM((112, L), jnp.float32)],
    )(
        par, got_c1, got_c2, got_b1, got_b2, ext_b, ext_cols_b, rows_b, ext_cols, cols_right, cols_left, edges, coeffs,
        vector_b, product, right_side, transmissibility, well_mask, diag_blocks, inverse, couple_blocks,
    )
    gathered = lax.all_to_all(local, ("gx", "gy"), 0, 0, tiled=True)
    answer, estimate = call(finish_kernel, [VMEM()] * 3, [fields, shape(1, 1)])(gathered, z_one, z_two)
    return (answer, estimate.reshape(()))


def solution(mesh):
    return jax.shard_map(
        on_device,
        mesh=mesh,
        in_specs=(
            P(None, "gx", "gy"),
            P(None, None, "gx", "gy"),
            P(None, None, "gx", "gy"),
            P(None, "gx", "gy"),
            P(None, "gx", "gy"),
            P("gx", "gy"),
        ),
        out_specs=(P(None, "gx", "gy"), P()),
        check_vma=False,
    )
```

```python
import functools

import jax
import jax.numpy as jnp
from jax import lax
from jax.experimental import pallas as pl
from jax.experimental.pallas import tpu as pltpu
from jax.sharding import PartitionSpec as P

NC = 9
COARSE_SWEEPS = 6
RELAX = 0.8
WELL_BOOST = 8.0

R, L = 32, 128
HALO = 32
EX, EY = 3 * R, 2 * L

AX_EDGE = 6 * R
AX_COL = AX_EDGE + 24
AX_ROWS = AX_COL + R
AY_ROWS = 2 * EX
BX_EDGE = R
BX_COL = BX_EDGE + 16
BX_RING = BX_COL + R
BX_ROWS = BX_RING + 112
RING_EFF, RING_NEXT, RING_TRANS, RING_VECTOR, RING_STATIC = 81, 90, 99, 103, 104

CENTER, EAST, WEST, NORTH, SOUTH, SCALE = range(6)


def iotas(shape):
    return (lax.broadcasted_iota(jnp.int32, shape, 0), lax.broadcasted_iota(jnp.int32, shape, 1))


def shifted(values, axis, step):
    return pltpu.roll(values, (-step) % values.shape[axis], axis)


def lane_roll(values, shift):
    shift = shift % values.shape[1]
    return values if shift == 0 else pltpu.roll(values, shift, 1)


def first_is_up(par_ref, which, shape):
    return jnp.broadcast_to(par_ref[which : which + 1, :], shape) == 0


def put(par_ref, which, first, second, rows, up, down):
    mask = first_is_up(par_ref, which, up.shape)
    first[rows, :] = jnp.where(mask, up, down)
    second[rows, :] = jnp.where(mask, down, up)


def take(par_ref, which, first, second, rows):
    one, two = (first[rows, :], second[rows, :])
    mask = first_is_up(par_ref, which, one.shape)
    return (jnp.where(mask, one, two), jnp.where(mask, two, one))


def pack_columns(parts):
    shape = parts[0][0].shape
    lanes = iotas(shape)[1]
    packed = jnp.zeros(shape, jnp.float32)
    for values, lane, target in parts:
        packed = jnp.where(lanes == target, lane_roll(values, target - lane), packed)
    return packed


def setup_kernel(
    par, rhs_hbm, diag_hbm, couple_hbm, trans_hbm, weights_hbm, wells_hbm, msg1, msg2, own, cols,
    rhs, diag0, couple0, trans, weights, wells, sems,
):
    pairs = (
        (weights_hbm, weights),
        (couple_hbm.at[:, 0:1], couple0),
        (diag_hbm.at[:, 0:1], diag0),
        (trans_hbm, trans),
        (rhs_hbm, rhs),
        (wells_hbm, wells),
    )
    copies = [pltpu.make_async_copy(a, b, sems.at[i]) for i, (a, b) in enumerate(pairs)]
    for copy in copies:
        copy.start()
    for copy in copies:
        copy.wait()
    rows, lanes = iotas((R, L))
    center = WELL_BOOST * wells[...].astype(jnp.float32) * weights[0]
    pressure = jnp.zeros((R, L), jnp.float32)
    links = [jnp.zeros((R, L), jnp.float32) for _ in range(4)]
    for c in range(NC):
        w, col = (weights[c], couple0[c, 0])
        center = center + w * diag0[c, 0]
        pressure = pressure + w * rhs[c]
        for d, (axis, step) in enumerate(((0, 1), (0, -1), (1, 1), (1, -1))):
            links[d] = links[d] + w * shifted(col, axis, step)
    inside = (rows != R - 1, rows != 0, lanes != L - 1, lanes != 0)
    fields = [center]
    for d in range(4):
        fields.append(jnp.where(inside[d], -trans[d] * links[d], 0.0))
    fields.append(pressure)
    for k, field in enumerate(fields):
        span = pl.ds(k * R, R)
        own[span, :] = field
        msg1[span, :] = field
        msg2[span, :] = field
    t_up, t_down = (trans[0, R - 1 : R, :], trans[1, 0:1, :])
    t_right, t_left = (trans[2], trans[3])
    for c in range(NC):
        put(par, 0, msg1, msg2, pl.ds(AX_EDGE + c, 1), couple0[c, 0, R - 1 : R, :], couple0[c, 0, 0:1, :])
        put(par, 0, msg1, msg2, pl.ds(AX_EDGE + NC + c, 1), t_up * weights[c, R - 1 : R, :], t_down * weights[c, 0:1, :])
    blank = jnp.zeros((24 - 2 * NC, L), jnp.float32)
    msg1[pl.ds(AX_EDGE + 2 * NC, 24 - 2 * NC), :] = blank
    msg2[pl.ds(AX_EDGE + 2 * NC, 24 - 2 * NC), :] = blank
    parts = []
    for c in range(NC):
        col, w = (couple0[c, 0], weights[c])
        parts += [(col, 0, c), (t_left * w, 0, NC + c), (col, L - 1, 2 * NC + c), (t_right * w, L - 1, 3 * NC + c)]
    packed = pack_columns(parts)
    cols[...] = packed
    msg1[pl.ds(AX_COL, R), :] = packed
    msg2[pl.ds(AX_COL, R), :] = packed


def inverse_kernel(diag, wells, out):
    boost = WELL_BOOST * wells[...].astype(jnp.float32)
    a = [[diag[i, j] + boost if i == j else diag[i, j] for j in range(NC)] for i in range(NC)]
    for k in range(NC):
        inv = 1.0 / a[k][k]
        a[k] = [inv if j == k else a[k][j] * inv for j in range(NC)]
        for i in range(NC):
            if i != k:
                factor = a[i][k]
                a[i] = [-factor * inv if j == k else a[i][j] - factor * a[k][j] for j in range(NC)]
    for i in range(NC):
        for j in range(NC):
            out[i, j] = a[i][j]


def ring_kernel(inverse, diag, couple, trans, wells, pack_left, pack_right, rows_up, rows_down):
    boost = WELL_BOOST * wells[...].astype(jnp.float32)
    entries = []
    for k in range(NC):
        for c in range(NC):
            total = couple[c, 0] * inverse[0, k]
            for m in range(1, NC):
                total = total + couple[c, m] * inverse[m, k]
            entries.append((total, 0, NC * k + c))
    for c in range(NC):
        entries.append((diag[c, 0] + boost if c == 0 else diag[c, 0], 0, RING_EFF + c))
        entries.append((couple[c, 0], 1, RING_NEXT + c))
    for d in range(4):
        entries.append((trans[d], 0, RING_TRANS + d))
    pack_left[...] = pack_columns([(v, inward, place) for v, inward, place in entries])
    pack_right[...] = pack_columns([(v, L - 1 - inward, place) for v, inward, place in entries])
    zero = jnp.zeros((1, L), jnp.float32)

    @pl.when(pl.program_id(0) == 0)
    def _():
        rows_down[pl.ds(RING_STATIC - 1, 1), :] = zero
        for v, inward, place in entries:
            rows_down[pl.ds(place, 1), :] = v[inward : inward + 1, :]

    @pl.when(pl.program_id(0) == R // 8 - 1)
    def _():
        rows_up[pl.ds(RING_STATIC - 1, 1), :] = zero
        for v, inward, place in entries:
            rows_up[pl.ds(place, 1), :] = v[7 - inward : 8 - inward, :]


def setup_middle_kernel(par, got1, got2, own, cols, couple0, trans, weights, _, msg1, msg2, ext, ext_cols, edges):
    rows, lanes = iotas((EX, L))

    def dots(span_of):
        total = jnp.zeros((1, L), jnp.float32)
        for c in range(NC):
            total = total + span_of(c)
        return -total

    ups, downs, tw_ups, tw_downs = ([], [], [], [])
    for c in range(NC):
        up, down = take(par, 0, got1, got2, pl.ds(AX_EDGE + c, 1))
        ups.append(up)
        downs.append(down)
        up, down = take(par, 0, got1, got2, pl.ds(AX_EDGE + NC + c, 1))
        tw_ups.append(up)
        tw_downs.append(down)
        edges[pl.ds(c, 1), :] = ups[c]
        edges[pl.ds(NC + c, 1), :] = downs[c]
        edges[pl.ds(2 * NC + c, 1), :] = tw_ups[c]
        edges[pl.ds(3 * NC + c, 1), :] = tw_downs[c]
    t_up, t_down = (trans[0, R - 1 : R, :], trans[1, 0:1, :])
    east_own = dots(lambda c: t_up * weights[c, R - 1 : R, :] * ups[c])
    west_own = dots(lambda c: t_down * weights[c, 0:1, :] * downs[c])
    west_up = dots(lambda c: tw_ups[c] * couple0[c, 0, R - 1 : R, :])
    east_down = dots(lambda c: tw_downs[c] * couple0[c, 0, 0:1, :])
    fields = []
    for k in range(6):
        up, down = take(par, 0, got1, got2, pl.ds(k * R, R))
        field = jnp.concatenate([own[pl.ds(k * R, R), :], up, down], axis=0)
        if k == CENTER:
            field = jnp.where(field == 0.0, 1.0, field)
        if k == EAST:
            field = jnp.where(rows == R - 1, east_own, jnp.where(rows == EX - 1, east_down, field))
        if k == WEST:
            field = jnp.where(rows == 0, west_own, jnp.where(rows == R, west_up, field))
        ext[k] = field
        fields.append(field)
    up, down = take(par, 0, got1, got2, pl.ds(AX_COL, R))
    packed = jnp.concatenate([cols[...], up, down], axis=0)
    ext_cols[...] = packed
    to_right = [lane_roll(f, HALO * (k % 4) + HALO) for k, f in enumerate(fields)]
    to_left = [lane_roll(f, HALO * (k % 4)) for k, f in enumerate(fields)]
    group = lanes // HALO

    def quad(parts):
        result = parts[-1]
        for g in range(len(parts) - 2, -1, -1):
            result = jnp.where(group == g, parts[g], result)
        return result

    put(par, 1, msg1, msg2, pl.ds(0, EX), quad(to_right[:4]), quad(to_left[:4]))
    put(
        par,
        1,
        msg1,
        msg2,
        pl.ds(EX, EX),
        quad(to_right[4:] + [lane_roll(packed, 64 - 2 * NC)]),
        quad(to_left[4:] + [lane_roll(packed, 64)]),
    )


def lane_sum(product, start):
    lanes = iotas(product.shape)[1]
    keep = jnp.logical_and(lanes >= start, lanes < start + NC)
    return jnp.sum(jnp.where(keep, product, 0.0), axis=1, keepdims=True)


def lane_pairs(values, step):
    lanes = iotas(values.shape)[1]
    return values + jnp.where((lanes // step) % 2 == 0, lane_roll(values, -step), lane_roll(values, step))


def even_rows(ref, half):
    return ref.at[half][pl.ds(0, ref.shape[1] // 2, stride=2), :]


def odd_rows(ref, half):
    return ref.at[half][pl.ds(1, ref.shape[1] // 2, stride=2), :]


def restrict(values, temp, step):
    result = []
    for half in range(2):
        temp[half] = values[half]
        result.append(lane_pairs(even_rows(temp, half) + odd_rows(temp, half), step))
    return result


def prolong(values, temp):
    result = []
    for half in range(2):
        count = values[half].shape[0]
        temp.at[half][pl.ds(0, count, stride=2), :] = values[half]
        temp.at[half][pl.ds(1, count, stride=2), :] = values[half]
        result.append(temp[half])
    return result


def coarsen_into(fine, coarse, temp, level):
    step = 2**level
    for half in range(2):
        lane_even = (iotas(fine.shape[2:])[1] // step) % 2 == 0
        center, east, west, north, south = (fine[d, half] for d in range(5))
        temp[half] = center + jnp.where(lane_even, north, south)
        total = even_rows(temp, half) + odd_rows(temp, half)
        temp[half] = east
        total = total + even_rows(temp, half)
        coarse[EAST, half] = lane_pairs(odd_rows(temp, half), step)
        temp[half] = west
        total = total + odd_rows(temp, half)
        coarse[WEST, half] = lane_pairs(even_rows(temp, half), step)
        total = lane_pairs(total, step)
        coarse[CENTER, half] = total
        coarse[SCALE, half] = RELAX / total
        temp[half] = jnp.where(lane_even, 0.0, north)
        coarse[NORTH, half] = lane_pairs(even_rows(temp, half) + odd_rows(temp, half), step)
        temp[half] = jnp.where(lane_even, south, 0.0)
        coarse[SOUTH, half] = lane_pairs(even_rows(temp, half) + odd_rows(temp, half), step)


def level_apply(values, coeffs, guarded, level):
    step = 2**level
    count = values[0].shape[0]
    lanes = iotas(values[0].shape)[1]
    right = [lane_roll(v, -step) for v in values]
    left = [lane_roll(v, step) for v in values]
    result = []
    for half in range(2):
        v = values[half]
        guarded[half, pl.ds(8, count), :] = v
        guarded[half, pl.ds(7, 1), :] = v[count - 1 : count]
        guarded[half, pl.ds(8 + count, 1), :] = v[0:1]
        result.append(
            coeffs[CENTER, half] * v
            + (
                coeffs[EAST, half] * guarded[half, pl.ds(9, count), :]
                + coeffs[WEST, half] * guarded[half, pl.ds(7, count), :]
                + coeffs[NORTH, half] * jnp.where(lanes >= L - step, right[1 - half], right[half])
                + coeffs[SOUTH, half] * jnp.where(lanes < step, left[1 - half], left[half])
            )
        )
    return result


def sweep(values, source, coeffs, guarded, level):
    applied = level_apply(values, coeffs, guarded, level)
    return [v + coeffs[SCALE, h] * (f - a) for h, (v, f, a) in enumerate(zip(values, source, applied))]


def difference(source, applied):
    return [f - a for f, a in zip(source, applied)]


def scaled(source, coeffs):
    return [coeffs[SCALE, h] * f for h, f in enumerate(source)]


def vcycle(source, levels, guards, temps):
    values0 = scaled(source, levels[0])
    source1 = restrict(difference(source, level_apply(values0, levels[0], guards[0], 0)), temps[0], 1)
    values1 = scaled(source1, levels[1])
    source2 = restrict(difference(source1, level_apply(values1, levels[1], guards[1], 1)), temps[1], 2)
    values2 = scaled(source2, levels[2])
    for _ in range(COARSE_SWEEPS - 1):
        values2 = sweep(values2, source2, levels[2], guards[2], 2)
    values1 = [v + e for v, e in zip(values1, prolong(values2, temps[1]))]
    values1 = sweep(values1, source1, levels[1], guards[1], 1)
    values0 = [v + e for v, e in zip(values0, prolong(values1, temps[0]))]
    return sweep(values0, source, levels[0], guards[0], 0)


def ghost_column(packed, start, to_lane, lane):
    return lane_roll(packed, to_lane - (start + lane))


def neighbour_sum(values, trans, guarded, up_row, down_row, right_col, left_col):
    lanes = iotas((R, L))[1]
    guarded[pl.ds(8, R), :] = values
    guarded[pl.ds(7, 1), :] = down_row
    guarded[pl.ds(8 + R, 1), :] = up_row
    north = jnp.where(lanes == L - 1, right_col, shifted(values, 1, 1))
    south = jnp.where(lanes == 0, left_col, shifted(values, 1, -1))
    return trans[0] * guarded[pl.ds(9, R), :] + trans[1] * guarded[pl.ds(7, R), :] + trans[2] * north + trans[3] * south


def ghost_rows(trans, up_row, down_row):
    rows, _ = iotas((R, L))
    return jnp.where(rows == R - 1, trans[0] * up_row, 0.0) + jnp.where(rows == 0, trans[1] * down_row, 0.0)


def ghost_columns(trans, right_col, left_col):
    _, lanes = iotas((R, L))
    return jnp.where(lanes == L - 1, trans[2] * right_col, 0.0) + jnp.where(lanes == 0, trans[3] * left_col, 0.0)


def one_step(pressure, vector, edges, col_right, col_left, diag, inverse, couple, trans, boost, z_out, around_rows):
    p = pressure[0][0:R]
    up_row, down_row = (pressure[0][R : R + 1], pressure[0][EX - 1 : EX])
    far = pressure[1][0:R]
    right_p, left_p = (lane_roll(far, L - 1), lane_roll(far, 1))
    second = []
    for c in range(NC):
        own = diag[c, 0] * p
        if c == 0:
            own = own + boost * p
        around = neighbour_sum(
            couple[c, 0] * p,
            trans,
            around_rows.at[c],
            edges[pl.ds(c, 1), :] * up_row,
            edges[pl.ds(NC + c, 1), :] * down_row,
            ghost_column(col_right, 64, L - 1, c) * right_p,
            ghost_column(col_left, 64, 0, c) * left_p,
        )
        second.append(vector[c] - (own - around))
    rest = []
    for c in range(NC):
        total = inverse[c, 0] * second[0]
        for k in range(1, NC):
            total = total + inverse[c, k] * second[k]
        rest.append(total)
        z_out[c] = total + p if c == 0 else total
    products = []
    for c in range(NC):
        product = couple[c, 0] * rest[0]
        for k in range(1, NC):
            product = product + couple[c, k] * rest[k]
        products.append(product)
    return products


def first_step_kernel(
    par, got1, got2, ext, ext_cols, edges, rhs, trans, weights, wells, diag, inverse, couple, rows_up, rows_down,
    msg1, msg2, z_out, partial, product, level0, level1, level2, cols_right, cols_left, pressure_part, product_cols,
    guard0, guard1, guard2, temp0, temp1, around_rows,
):
    rows, lanes = iotas((EX, L))
    right, left = take(par, 1, got1, got2, pl.ds(EX, EX))
    cols_right[...] = right
    cols_left[...] = left
    packed = ext_cols[...]
    north_own = -lane_sum(lane_roll(packed, 64 - 3 * NC) * right, 64)
    south_right = -lane_sum(lane_roll(packed, 64 - NC) * right, 64 + NC)
    south_own = -lane_sum(lane_roll(packed, 64 - NC) * left, 64)
    north_left = -lane_sum(lane_roll(packed, 64 + NC) * left, 64 + NC)
    right_four, left_four = take(par, 1, got1, got2, pl.ds(0, EX))
    source = None
    for k in range(6):
        from_right = lane_roll(right_four if k < 4 else right, -HALO * (k % 4))
        from_left = lane_roll(left_four if k < 4 else left, L - HALO - HALO * (k % 4))
        near = ext[k]
        far = jnp.where(lanes < HALO, from_right, jnp.where(lanes >= L - HALO, from_left, 0.0))
        if k == CENTER:
            far = jnp.where(far == 0.0, 1.0, far)
        if k == NORTH:
            near = jnp.where(lanes == L - 1, north_own, near)
            far = jnp.where(lanes == L - 1, north_left, far)
        if k == SOUTH:
            near = jnp.where(lanes == 0, south_own, near)
            far = jnp.where(lanes == 0, south_right, far)
        if k == 5:
            source = [near, far]
        else:
            level0[k, 0] = near
            level0[k, 1] = far
        if k == CENTER:
            level0[SCALE, 0] = RELAX / near
            level0[SCALE, 1] = RELAX / far
    levels = (level0, level1, level2)
    coarsen_into(level0, level1, temp0, 0)
    coarsen_into(level1, level2, temp1, 1)
    pressure = vcycle(source, levels, (guard0, guard1, guard2), (temp0, temp1))
    boost = WELL_BOOST * wells[...].astype(jnp.float32)
    vector = [rhs[c] for c in range(NC)]
    products = one_step(
        pressure, vector, edges, right[0:R], left[0:R], diag, inverse, couple, trans, boost, z_out,
        around_rows,
    )
    put(par, 0, msg1, msg2, pl.ds(BX_RING, RING_STATIC), rows_up[...], rows_down[...])
    weighed = jnp.zeros((R, L), jnp.float32)
    zero = jnp.zeros((1, L), jnp.float32)
    parts = []
    for c in range(NC):
        product[c] = products[c]
        value = -neighbour_sum(products[c], trans, around_rows.at[c], zero, zero, 0.0, 0.0)
        partial[c] = value
        weighed = weighed + weights[c] * value
        last, first = (slice(R - 1, R), slice(0, 1))
        put(par, 0, msg1, msg2, pl.ds(BX_EDGE + c, 1), products[c][last], products[c][first])
        put(par, 0, msg1, msg2, pl.ds(BX_RING + RING_VECTOR + c, 1), value[last], value[first])
        parts += [(products[c], 0, c), (products[c], L - 1, NC + c)]
    blank = jnp.zeros((16 - NC, L), jnp.float32)
    columns = pack_columns(parts)
    pressure_part[...] = weighed
    product_cols[...] = columns
    for msg in (msg1, msg2):
        msg[pl.ds(0, R), :] = weighed
        msg[pl.ds(BX_EDGE + NC, 16 - NC), :] = blank
        msg[pl.ds(BX_COL, R), :] = columns


def between_kernel(
    par, got1, got2, pressure_part, product_cols, product, edges, trans, weights, partial, pack_left, pack_right,
    msg1, msg2, ext, ext_cols, rows_out, vector_out,
):
    rows, lanes = iotas((EX, L))
    t_up, t_down = (trans[0, R - 1 : R, :], trans[1, 0:1, :])
    own_up, own_down, far_up, far_down = (jnp.zeros((1, L), jnp.float32) for _ in range(4))
    to_right, to_left = ([], [])
    for c in range(NC):
        up, down = take(par, 0, got1, got2, pl.ds(BX_EDGE + c, 1))
        rows_out[pl.ds(c, 1), :] = up
        rows_out[pl.ds(NC + c, 1), :] = down
        own_up = own_up + t_up * weights[c, R - 1 : R, :] * up
        own_down = own_down + t_down * weights[c, 0:1, :] * down
        far_up = far_up + edges[pl.ds(2 * NC + c, 1), :] * product[c, R - 1 : R, :]
        far_down = far_down + edges[pl.ds(3 * NC + c, 1), :] * product[c, 0:1, :]
        value = partial[c] - ghost_rows(trans, up, down)
        vector_out[c] = value
        to_right.append((value, L - 1, RING_VECTOR + c))
        to_left.append((value, 0, RING_VECTOR + c))
    up, down = take(par, 0, got1, got2, pl.ds(0, R))
    field = jnp.concatenate([pressure_part[...], up, down], axis=0)
    edge = jnp.where(rows == R - 1, own_up, 0.0) + jnp.where(rows == 0, own_down, 0.0)
    edge = edge + jnp.where(rows == R, far_up, 0.0) + jnp.where(rows == EX - 1, far_down, 0.0)
    field = field - edge
    ext[...] = field
    up, down = take(par, 0, got1, got2, pl.ds(BX_COL, R))
    packed = jnp.concatenate([product_cols[...], up, down], axis=0)
    ext_cols[...] = packed
    near = lanes < HALO
    put(
        par, 1, msg1, msg2, pl.ds(0, EX),
        jnp.where(near, lane_roll(field, HALO), lane_roll(packed, HALO - NC)),
        jnp.where(near, field, lane_roll(packed, HALO)),
    )
    fixed = iotas((R, L))[1] < RING_VECTOR
    put(
        par, 1, msg1, msg2, pl.ds(EX, R),
        jnp.where(fixed, pack_right[...], pack_columns(to_right)),
        jnp.where(fixed, pack_left[...], pack_columns(to_left)),
    )


def row_ring(ring, outward, inward, pressure, row, out_row, own_row, edge_cols, product_row, couple_row, corners, old_corners):
    lanes = iotas((1, L))[1]
    near, far = pressure
    p, beyond = (near[row : row + 1], far[row : row + 1])
    p_right, p_left = (beyond[:, 0:1], beyond[:, L - 1 : L])
    p_out, p_own = (near[out_row : out_row + 1], near[own_row : own_row + 1])
    t_out, t_in = (ring(RING_TRANS + outward), ring(RING_TRANS + inward))
    t_right, t_left = (ring(RING_TRANS + 2), ring(RING_TRANS + 3))
    second = []
    for c in range(NC):
        beside = edge_cols(c) * p
        old_right, old_left = (ghost_column(old_corners[0], 64, L - 1, c), ghost_column(old_corners[1], 64, 0, c))
        new_right, new_left = (ghost_column(corners[0], HALO, L - 1, c), ghost_column(corners[1], HALO, 0, c))
        north = jnp.where(lanes == L - 1, old_right * p_right, shifted(beside, 1, 1))
        south = jnp.where(lanes == 0, old_left * p_left, shifted(beside, 1, -1))
        value = ring(RING_VECTOR + c) - t_in * product_row(c)
        value = value - jnp.where(lanes == L - 1, t_right * new_right, 0.0)
        value = value - jnp.where(lanes == 0, t_left * new_left, 0.0)
        second.append(
            value
            - ring(RING_EFF + c) * p
            + t_out * (ring(RING_NEXT + c) * p_out)
            + t_in * (couple_row(c) * p_own)
            + t_right * north
            + t_left * south
        )
    return second


def column_ring(pack, outward, inward, p, p_out, p_own, p_up, p_down, own_couple, own_product, beside_up, beside_down):
    lanes = iotas((R, L))[1]

    def trans(d):
        return pack[:, RING_TRANS + d : RING_TRANS + d + 1]

    second = (
        lane_roll(pack, -RING_VECTOR)
        - trans(inward) * own_product
        - lane_roll(pack, -RING_EFF) * p
        + trans(outward) * (lane_roll(pack, -RING_NEXT) * p_out)
        + trans(inward) * (own_couple * p_own)
        + trans(0) * (beside_up * p_up)
        + trans(1) * (beside_down * p_down)
    )
    spread = jnp.zeros((R, L), jnp.float32)
    for k in range(NC):
        within = jnp.logical_and(lanes >= NC * k, lanes < NC * k + NC)
        spread = jnp.where(within, second[:, k : k + 1], spread)
    terms = pack * spread
    total = terms
    for k in range(1, NC):
        total = total + lane_roll(terms, -NC * k)
    return total


def second_step_kernel(
    par, got1, got2, gotx1, gotx2, ext, ext_cols, rows_in, setup_cols, cols_right, cols_left, edges,
    level0, level1, level2, partial,
    product, rhs, trans, wells, diag, inverse, couple,
    z_out, dots, ring_up, ring_down, guard0, guard1, guard2, temp0, temp1, around_rows,
):
    rows, lanes = iotas((EX, L))
    right, left = take(par, 1, got1, got2, pl.ds(0, EX))
    packed, tw = (ext_cols[...], setup_cols[...])
    old_right, old_left = (cols_right[...], cols_left[...])
    own_right = lane_sum(lane_roll(tw, HALO - 3 * NC) * right, HALO)
    own_left = lane_sum(lane_roll(tw, HALO - NC) * left, HALO)
    far_right = lane_sum(old_right * lane_roll(packed, 64), 64 + NC)
    far_left = lane_sum(old_left * lane_roll(packed, 64 + NC), 64 + NC)
    near = ext[...] - jnp.where(lanes == L - 1, own_right, 0.0) - jnp.where(lanes == 0, own_left, 0.0)
    far = jnp.where(
        lanes < HALO, right, jnp.where(lanes >= L - HALO, lane_roll(left, L - HALO), 0.0)
    )
    far = far - jnp.where(lanes == 0, far_right, 0.0) - jnp.where(lanes == L - 1, far_left, 0.0)
    pressure = vcycle([near, far], (level0, level1, level2), (guard0, guard1, guard2), (temp0, temp1))
    vector = []
    for c in range(NC):
        columns = ghost_columns(
            trans, ghost_column(right[0:R], HALO, L - 1, c), ghost_column(left[0:R], HALO, 0, c)
        )
        vector.append(partial[c] - columns)
    boost = WELL_BOOST * wells[...].astype(jnp.float32)
    products = one_step(
        pressure, vector, edges, old_right[0:R], old_left[0:R], diag, inverse, couple, trans, boost, z_out,
        around_rows,
    )
    up, down = take(par, 0, gotx1, gotx2, pl.ds(BX_RING, 112))
    ring_up[...] = up
    ring_down[...] = down
    second_up = row_ring(
        lambda i: ring_up[pl.ds(i, 1), :], 0, 1, pressure, R, R + 1, R - 1,
        lambda c: edges[pl.ds(c, 1), :], lambda c: product[c, R - 1 : R, :], lambda c: couple[c, 0, R - 1 : R, :],
        (right[R : R + 1], left[R : R + 1]), (old_right[R : R + 1], old_left[R : R + 1]),
    )
    second_down = row_ring(
        lambda i: ring_down[pl.ds(i, 1), :], 1, 0, pressure, EX - 1, EX - 2, 0,
        lambda c: edges[pl.ds(NC + c, 1), :], lambda c: product[c, 0:1, :], lambda c: couple[c, 0, 0:1, :],
        (right[EX - 1 : EX], left[EX - 1 : EX]), (old_right[EX - 1 : EX], old_left[EX - 1 : EX]),
    )
    product_up = ring_up[pl.ds(0, NC), :] * second_up[0]
    product_down = ring_down[pl.ds(0, NC), :] * second_down[0]
    for k in range(1, NC):
        product_up = product_up + ring_up[pl.ds(NC * k, NC), :] * second_up[k]
        product_down = product_down + ring_down[pl.ds(NC * k, NC), :] * second_down[k]
    pack_right, pack_left = take(par, 1, got1, got2, pl.ds(EX, R))
    far_p = pressure[1]
    far_up, far_down = (shifted(far_p, 0, 1)[0:R], shifted(far_p, 0, -1)[0:R])
    far_p, near_p = (far_p[0:R], pressure[0][0:R])
    right_cols = column_ring(
        pack_right, 2, 3, far_p[:, 0:1], far_p[:, 1:2], near_p[:, L - 1 : L], far_up[:, 0:1], far_down[:, 0:1],
        lane_roll(tw[0:R], -2 * NC), lane_roll(packed[0:R], -NC),
        lane_roll(shifted(old_right, 0, 1)[0:R], -64), lane_roll(shifted(old_right, 0, -1)[0:R], -64),
    )
    left_cols = column_ring(
        pack_left, 3, 2, far_p[:, L - 1 : L], far_p[:, L - 2 : L - 1], near_p[:, 0:1], far_up[:, L - 1 : L],
        far_down[:, L - 1 : L], tw[0:R], packed[0:R],
        lane_roll(shifted(old_left, 0, 1)[0:R], -64), lane_roll(shifted(old_left, 0, -1)[0:R], -64),
    )
    sums = [jnp.zeros((R, L), jnp.float32) for _ in range(6)]
    for c in range(NC):
        two = -neighbour_sum(
            products[c], trans, around_rows.at[c], product_up[c : c + 1], product_down[c : c + 1],
            ghost_column(right_cols, 0, L - 1, c), ghost_column(left_cols, 0, 0, c),
        )
        zero, one = (rhs[c], vector[c])
        for k, (a, b) in enumerate(((zero, zero), (zero, one), (one, one), (zero, two), (one, two), (two, two))):
            sums[k] = sums[k] + a * b
    lane = iotas((1, L))[1]
    row = jnp.zeros((1, L), jnp.float32)
    for k, total in enumerate(sums):
        row = jnp.where(lane == k, jnp.sum(total, keepdims=True), row)
    dots[...] = jnp.broadcast_to(row, dots.shape)


def finish_kernel(gathered, z_one, z_two, out, estimate):
    row = jnp.sum(gathered[...], axis=0, keepdims=True)
    lanes = iotas((1, L))[1]
    g00, g01, g11, g02, g12, g22 = (
        jnp.sum(jnp.where(lanes == k, row, 0.0), axis=1, keepdims=True) for k in range(6)
    )
    beta = jnp.sqrt(g00)
    shift = g01 / g00
    h00 = 1.0 + shift
    length2 = g11 - shift * g01
    length = jnp.sqrt(length2)
    h10 = length / beta
    h01 = (g02 - shift * g01) / (beta * length)
    above = (g12 - shift * g02 - shift * (g11 - shift * g01)) / length2
    h11 = 1.0 + above
    h21 = jnp.sqrt((g22 - 2.0 * shift * g12 + shift * shift * g11) / length2 - h01 * h01 - above * above)
    radius0 = jnp.sqrt(h00 * h00 + h10 * h10)
    cos0, sin0 = (h00 / radius0, h10 / radius0)
    r01 = cos0 * h01 + sin0 * h11
    mid = cos0 * h11 - sin0 * h01
    radius1 = jnp.sqrt(mid * mid + h21 * h21)
    cos1, sin1 = (mid / radius1, h21 / radius1)
    rhs0, rhs1 = (cos0 * beta, -sin0 * beta)
    estimate[...] = jnp.abs(sin1 * rhs1)
    y1 = cos1 * rhs1 / radius1
    y0 = (rhs0 - r01 * y1) / radius0
    weight1 = y1 / length
    weight0 = y0 / beta - weight1 * shift
    for c in range(NC):
        out[c] = weight0 * z_one[c] + weight1 * z_two[c]


VMEM = functools.partial(pl.BlockSpec, memory_space=pltpu.VMEM)
HBM = functools.partial(pl.BlockSpec, memory_space=pltpu.HBM)
ANY = functools.partial(pl.BlockSpec, memory_space=pl.ANY)


def shape(*dims):
    return jax.ShapeDtypeStruct(dims, jnp.float32)


def call(kernel, in_specs, outs, scratch=(), cost=20_000_000):
    return pl.pallas_call(
        kernel,
        in_specs=list(in_specs),
        out_specs=[VMEM()] * len(outs),
        out_shape=list(outs),
        scratch_shapes=list(scratch),
        cost_estimate=pl.CostEstimate(flops=cost, bytes_accessed=1_000_000, transcendentals=0),
        compiler_params=pltpu.CompilerParams(vmem_limit_bytes=30 * 1024 * 1024),
    )


def swap(first, second, axis):
    peers = lax.axis_size(axis)
    pairs = [(i, i ^ 1) for i in range(peers) if i ^ 1 < peers]
    others = [(i, ((i + 1) ^ 1) - 1) for i in range(1, peers) if ((i + 1) ^ 1) - 1 < peers]
    return (lax.ppermute(first, axis, others), lax.ppermute(second, axis, pairs))


def on_device(right_side, diag_blocks, couple_blocks, transmissibility, pressure_weights, well_mask):
    par = jnp.stack([1 - (lax.axis_index("gx") & 1), 1 - (lax.axis_index("gy") & 1)]).astype(jnp.int32)
    par = jnp.broadcast_to(par[:, None], (2, L))
    column = pl.BlockSpec((NC, 1, R, L), lambda i: (0, 0, 0, 0))

    def whole(*dims):
        return pl.BlockSpec(dims, lambda i: (0,) * len(dims))

    msg_a1, msg_a2, own, cols = call(
        setup_kernel,
        [VMEM()] + [HBM()] * 6,
        [shape(AX_ROWS, L), shape(AX_ROWS, L), shape(6 * R, L), shape(R, L)],
        [
            pltpu.VMEM((NC, R, L), jnp.float32),
            pltpu.VMEM((NC, 1, R, L), jnp.float32),
            pltpu.VMEM((NC, 1, R, L), jnp.float32),
            pltpu.VMEM((4, R, L), jnp.float32),
            pltpu.VMEM((NC, R, L), jnp.float32),
            pltpu.VMEM((R, L), jnp.int32),
            pltpu.SemaphoreType.DMA((6,)),
        ],
    )(
        par,
        *(
            pltpu.with_memory_space_constraint(x, pltpu.HBM)
            for x in (right_side, diag_blocks, couple_blocks, transmissibility, pressure_weights, well_mask)
        ),
    )

    got_a1, got_a2 = swap(msg_a1, msg_a2, "gx")

    slab = pl.BlockSpec((NC, NC, 8, L), lambda i: (0, 0, i, 0))
    strip = pl.BlockSpec((8, L), lambda i: (i, 0))
    inverse = pl.pallas_call(
        inverse_kernel,
        grid=(R // 8,),
        in_specs=[slab, strip],
        out_specs=slab,
        out_shape=shape(NC, NC, R, L),
        cost_estimate=pl.CostEstimate(flops=20_000_000, bytes_accessed=2_700_000, transcendentals=0),
        compiler_params=pltpu.CompilerParams(vmem_limit_bytes=30 * 1024 * 1024),
    )(diag_blocks, well_mask)
    pack_left, pack_right, rows_up, rows_down = pl.pallas_call(
        ring_kernel,
        grid=(R // 8,),
        in_specs=[slab, slab, slab, pl.BlockSpec((4, 8, L), lambda i: (0, i, 0)), strip],
        out_specs=[strip, strip, whole(RING_STATIC, L), whole(RING_STATIC, L)],
        out_shape=[shape(R, L), shape(R, L), shape(RING_STATIC, L), shape(RING_STATIC, L)],
        cost_estimate=pl.CostEstimate(flops=20_000_000, bytes_accessed=2_700_000, transcendentals=0),
        compiler_params=pltpu.CompilerParams(vmem_limit_bytes=30 * 1024 * 1024),
    )(inverse, diag_blocks, couple_blocks, transmissibility, well_mask)

    msg_y1, msg_y2, ext, ext_cols, edges = pl.pallas_call(
        setup_middle_kernel,
        grid=(1,),
        in_specs=[
            VMEM(), whole(AX_ROWS, L), whole(AX_ROWS, L), whole(6 * R, L), whole(R, L), column,
            whole(4, R, L), whole(NC, R, L), ANY(),
        ],
        out_specs=[whole(AY_ROWS, L), whole(AY_ROWS, L), whole(6, EX, L), whole(EX, L), whole(4 * NC, L)],
        out_shape=[shape(AY_ROWS, L), shape(AY_ROWS, L), shape(6, EX, L), shape(EX, L), shape(4 * NC, L)],
        compiler_params=pltpu.CompilerParams(vmem_limit_bytes=30 * 1024 * 1024),
    )(par, got_a1, got_a2, own, cols, couple_blocks, transmissibility, pressure_weights, inverse)

    got_y1, got_y2 = swap(msg_y1, msg_y2, "gy")

    fields = shape(NC, R, L)
    work = [
        pltpu.VMEM(dims, jnp.float32)
        for dims in (
            (2, EX + 16, L), (2, EX // 2 + 16, L), (2, EX // 4 + 16, L), (2, EX, L), (2, EX // 2, L), (NC, R + 16, L),
        )
    ]
    msg_b1, msg_b2, z_one, partial, product, level0, level1, level2, cols_right, cols_left, pressure_part, product_cols = call(
        first_step_kernel,
        [VMEM()] + [VMEM()] * 14,
        [
            shape(BX_ROWS, L), shape(BX_ROWS, L), fields, fields, fields, shape(6, 2, EX, L),
            shape(6, 2, EX // 2, L), shape(6, 2, EX // 4, L),
            shape(EX, L), shape(EX, L), shape(R, L), shape(R, L),
        ],
        work,
    )(
        par, got_y1, got_y2, ext, ext_cols, edges, right_side, transmissibility, pressure_weights, well_mask,
        diag_blocks, inverse, couple_blocks, rows_up, rows_down,
    )

    got_b1, got_b2 = swap(msg_b1, msg_b2, "gx")
    msg_c1, msg_c2, ext_b, ext_cols_b, rows_b, vector_b = call(
        between_kernel,
        [VMEM()] + [VMEM()] * 11,
        [shape(EX + R, L), shape(EX + R, L), shape(EX, L), shape(EX, L), shape(2 * NC, L), fields],
    )(
        par, got_b1, got_b2, pressure_part, product_cols, product, edges, transmissibility, pressure_weights,
        partial, pack_left, pack_right,
    )
    got_c1, got_c2 = swap(msg_c1, msg_c2, "gy")

    devices = lax.axis_size("gx") * lax.axis_size("gy")
    z_two, local = call(
        second_step_kernel,
        [VMEM()] * 23,
        [fields, shape(devices, L)],
        [pltpu.VMEM((112, L), jnp.float32), pltpu.VMEM((112, L), jnp.float32)] + work,
    )(
        par, got_c1, got_c2, got_b1, got_b2, ext_b, ext_cols_b, rows_b, ext_cols, cols_right, cols_left, edges,
        level0, level1, level2, vector_b, product, right_side, transmissibility, well_mask, diag_blocks, inverse, couple_blocks,
    )
    gathered = lax.all_to_all(local, ("gx", "gy"), 0, 0, tiled=True)
    answer, estimate = call(finish_kernel, [VMEM()] * 3, [fields, shape(1, 1)])(gathered, z_one, z_two)
    return (answer, estimate.reshape(()))


def solution(mesh):
    return jax.shard_map(
        on_device,
        mesh=mesh,
        in_specs=(
            P(None, "gx", "gy"),
            P(None, None, "gx", "gy"),
            P(None, None, "gx", "gy"),
            P(None, "gx", "gy"),
            P(None, "gx", "gy"),
            P("gx", "gy"),
        ),
        out_specs=(P(None, "gx", "gy"), P()),
        check_vma=False,
    )
```

```python
import functools

import jax
import jax.numpy as jnp
from jax import lax
from jax.experimental import pallas as pl
from jax.experimental.pallas import tpu as pltpu
from jax.sharding import PartitionSpec as P

NC = 9
COARSE_SWEEPS = 6
RELAX = 0.8
WELL_BOOST = 8.0

R, L = 32, 128
HALO = 32
EX, EY = 3 * R, 2 * L

AX_EDGE = 6 * R
AX_COL = AX_EDGE + 24
AX_ROWS = AX_COL + 16
AY_ROWS = 2 * EX
BX_EDGE = R
BX_COL = BX_EDGE + 16
BX_RING = BX_COL + 8
BX_ROWS = BX_RING + 112
RING_EFF, RING_NEXT, RING_TRANS, RING_VECTOR, RING_STATIC = 81, 90, 99, 103, 104

CENTER, EAST, WEST, NORTH, SOUTH, SCALE = range(6)


def iotas(shape):
    return (lax.broadcasted_iota(jnp.int32, shape, 0), lax.broadcasted_iota(jnp.int32, shape, 1))


def shifted(values, axis, step):
    return pltpu.roll(values, (-step) % values.shape[axis], axis)


def lane_roll(values, shift):
    shift = shift % values.shape[1]
    return values if shift == 0 else pltpu.roll(values, shift, 1)


def first_is_up(par_ref, which, shape):
    return jnp.broadcast_to(par_ref[which : which + 1, :], shape) == 0


def put(par_ref, which, first, second, rows, up, down):
    mask = first_is_up(par_ref, which, up.shape)
    first[rows, :] = jnp.where(mask, up, down)
    second[rows, :] = jnp.where(mask, down, up)


def take(par_ref, which, first, second, rows):
    one, two = (first[rows, :], second[rows, :])
    mask = first_is_up(par_ref, which, one.shape)
    return (jnp.where(mask, one, two), jnp.where(mask, two, one))


def pack_columns(parts):
    shape = parts[0][0].shape
    lanes = iotas(shape)[1]
    packed = jnp.zeros(shape, jnp.float32)
    for values, lane, target in parts:
        packed = jnp.where(lanes == target, lane_roll(values, target - lane), packed)
    return packed


def fold(values, width, rows, per_group):
    lanes = iotas((rows, L))[1]
    blocks = []
    for start in range(0, values.shape[0], rows * per_group):
        block = values[start : start + rows]
        for g in range(1, per_group):
            first = start + g * rows
            if first < values.shape[0]:
                block = jnp.where(lanes >= g * width, lane_roll(values[first : first + rows], g * width), block)
        blocks.append(block)
    return blocks[0] if len(blocks) == 1 else jnp.concatenate(blocks, axis=0)


def unfold(folded, width, rows, per_group, total):
    parts = []
    for g in range(total // rows):
        block = folded[g // per_group * rows : (g // per_group + 1) * rows]
        parts.append(lane_roll(block, -(g % per_group) * width))
    return jnp.concatenate(parts, axis=0)


def setup_kernel(
    par, rhs_hbm, diag_hbm, couple_hbm, trans_hbm, weights_hbm, wells_hbm, msg1, msg2, own, cols,
    rhs, diag0, couple0, trans, weights, wells, sems,
):
    pairs = (
        (weights_hbm, weights),
        (couple_hbm.at[:, 0:1], couple0),
        (trans_hbm, trans),
        (diag_hbm.at[:, 0:1], diag0),
        (rhs_hbm, rhs),
        (wells_hbm, wells),
    )
    copies = [pltpu.make_async_copy(a, b, sems.at[i]) for i, (a, b) in enumerate(pairs)]
    for copy in copies:
        copy.start()
    for copy in copies[:3]:
        copy.wait()
    rows, lanes = iotas((R, L))
    links = [jnp.zeros((R, L), jnp.float32) for _ in range(4)]
    for c in range(NC):
        w, col = (weights[c], couple0[c, 0])
        for d, (axis, step) in enumerate(((0, 1), (0, -1), (1, 1), (1, -1))):
            links[d] = links[d] + w * shifted(col, axis, step)
    inside = (rows != R - 1, rows != 0, lanes != L - 1, lanes != 0)
    fields = [None] + [jnp.where(inside[d], -trans[d] * links[d], 0.0) for d in range(4)] + [None]
    t_up, t_down = (trans[0, R - 1 : R, :], trans[1, 0:1, :])
    t_right, t_left = (trans[2], trans[3])
    for c in range(NC):
        put(par, 0, msg1, msg2, pl.ds(AX_EDGE + c, 1), couple0[c, 0, R - 1 : R, :], couple0[c, 0, 0:1, :])
        put(par, 0, msg1, msg2, pl.ds(AX_EDGE + NC + c, 1), t_up * weights[c, R - 1 : R, :], t_down * weights[c, 0:1, :])
    blank = jnp.zeros((24 - 2 * NC, L), jnp.float32)
    msg1[pl.ds(AX_EDGE + 2 * NC, 24 - 2 * NC), :] = blank
    msg2[pl.ds(AX_EDGE + 2 * NC, 24 - 2 * NC), :] = blank
    parts = []
    for c in range(NC):
        col, w = (couple0[c, 0], weights[c])
        parts += [(col, 0, c), (t_left * w, 0, NC + c), (col, L - 1, 2 * NC + c), (t_right * w, L - 1, 3 * NC + c)]
    packed = pack_columns(parts)
    cols[...] = packed
    folded = fold(packed, 4 * NC, 8, 3)
    msg1[pl.ds(AX_COL, 16), :] = folded
    msg2[pl.ds(AX_COL, 16), :] = folded
    for copy in copies[3:]:
        copy.wait()
    center = WELL_BOOST * wells[...].astype(jnp.float32) * weights[0]
    pressure = jnp.zeros((R, L), jnp.float32)
    for c in range(NC):
        center = center + weights[c] * diag0[c, 0]
        pressure = pressure + weights[c] * rhs[c]
    fields[0], fields[5] = (center, pressure)
    for k, field in enumerate(fields):
        span = pl.ds(k * R, R)
        own[span, :] = field
        msg1[span, :] = field
        msg2[span, :] = field


def inverse_kernel(diag, wells, out):
    boost = WELL_BOOST * wells[...].astype(jnp.float32)
    a = [[diag[i, j] + boost if i == j else diag[i, j] for j in range(NC)] for i in range(NC)]
    for k in range(NC):
        inv = 1.0 / a[k][k]
        a[k] = [inv if j == k else a[k][j] * inv for j in range(NC)]
        for i in range(NC):
            if i != k:
                factor = a[i][k]
                a[i] = [-factor * inv if j == k else a[i][j] - factor * a[k][j] for j in range(NC)]
    for i in range(NC):
        for j in range(NC):
            out[i, j] = a[i][j]


def ring_kernel(inverse, diag, couple, trans, wells, pack_left, pack_right, rows_up, rows_down):
    boost = WELL_BOOST * wells[...].astype(jnp.float32)
    entries = []
    for k in range(NC):
        for c in range(NC):
            total = couple[c, 0] * inverse[0, k]
            for m in range(1, NC):
                total = total + couple[c, m] * inverse[m, k]
            entries.append((total, 0, NC * k + c))
    for c in range(NC):
        entries.append((diag[c, 0] + boost if c == 0 else diag[c, 0], 0, RING_EFF + c))
        entries.append((couple[c, 0], 1, RING_NEXT + c))
    for d in range(4):
        entries.append((trans[d], 0, RING_TRANS + d))
    pack_left[...] = pack_columns([(v, inward, place) for v, inward, place in entries])
    pack_right[...] = pack_columns([(v, L - 1 - inward, place) for v, inward, place in entries])
    zero = jnp.zeros((1, L), jnp.float32)

    @pl.when(pl.program_id(0) == 0)
    def _():
        rows_down[pl.ds(RING_STATIC - 1, 1), :] = zero
        for v, inward, place in entries:
            rows_down[pl.ds(place, 1), :] = v[inward : inward + 1, :]

    @pl.when(pl.program_id(0) == R // 8 - 1)
    def _():
        rows_up[pl.ds(RING_STATIC - 1, 1), :] = zero
        for v, inward, place in entries:
            rows_up[pl.ds(place, 1), :] = v[7 - inward : 8 - inward, :]


def setup_middle_kernel(par, got1, got2, own, cols, couple0, trans, weights, _, msg1, msg2, ext, ext_cols, edges):
    rows, lanes = iotas((EX, L))

    def dots(span_of):
        total = jnp.zeros((1, L), jnp.float32)
        for c in range(NC):
            total = total + span_of(c)
        return -total

    ups, downs, tw_ups, tw_downs = ([], [], [], [])
    for c in range(NC):
        up, down = take(par, 0, got1, got2, pl.ds(AX_EDGE + c, 1))
        ups.append(up)
        downs.append(down)
        up, down = take(par, 0, got1, got2, pl.ds(AX_EDGE + NC + c, 1))
        tw_ups.append(up)
        tw_downs.append(down)
        edges[pl.ds(c, 1), :] = ups[c]
        edges[pl.ds(NC + c, 1), :] = downs[c]
        edges[pl.ds(2 * NC + c, 1), :] = tw_ups[c]
        edges[pl.ds(3 * NC + c, 1), :] = tw_downs[c]
    t_up, t_down = (trans[0, R - 1 : R, :], trans[1, 0:1, :])
    east_own = dots(lambda c: t_up * weights[c, R - 1 : R, :] * ups[c])
    west_own = dots(lambda c: t_down * weights[c, 0:1, :] * downs[c])
    west_up = dots(lambda c: tw_ups[c] * couple0[c, 0, R - 1 : R, :])
    east_down = dots(lambda c: tw_downs[c] * couple0[c, 0, 0:1, :])
    fields = []
    for k in range(6):
        up, down = take(par, 0, got1, got2, pl.ds(k * R, R))
        field = jnp.concatenate([own[pl.ds(k * R, R), :], up, down], axis=0)
        if k == CENTER:
            field = jnp.where(field == 0.0, 1.0, field)
        if k == EAST:
            field = jnp.where(rows == R - 1, east_own, jnp.where(rows == EX - 1, east_down, field))
        if k == WEST:
            field = jnp.where(rows == 0, west_own, jnp.where(rows == R, west_up, field))
        ext[k] = field
        fields.append(field)
    up, down = (unfold(v, 4 * NC, 8, 3, R) for v in take(par, 0, got1, got2, pl.ds(AX_COL, 16)))
    packed = jnp.concatenate([cols[...], up, down], axis=0)
    ext_cols[...] = packed
    to_right = [lane_roll(f, HALO * (k % 4) + HALO) for k, f in enumerate(fields)]
    to_left = [lane_roll(f, HALO * (k % 4)) for k, f in enumerate(fields)]
    group = lanes // HALO

    def quad(parts):
        result = parts[-1]
        for g in range(len(parts) - 2, -1, -1):
            result = jnp.where(group == g, parts[g], result)
        return result

    put(par, 1, msg1, msg2, pl.ds(0, EX), quad(to_right[:4]), quad(to_left[:4]))
    put(
        par,
        1,
        msg1,
        msg2,
        pl.ds(EX, EX),
        quad(to_right[4:] + [lane_roll(packed, 64 - 2 * NC)]),
        quad(to_left[4:] + [lane_roll(packed, 64)]),
    )


def lane_sum(product, start):
    lanes = iotas(product.shape)[1]
    keep = jnp.logical_and(lanes >= start, lanes < start + NC)
    return jnp.sum(jnp.where(keep, product, 0.0), axis=1, keepdims=True)


def lane_pairs(values, step):
    lanes = iotas(values.shape)[1]
    return values + jnp.where((lanes // step) % 2 == 0, lane_roll(values, -step), lane_roll(values, step))


def even_rows(ref, half):
    return ref.at[half][pl.ds(0, ref.shape[1] // 2, stride=2), :]


def odd_rows(ref, half):
    return ref.at[half][pl.ds(1, ref.shape[1] // 2, stride=2), :]


def restrict(values, temp, step):
    result = []
    for half in range(2):
        temp[half] = values[half]
        result.append(lane_pairs(even_rows(temp, half) + odd_rows(temp, half), step))
    return result


def prolong(values, temp):
    result = []
    for half in range(2):
        count = values[half].shape[0]
        temp.at[half][pl.ds(0, count, stride=2), :] = values[half]
        temp.at[half][pl.ds(1, count, stride=2), :] = values[half]
        result.append(temp[half])
    return result


def coarsen_into(fine, coarse, temp, level):
    step = 2**level
    for half in range(2):
        lane_even = (iotas(fine.shape[2:])[1] // step) % 2 == 0
        center, east, west, north, south = (fine[d, half] for d in range(5))
        temp[half] = center + jnp.where(lane_even, north, south)
        total = even_rows(temp, half) + odd_rows(temp, half)
        temp[half] = east
        total = total + even_rows(temp, half)
        coarse[EAST, half] = lane_pairs(odd_rows(temp, half), step)
        temp[half] = west
        total = total + odd_rows(temp, half)
        coarse[WEST, half] = lane_pairs(even_rows(temp, half), step)
        total = lane_pairs(total, step)
        coarse[CENTER, half] = total
        coarse[SCALE, half] = RELAX / total
        temp[half] = jnp.where(lane_even, 0.0, north)
        coarse[NORTH, half] = lane_pairs(even_rows(temp, half) + odd_rows(temp, half), step)
        temp[half] = jnp.where(lane_even, south, 0.0)
        coarse[SOUTH, half] = lane_pairs(even_rows(temp, half) + odd_rows(temp, half), step)


def level_apply(values, coeffs, guarded, level):
    step = 2**level
    count = values[0].shape[0]
    lanes = iotas(values[0].shape)[1]
    right = [lane_roll(v, -step) for v in values]
    left = [lane_roll(v, step) for v in values]
    result = []
    for half in range(2):
        v = values[half]
        guarded[half, pl.ds(8, count), :] = v
        guarded[half, pl.ds(7, 1), :] = v[count - 1 : count]
        guarded[half, pl.ds(8 + count, 1), :] = v[0:1]
        result.append(
            coeffs[CENTER, half] * v
            + (
                coeffs[EAST, half] * guarded[half, pl.ds(9, count), :]
                + coeffs[WEST, half] * guarded[half, pl.ds(7, count), :]
                + coeffs[NORTH, half] * jnp.where(lanes >= L - step, right[1 - half], right[half])
                + coeffs[SOUTH, half] * jnp.where(lanes < step, left[1 - half], left[half])
            )
        )
    return result


def sweep(values, source, coeffs, guarded, level):
    applied = level_apply(values, coeffs, guarded, level)
    return [v + coeffs[SCALE, h] * (f - a) for h, (v, f, a) in enumerate(zip(values, source, applied))]


def difference(source, applied):
    return [f - a for f, a in zip(source, applied)]


def scaled(source, coeffs):
    return [coeffs[SCALE, h] * f for h, f in enumerate(source)]


def vcycle(source, levels, guards, temps):
    values0 = scaled(source, levels[0])
    source1 = restrict(difference(source, level_apply(values0, levels[0], guards[0], 0)), temps[0], 1)
    values1 = scaled(source1, levels[1])
    source2 = restrict(difference(source1, level_apply(values1, levels[1], guards[1], 1)), temps[1], 2)
    values2 = scaled(source2, levels[2])
    for _ in range(COARSE_SWEEPS - 1):
        values2 = sweep(values2, source2, levels[2], guards[2], 2)
    values1 = [v + e for v, e in zip(values1, prolong(values2, temps[1]))]
    values1 = sweep(values1, source1, levels[1], guards[1], 1)
    values0 = [v + e for v, e in zip(values0, prolong(values1, temps[0]))]
    return sweep(values0, source, levels[0], guards[0], 0)


def ghost_column(packed, start, to_lane, lane):
    return lane_roll(packed, to_lane - (start + lane))


def neighbour_sum(values, trans, guarded, up_row, down_row, right_col, left_col):
    lanes = iotas((R, L))[1]
    guarded[pl.ds(8, R), :] = values
    guarded[pl.ds(7, 1), :] = down_row
    guarded[pl.ds(8 + R, 1), :] = up_row
    north = jnp.where(lanes == L - 1, right_col, shifted(values, 1, 1))
    south = jnp.where(lanes == 0, left_col, shifted(values, 1, -1))
    return trans[0] * guarded[pl.ds(9, R), :] + trans[1] * guarded[pl.ds(7, R), :] + trans[2] * north + trans[3] * south


def ghost_rows(trans, up_row, down_row):
    rows, _ = iotas((R, L))
    return jnp.where(rows == R - 1, trans[0] * up_row, 0.0) + jnp.where(rows == 0, trans[1] * down_row, 0.0)


def ghost_columns(trans, right_col, left_col):
    _, lanes = iotas((R, L))
    return jnp.where(lanes == L - 1, trans[2] * right_col, 0.0) + jnp.where(lanes == 0, trans[3] * left_col, 0.0)


def one_step(pressure, vector, edges, col_right, col_left, diag, inverse, couple, trans, boost, z_out, around_rows):
    p = pressure[0][0:R]
    up_row, down_row = (pressure[0][R : R + 1], pressure[0][EX - 1 : EX])
    far = pressure[1][0:R]
    right_p, left_p = (lane_roll(far, L - 1), lane_roll(far, 1))
    second = []
    for c in range(NC):
        own = diag[c, 0] * p
        if c == 0:
            own = own + boost * p
        around = neighbour_sum(
            couple[c, 0] * p,
            trans,
            around_rows.at[c],
            edges[pl.ds(c, 1), :] * up_row,
            edges[pl.ds(NC + c, 1), :] * down_row,
            ghost_column(col_right, 64, L - 1, c) * right_p,
            ghost_column(col_left, 64, 0, c) * left_p,
        )
        second.append(vector[c] - (own - around))
    rest = []
    for c in range(NC):
        total = inverse[c, 0] * second[0]
        for k in range(1, NC):
            total = total + inverse[c, k] * second[k]
        rest.append(total)
        z_out[c] = total + p if c == 0 else total
    products = []
    for c in range(NC):
        product = couple[c, 0] * rest[0]
        for k in range(1, NC):
            product = product + couple[c, k] * rest[k]
        products.append(product)
    return products


def first_step_kernel(
    par, got1, got2, ext, ext_cols, edges, rhs, trans, weights, wells, diag, inverse, couple, rows_up, rows_down,
    msg1, msg2, z_out, partial, product, level0, level1, level2, cols_right, cols_left, pressure_part, product_cols,
    guard0, guard1, guard2, temp0, temp1, around_rows,
):
    rows, lanes = iotas((EX, L))
    right, left = take(par, 1, got1, got2, pl.ds(EX, EX))
    cols_right[...] = right
    cols_left[...] = left
    packed = ext_cols[...]
    north_own = -lane_sum(lane_roll(packed, 64 - 3 * NC) * right, 64)
    south_right = -lane_sum(lane_roll(packed, 64 - NC) * right, 64 + NC)
    south_own = -lane_sum(lane_roll(packed, 64 - NC) * left, 64)
    north_left = -lane_sum(lane_roll(packed, 64 + NC) * left, 64 + NC)
    right_four, left_four = take(par, 1, got1, got2, pl.ds(0, EX))
    source = None
    for k in range(6):
        from_right = lane_roll(right_four if k < 4 else right, -HALO * (k % 4))
        from_left = lane_roll(left_four if k < 4 else left, L - HALO - HALO * (k % 4))
        near = ext[k]
        far = jnp.where(lanes < HALO, from_right, jnp.where(lanes >= L - HALO, from_left, 0.0))
        if k == CENTER:
            far = jnp.where(far == 0.0, 1.0, far)
        if k == NORTH:
            near = jnp.where(lanes == L - 1, north_own, near)
            far = jnp.where(lanes == L - 1, north_left, far)
        if k == SOUTH:
            near = jnp.where(lanes == 0, south_own, near)
            far = jnp.where(lanes == 0, south_right, far)
        if k == 5:
            source = [near, far]
        else:
            level0[k, 0] = near
            level0[k, 1] = far
        if k == CENTER:
            level0[SCALE, 0] = RELAX / near
            level0[SCALE, 1] = RELAX / far
    levels = (level0, level1, level2)
    coarsen_into(level0, level1, temp0, 0)
    coarsen_into(level1, level2, temp1, 1)
    pressure = vcycle(source, levels, (guard0, guard1, guard2), (temp0, temp1))
    boost = WELL_BOOST * wells[...].astype(jnp.float32)
    vector = [rhs[c] for c in range(NC)]
    products = one_step(
        pressure, vector, edges, right[0:R], left[0:R], diag, inverse, couple, trans, boost, z_out,
        around_rows,
    )
    put(par, 0, msg1, msg2, pl.ds(BX_RING, RING_STATIC), rows_up[...], rows_down[...])
    weighed = jnp.zeros((R, L), jnp.float32)
    zero = jnp.zeros((1, L), jnp.float32)
    parts = []
    for c in range(NC):
        product[c] = products[c]
        value = -neighbour_sum(products[c], trans, around_rows.at[c], zero, zero, 0.0, 0.0)
        partial[c] = value
        weighed = weighed + weights[c] * value
        last, first = (slice(R - 1, R), slice(0, 1))
        put(par, 0, msg1, msg2, pl.ds(BX_EDGE + c, 1), products[c][last], products[c][first])
        put(par, 0, msg1, msg2, pl.ds(BX_RING + RING_VECTOR + c, 1), value[last], value[first])
        parts += [(products[c], 0, c), (products[c], L - 1, NC + c)]
    blank = jnp.zeros((16 - NC, L), jnp.float32)
    columns = pack_columns(parts)
    pressure_part[...] = weighed
    product_cols[...] = columns
    for msg in (msg1, msg2):
        msg[pl.ds(0, R), :] = weighed
        msg[pl.ds(BX_EDGE + NC, 16 - NC), :] = blank
        msg[pl.ds(BX_COL, 8), :] = fold(columns, 2 * NC, 8, 4)


def between_kernel(
    par, got1, got2, pressure_part, product_cols, product, edges, trans, weights, partial, pack_left, pack_right,
    msg1, msg2, ext, ext_cols, rows_out, vector_out,
):
    rows, lanes = iotas((EX, L))
    t_up, t_down = (trans[0, R - 1 : R, :], trans[1, 0:1, :])
    own_up, own_down, far_up, far_down = (jnp.zeros((1, L), jnp.float32) for _ in range(4))
    to_right, to_left = ([], [])
    for c in range(NC):
        up, down = take(par, 0, got1, got2, pl.ds(BX_EDGE + c, 1))
        rows_out[pl.ds(c, 1), :] = up
        rows_out[pl.ds(NC + c, 1), :] = down
        own_up = own_up + t_up * weights[c, R - 1 : R, :] * up
        own_down = own_down + t_down * weights[c, 0:1, :] * down
        far_up = far_up + edges[pl.ds(2 * NC + c, 1), :] * product[c, R - 1 : R, :]
        far_down = far_down + edges[pl.ds(3 * NC + c, 1), :] * product[c, 0:1, :]
        value = partial[c] - ghost_rows(trans, up, down)
        vector_out[c] = value
        to_right.append((value, L - 1, RING_VECTOR + c))
        to_left.append((value, 0, RING_VECTOR + c))
    up, down = take(par, 0, got1, got2, pl.ds(0, R))
    field = jnp.concatenate([pressure_part[...], up, down], axis=0)
    edge = jnp.where(rows == R - 1, own_up, 0.0) + jnp.where(rows == 0, own_down, 0.0)
    edge = edge + jnp.where(rows == R, far_up, 0.0) + jnp.where(rows == EX - 1, far_down, 0.0)
    field = field - edge
    ext[...] = field
    up, down = (unfold(v, 2 * NC, 8, 4, R) for v in take(par, 0, got1, got2, pl.ds(BX_COL, 8)))
    packed = jnp.concatenate([product_cols[...], up, down], axis=0)
    ext_cols[...] = packed
    near = lanes < HALO
    put(
        par, 1, msg1, msg2, pl.ds(0, R),
        fold(jnp.where(near, lane_roll(field, HALO), lane_roll(packed, HALO - NC)), HALO + NC, R, 3),
        fold(jnp.where(near, field, lane_roll(packed, HALO)), HALO + NC, R, 3),
    )
    fixed = iotas((R, L))[1] < RING_VECTOR
    put(
        par, 1, msg1, msg2, pl.ds(R, R),
        jnp.where(fixed, pack_right[...], pack_columns(to_right)),
        jnp.where(fixed, pack_left[...], pack_columns(to_left)),
    )


def row_ring(ring, outward, inward, pressure, row, out_row, own_row, edge_cols, product_row, couple_row, corners, old_corners):
    lanes = iotas((1, L))[1]
    near, far = pressure
    p, beyond = (near[row : row + 1], far[row : row + 1])
    p_right, p_left = (beyond[:, 0:1], beyond[:, L - 1 : L])
    p_out, p_own = (near[out_row : out_row + 1], near[own_row : own_row + 1])
    t_out, t_in = (ring(RING_TRANS + outward), ring(RING_TRANS + inward))
    t_right, t_left = (ring(RING_TRANS + 2), ring(RING_TRANS + 3))
    second = []
    for c in range(NC):
        beside = edge_cols(c) * p
        old_right, old_left = (ghost_column(old_corners[0], 64, L - 1, c), ghost_column(old_corners[1], 64, 0, c))
        new_right, new_left = (ghost_column(corners[0], HALO, L - 1, c), ghost_column(corners[1], HALO, 0, c))
        north = jnp.where(lanes == L - 1, old_right * p_right, shifted(beside, 1, 1))
        south = jnp.where(lanes == 0, old_left * p_left, shifted(beside, 1, -1))
        value = ring(RING_VECTOR + c) - t_in * product_row(c)
        value = value - jnp.where(lanes == L - 1, t_right * new_right, 0.0)
        value = value - jnp.where(lanes == 0, t_left * new_left, 0.0)
        second.append(
            value
            - ring(RING_EFF + c) * p
            + t_out * (ring(RING_NEXT + c) * p_out)
            + t_in * (couple_row(c) * p_own)
            + t_right * north
            + t_left * south
        )
    return second


def column_ring(pack, outward, inward, p, p_out, p_own, p_up, p_down, own_couple, own_product, beside_up, beside_down):
    lanes = iotas((R, L))[1]

    def trans(d):
        return pack[:, RING_TRANS + d : RING_TRANS + d + 1]

    second = (
        lane_roll(pack, -RING_VECTOR)
        - trans(inward) * own_product
        - lane_roll(pack, -RING_EFF) * p
        + trans(outward) * (lane_roll(pack, -RING_NEXT) * p_out)
        + trans(inward) * (own_couple * p_own)
        + trans(0) * (beside_up * p_up)
        + trans(1) * (beside_down * p_down)
    )
    spread = jnp.zeros((R, L), jnp.float32)
    for k in range(NC):
        within = jnp.logical_and(lanes >= NC * k, lanes < NC * k + NC)
        spread = jnp.where(within, second[:, k : k + 1], spread)
    terms = pack * spread
    total = terms
    for k in range(1, NC):
        total = total + lane_roll(terms, -NC * k)
    return total


def second_step_kernel(
    par, got1, got2, gotx1, gotx2, ext, ext_cols, rows_in, setup_cols, cols_right, cols_left, edges,
    level0, level1, level2, partial,
    product, rhs, trans, wells, diag, inverse, couple,
    z_out, dots, ring_up, ring_down, guard0, guard1, guard2, temp0, temp1, around_rows,
):
    rows, lanes = iotas((EX, L))
    right, left = (unfold(v, HALO + NC, R, 3, EX) for v in take(par, 1, got1, got2, pl.ds(0, R)))
    packed, tw = (ext_cols[...], setup_cols[...])
    old_right, old_left = (cols_right[...], cols_left[...])
    own_right = lane_sum(lane_roll(tw, HALO - 3 * NC) * right, HALO)
    own_left = lane_sum(lane_roll(tw, HALO - NC) * left, HALO)
    far_right = lane_sum(old_right * lane_roll(packed, 64), 64 + NC)
    far_left = lane_sum(old_left * lane_roll(packed, 64 + NC), 64 + NC)
    near = ext[...] - jnp.where(lanes == L - 1, own_right, 0.0) - jnp.where(lanes == 0, own_left, 0.0)
    far = jnp.where(
        lanes < HALO, right, jnp.where(lanes >= L - HALO, lane_roll(left, L - HALO), 0.0)
    )
    far = far - jnp.where(lanes == 0, far_right, 0.0) - jnp.where(lanes == L - 1, far_left, 0.0)
    pressure = vcycle([near, far], (level0, level1, level2), (guard0, guard1, guard2), (temp0, temp1))
    vector = []
    for c in range(NC):
        columns = ghost_columns(
            trans, ghost_column(right[0:R], HALO, L - 1, c), ghost_column(left[0:R], HALO, 0, c)
        )
        vector.append(partial[c] - columns)
    boost = WELL_BOOST * wells[...].astype(jnp.float32)
    products = one_step(
        pressure, vector, edges, old_right[0:R], old_left[0:R], diag, inverse, couple, trans, boost, z_out,
        around_rows,
    )
    up, down = take(par, 0, gotx1, gotx2, pl.ds(BX_RING, 112))
    ring_up[...] = up
    ring_down[...] = down
    second_up = row_ring(
        lambda i: ring_up[pl.ds(i, 1), :], 0, 1, pressure, R, R + 1, R - 1,
        lambda c: edges[pl.ds(c, 1), :], lambda c: product[c, R - 1 : R, :], lambda c: couple[c, 0, R - 1 : R, :],
        (right[R : R + 1], left[R : R + 1]), (old_right[R : R + 1], old_left[R : R + 1]),
    )
    second_down = row_ring(
        lambda i: ring_down[pl.ds(i, 1), :], 1, 0, pressure, EX - 1, EX - 2, 0,
        lambda c: edges[pl.ds(NC + c, 1), :], lambda c: product[c, 0:1, :], lambda c: couple[c, 0, 0:1, :],
        (right[EX - 1 : EX], left[EX - 1 : EX]), (old_right[EX - 1 : EX], old_left[EX - 1 : EX]),
    )
    product_up = ring_up[pl.ds(0, NC), :] * second_up[0]
    product_down = ring_down[pl.ds(0, NC), :] * second_down[0]
    for k in range(1, NC):
        product_up = product_up + ring_up[pl.ds(NC * k, NC), :] * second_up[k]
        product_down = product_down + ring_down[pl.ds(NC * k, NC), :] * second_down[k]
    pack_right, pack_left = take(par, 1, got1, got2, pl.ds(R, R))
    far_p = pressure[1]
    far_up, far_down = (shifted(far_p, 0, 1)[0:R], shifted(far_p, 0, -1)[0:R])
    far_p, near_p = (far_p[0:R], pressure[0][0:R])
    right_cols = column_ring(
        pack_right, 2, 3, far_p[:, 0:1], far_p[:, 1:2], near_p[:, L - 1 : L], far_up[:, 0:1], far_down[:, 0:1],
        lane_roll(tw[0:R], -2 * NC), lane_roll(packed[0:R], -NC),
        lane_roll(shifted(old_right, 0, 1)[0:R], -64), lane_roll(shifted(old_right, 0, -1)[0:R], -64),
    )
    left_cols = column_ring(
        pack_left, 3, 2, far_p[:, L - 1 : L], far_p[:, L - 2 : L - 1], near_p[:, 0:1], far_up[:, L - 1 : L],
        far_down[:, L - 1 : L], tw[0:R], packed[0:R],
        lane_roll(shifted(old_left, 0, 1)[0:R], -64), lane_roll(shifted(old_left, 0, -1)[0:R], -64),
    )
    sums = [jnp.zeros((R, L), jnp.float32) for _ in range(6)]
    for c in range(NC):
        two = -neighbour_sum(
            products[c], trans, around_rows.at[c], product_up[c : c + 1], product_down[c : c + 1],
            ghost_column(right_cols, 0, L - 1, c), ghost_column(left_cols, 0, 0, c),
        )
        zero, one = (rhs[c], vector[c])
        for k, (a, b) in enumerate(((zero, zero), (zero, one), (one, one), (zero, two), (one, two), (two, two))):
            sums[k] = sums[k] + a * b
    lane = iotas((1, L))[1]
    row = jnp.zeros((1, L), jnp.float32)
    for k, total in enumerate(sums):
        row = jnp.where(lane == k, jnp.sum(total, keepdims=True), row)
    dots[...] = jnp.broadcast_to(row, dots.shape)


def finish_kernel(gathered, z_one, z_two, out, estimate):
    row = jnp.sum(gathered[...], axis=0, keepdims=True)
    lanes = iotas((1, L))[1]
    g00, g01, g11, g02, g12, g22 = (
        jnp.sum(jnp.where(lanes == k, row, 0.0), axis=1, keepdims=True) for k in range(6)
    )
    beta = jnp.sqrt(g00)
    shift = g01 / g00
    h00 = 1.0 + shift
    length2 = g11 - shift * g01
    length = jnp.sqrt(length2)
    h10 = length / beta
    h01 = (g02 - shift * g01) / (beta * length)
    above = (g12 - shift * g02 - shift * (g11 - shift * g01)) / length2
    h11 = 1.0 + above
    h21 = jnp.sqrt((g22 - 2.0 * shift * g12 + shift * shift * g11) / length2 - h01 * h01 - above * above)
    radius0 = jnp.sqrt(h00 * h00 + h10 * h10)
    cos0, sin0 = (h00 / radius0, h10 / radius0)
    r01 = cos0 * h01 + sin0 * h11
    mid = cos0 * h11 - sin0 * h01
    radius1 = jnp.sqrt(mid * mid + h21 * h21)
    cos1, sin1 = (mid / radius1, h21 / radius1)
    rhs0, rhs1 = (cos0 * beta, -sin0 * beta)
    estimate[...] = jnp.abs(sin1 * rhs1)
    y1 = cos1 * rhs1 / radius1
    y0 = (rhs0 - r01 * y1) / radius0
    weight1 = y1 / length
    weight0 = y0 / beta - weight1 * shift
    for c in range(NC):
        out[c] = weight0 * z_one[c] + weight1 * z_two[c]


VMEM = functools.partial(pl.BlockSpec, memory_space=pltpu.VMEM)
HBM = functools.partial(pl.BlockSpec, memory_space=pltpu.HBM)
ANY = functools.partial(pl.BlockSpec, memory_space=pl.ANY)


def shape(*dims):
    return jax.ShapeDtypeStruct(dims, jnp.float32)


def call(kernel, in_specs, outs, scratch=(), cost=20_000_000):
    return pl.pallas_call(
        kernel,
        in_specs=list(in_specs),
        out_specs=[VMEM()] * len(outs),
        out_shape=list(outs),
        scratch_shapes=list(scratch),
        cost_estimate=pl.CostEstimate(flops=cost, bytes_accessed=1_000_000, transcendentals=0),
        compiler_params=pltpu.CompilerParams(vmem_limit_bytes=30 * 1024 * 1024),
    )


def swap(first, second, axis):
    peers = lax.axis_size(axis)
    pairs = [(i, i ^ 1) for i in range(peers) if i ^ 1 < peers]
    others = [(i, ((i + 1) ^ 1) - 1) for i in range(1, peers) if ((i + 1) ^ 1) - 1 < peers]
    return (lax.ppermute(first, axis, others), lax.ppermute(second, axis, pairs))


def on_device(right_side, diag_blocks, couple_blocks, transmissibility, pressure_weights, well_mask):
    par = jnp.stack([1 - (lax.axis_index("gx") & 1), 1 - (lax.axis_index("gy") & 1)]).astype(jnp.int32)
    par = jnp.broadcast_to(par[:, None], (2, L))
    column = pl.BlockSpec((NC, 1, R, L), lambda i: (0, 0, 0, 0))

    def whole(*dims):
        return pl.BlockSpec(dims, lambda i: (0,) * len(dims))

    msg_a1, msg_a2, own, cols = call(
        setup_kernel,
        [VMEM()] + [HBM()] * 6,
        [shape(AX_ROWS, L), shape(AX_ROWS, L), shape(6 * R, L), shape(R, L)],
        [
            pltpu.VMEM((NC, R, L), jnp.float32),
            pltpu.VMEM((NC, 1, R, L), jnp.float32),
            pltpu.VMEM((NC, 1, R, L), jnp.float32),
            pltpu.VMEM((4, R, L), jnp.float32),
            pltpu.VMEM((NC, R, L), jnp.float32),
            pltpu.VMEM((R, L), jnp.int32),
            pltpu.SemaphoreType.DMA((6,)),
        ],
    )(
        par,
        *(
            pltpu.with_memory_space_constraint(x, pltpu.HBM)
            for x in (right_side, diag_blocks, couple_blocks, transmissibility, pressure_weights, well_mask)
        ),
    )

    got_a1, got_a2 = swap(msg_a1, msg_a2, "gx")

    slab = pl.BlockSpec((NC, NC, 8, L), lambda i: (0, 0, i, 0))
    strip = pl.BlockSpec((8, L), lambda i: (i, 0))
    inverse = pl.pallas_call(
        inverse_kernel,
        grid=(R // 8,),
        in_specs=[slab, strip],
        out_specs=slab,
        out_shape=shape(NC, NC, R, L),
        cost_estimate=pl.CostEstimate(flops=20_000_000, bytes_accessed=2_700_000, transcendentals=0),
        compiler_params=pltpu.CompilerParams(vmem_limit_bytes=30 * 1024 * 1024),
    )(diag_blocks, well_mask)
    pack_left, pack_right, rows_up, rows_down = pl.pallas_call(
        ring_kernel,
        grid=(R // 8,),
        in_specs=[slab, slab, slab, pl.BlockSpec((4, 8, L), lambda i: (0, i, 0)), strip],
        out_specs=[strip, strip, whole(RING_STATIC, L), whole(RING_STATIC, L)],
        out_shape=[shape(R, L), shape(R, L), shape(RING_STATIC, L), shape(RING_STATIC, L)],
        cost_estimate=pl.CostEstimate(flops=20_000_000, bytes_accessed=2_700_000, transcendentals=0),
        compiler_params=pltpu.CompilerParams(vmem_limit_bytes=30 * 1024 * 1024),
    )(inverse, diag_blocks, couple_blocks, transmissibility, well_mask)

    msg_y1, msg_y2, ext, ext_cols, edges = pl.pallas_call(
        setup_middle_kernel,
        grid=(1,),
        in_specs=[
            VMEM(), whole(AX_ROWS, L), whole(AX_ROWS, L), whole(6 * R, L), whole(R, L), column,
            whole(4, R, L), whole(NC, R, L), ANY(),
        ],
        out_specs=[whole(AY_ROWS, L), whole(AY_ROWS, L), whole(6, EX, L), whole(EX, L), whole(4 * NC, L)],
        out_shape=[shape(AY_ROWS, L), shape(AY_ROWS, L), shape(6, EX, L), shape(EX, L), shape(4 * NC, L)],
        compiler_params=pltpu.CompilerParams(vmem_limit_bytes=30 * 1024 * 1024),
    )(par, got_a1, got_a2, own, cols, couple_blocks, transmissibility, pressure_weights, inverse)

    got_y1, got_y2 = swap(msg_y1, msg_y2, "gy")

    fields = shape(NC, R, L)
    work = [
        pltpu.VMEM(dims, jnp.float32)
        for dims in (
            (2, EX + 16, L), (2, EX // 2 + 16, L), (2, EX // 4 + 16, L), (2, EX, L), (2, EX // 2, L), (NC, R + 16, L),
        )
    ]
    msg_b1, msg_b2, z_one, partial, product, level0, level1, level2, cols_right, cols_left, pressure_part, product_cols = call(
        first_step_kernel,
        [VMEM()] + [VMEM()] * 14,
        [
            shape(BX_ROWS, L), shape(BX_ROWS, L), fields, fields, fields, shape(6, 2, EX, L),
            shape(6, 2, EX // 2, L), shape(6, 2, EX // 4, L),
            shape(EX, L), shape(EX, L), shape(R, L), shape(R, L),
        ],
        work,
    )(
        par, got_y1, got_y2, ext, ext_cols, edges, right_side, transmissibility, pressure_weights, well_mask,
        diag_blocks, inverse, couple_blocks, rows_up, rows_down,
    )

    got_b1, got_b2 = swap(msg_b1, msg_b2, "gx")
    msg_c1, msg_c2, ext_b, ext_cols_b, rows_b, vector_b = call(
        between_kernel,
        [VMEM()] + [VMEM()] * 11,
        [shape(2 * R, L), shape(2 * R, L), shape(EX, L), shape(EX, L), shape(2 * NC, L), fields],
    )(
        par, got_b1, got_b2, pressure_part, product_cols, product, edges, transmissibility, pressure_weights,
        partial, pack_left, pack_right,
    )
    got_c1, got_c2 = swap(msg_c1, msg_c2, "gy")

    devices = lax.axis_size("gx") * lax.axis_size("gy")
    z_two, local = call(
        second_step_kernel,
        [VMEM()] * 23,
        [fields, shape(devices, L)],
        [pltpu.VMEM((112, L), jnp.float32), pltpu.VMEM((112, L), jnp.float32)] + work,
    )(
        par, got_c1, got_c2, got_b1, got_b2, ext_b, ext_cols_b, rows_b, ext_cols, cols_right, cols_left, edges,
        level0, level1, level2, vector_b, product, right_side, transmissibility, well_mask, diag_blocks, inverse, couple_blocks,
    )
    gathered = lax.all_to_all(local, ("gx", "gy"), 0, 0, tiled=True)
    answer, estimate = call(finish_kernel, [VMEM()] * 3, [fields, shape(1, 1)])(gathered, z_one, z_two)
    return (answer, estimate.reshape(()))


def solution(mesh):
    return jax.shard_map(
        on_device,
        mesh=mesh,
        in_specs=(
            P(None, "gx", "gy"),
            P(None, None, "gx", "gy"),
            P(None, None, "gx", "gy"),
            P(None, "gx", "gy"),
            P(None, "gx", "gy"),
            P("gx", "gy"),
        ),
        out_specs=(P(None, "gx", "gy"), P()),
        check_vma=False,
    )
```

```python
import functools

import jax
import jax.numpy as jnp
from jax import lax
from jax.experimental import pallas as pl
from jax.experimental.pallas import tpu as pltpu
from jax.sharding import PartitionSpec as P

NC = 9
COARSE_SWEEPS = 6
RELAX = 0.8
WELL_BOOST = 8.0

R, L = 32, 128
HALO = 32
EX, EY = 3 * R, 2 * L

AX_EDGE = 6 * R
AX_COL = AX_EDGE + 24
AX_ROWS = AX_COL + 16
AY_ROWS = 2 * EX
BX_EDGE = R
BX_COL = BX_EDGE + 16
BX_RING = BX_COL + 8
BX_ROWS = BX_RING + 112
RING_EFF, RING_NEXT, RING_TRANS, RING_VECTOR, RING_STATIC = 81, 90, 99, 103, 104

CENTER, EAST, WEST, NORTH, SOUTH, SCALE = range(6)


def iotas(shape):
    return (lax.broadcasted_iota(jnp.int32, shape, 0), lax.broadcasted_iota(jnp.int32, shape, 1))


def shifted(values, axis, step):
    return pltpu.roll(values, (-step) % values.shape[axis], axis)


def lane_roll(values, shift):
    shift = shift % values.shape[1]
    return values if shift == 0 else pltpu.roll(values, shift, 1)


def first_is_up(par_ref, which, shape):
    return jnp.broadcast_to(par_ref[which : which + 1, :], shape) == 0


def put(par_ref, which, first, second, rows, up, down):
    mask = first_is_up(par_ref, which, up.shape)
    first[rows, :] = jnp.where(mask, up, down)
    second[rows, :] = jnp.where(mask, down, up)


def take(par_ref, which, first, second, rows):
    one, two = (first[rows, :], second[rows, :])
    mask = first_is_up(par_ref, which, one.shape)
    return (jnp.where(mask, one, two), jnp.where(mask, two, one))


def pack_columns(parts):
    shape = parts[0][0].shape
    lanes = iotas(shape)[1]
    packed = jnp.zeros(shape, jnp.float32)
    for values, lane, target in parts:
        packed = jnp.where(lanes == target, lane_roll(values, target - lane), packed)
    return packed


def fold(values, width, rows, per_group):
    lanes = iotas((rows, L))[1]
    blocks = []
    for start in range(0, values.shape[0], rows * per_group):
        block = values[start : start + rows]
        for g in range(1, per_group):
            first = start + g * rows
            if first < values.shape[0]:
                block = jnp.where(lanes >= g * width, lane_roll(values[first : first + rows], g * width), block)
        blocks.append(block)
    return blocks[0] if len(blocks) == 1 else jnp.concatenate(blocks, axis=0)


def unfold(folded, width, rows, per_group, total):
    parts = []
    for g in range(total // rows):
        block = folded[g // per_group * rows : (g // per_group + 1) * rows]
        parts.append(lane_roll(block, -(g % per_group) * width))
    return jnp.concatenate(parts, axis=0)


def setup_kernel(
    par, rhs_hbm, diag_hbm, couple_hbm, trans_hbm, weights_hbm, wells_hbm, msg1, msg2, own, cols, diag0, couple0,
    rhs, trans, weights, wells, sems,
):
    pairs = (
        (weights_hbm, weights),
        (couple_hbm.at[:, 0:1], couple0),
        (trans_hbm, trans),
        (diag_hbm.at[:, 0:1], diag0),
        (rhs_hbm, rhs),
        (wells_hbm, wells),
    )
    copies = [pltpu.make_async_copy(a, b, sems.at[i]) for i, (a, b) in enumerate(pairs)]
    for copy in copies:
        copy.start()
    for copy in copies[:3]:
        copy.wait()
    rows, lanes = iotas((R, L))
    links = [jnp.zeros((R, L), jnp.float32) for _ in range(4)]
    for c in range(NC):
        w, col = (weights[c], couple0[c, 0])
        for d, (axis, step) in enumerate(((0, 1), (0, -1), (1, 1), (1, -1))):
            links[d] = links[d] + w * shifted(col, axis, step)
    inside = (rows != R - 1, rows != 0, lanes != L - 1, lanes != 0)
    fields = [None] + [jnp.where(inside[d], -trans[d] * links[d], 0.0) for d in range(4)] + [None]
    t_up, t_down = (trans[0, R - 1 : R, :], trans[1, 0:1, :])
    t_right, t_left = (trans[2], trans[3])
    for c in range(NC):
        put(par, 0, msg1, msg2, pl.ds(AX_EDGE + c, 1), couple0[c, 0, R - 1 : R, :], couple0[c, 0, 0:1, :])
        put(par, 0, msg1, msg2, pl.ds(AX_EDGE + NC + c, 1), t_up * weights[c, R - 1 : R, :], t_down * weights[c, 0:1, :])
    blank = jnp.zeros((24 - 2 * NC, L), jnp.float32)
    msg1[pl.ds(AX_EDGE + 2 * NC, 24 - 2 * NC), :] = blank
    msg2[pl.ds(AX_EDGE + 2 * NC, 24 - 2 * NC), :] = blank
    parts = []
    for c in range(NC):
        col, w = (couple0[c, 0], weights[c])
        parts += [(col, 0, c), (t_left * w, 0, NC + c), (col, L - 1, 2 * NC + c), (t_right * w, L - 1, 3 * NC + c)]
    packed = pack_columns(parts)
    cols[...] = packed
    folded = fold(packed, 4 * NC, 8, 3)
    msg1[pl.ds(AX_COL, 16), :] = folded
    msg2[pl.ds(AX_COL, 16), :] = folded
    for copy in copies[3:]:
        copy.wait()
    center = WELL_BOOST * wells[...].astype(jnp.float32) * weights[0]
    pressure = jnp.zeros((R, L), jnp.float32)
    for c in range(NC):
        center = center + weights[c] * diag0[c, 0]
        pressure = pressure + weights[c] * rhs[c]
    fields[0], fields[5] = (center, pressure)
    for k, field in enumerate(fields):
        span = pl.ds(k * R, R)
        own[span, :] = field
        msg1[span, :] = field
        msg2[span, :] = field


def inverse_kernel(diag, wells, out):
    boost = WELL_BOOST * wells[...].astype(jnp.float32)
    a = [[diag[i, j] + boost if i == j else diag[i, j] for j in range(NC)] for i in range(NC)]
    for k in range(NC):
        inv = 1.0 / a[k][k]
        a[k] = [inv if j == k else a[k][j] * inv for j in range(NC)]
        for i in range(NC):
            if i != k:
                factor = a[i][k]
                a[i] = [-factor * inv if j == k else a[i][j] - factor * a[k][j] for j in range(NC)]
    for i in range(NC):
        for j in range(NC):
            out[i, j] = a[i][j]


def ring_kernel(inverse, diag, couple, trans, wells, pack_left, pack_right, rows_up, rows_down):
    boost = WELL_BOOST * wells[...].astype(jnp.float32)
    entries = []
    for k in range(NC):
        for c in range(NC):
            total = couple[c, 0] * inverse[0, k]
            for m in range(1, NC):
                total = total + couple[c, m] * inverse[m, k]
            entries.append((total, 0, NC * k + c))
    for c in range(NC):
        entries.append((diag[c, 0] + boost if c == 0 else diag[c, 0], 0, RING_EFF + c))
        entries.append((couple[c, 0], 1, RING_NEXT + c))
    for d in range(4):
        entries.append((trans[d], 0, RING_TRANS + d))
    pack_left[...] = pack_columns([(v, inward, place) for v, inward, place in entries])
    pack_right[...] = pack_columns([(v, L - 1 - inward, place) for v, inward, place in entries])
    zero = jnp.zeros((1, L), jnp.float32)

    @pl.when(pl.program_id(0) == 0)
    def _():
        rows_down[pl.ds(RING_STATIC - 1, 1), :] = zero
        for v, inward, place in entries:
            rows_down[pl.ds(place, 1), :] = v[inward : inward + 1, :]

    @pl.when(pl.program_id(0) == R // 8 - 1)
    def _():
        rows_up[pl.ds(RING_STATIC - 1, 1), :] = zero
        for v, inward, place in entries:
            rows_up[pl.ds(place, 1), :] = v[7 - inward : 8 - inward, :]


def setup_middle_kernel(par, got1, got2, own, cols, couple0, trans, weights, _, msg1, msg2, ext, ext_cols, edges):
    rows, lanes = iotas((EX, L))

    def dots(span_of):
        total = jnp.zeros((1, L), jnp.float32)
        for c in range(NC):
            total = total + span_of(c)
        return -total

    ups, downs, tw_ups, tw_downs = ([], [], [], [])
    for c in range(NC):
        up, down = take(par, 0, got1, got2, pl.ds(AX_EDGE + c, 1))
        ups.append(up)
        downs.append(down)
        up, down = take(par, 0, got1, got2, pl.ds(AX_EDGE + NC + c, 1))
        tw_ups.append(up)
        tw_downs.append(down)
        edges[pl.ds(c, 1), :] = ups[c]
        edges[pl.ds(NC + c, 1), :] = downs[c]
        edges[pl.ds(2 * NC + c, 1), :] = tw_ups[c]
        edges[pl.ds(3 * NC + c, 1), :] = tw_downs[c]
    t_up, t_down = (trans[0, R - 1 : R, :], trans[1, 0:1, :])
    east_own = dots(lambda c: t_up * weights[c, R - 1 : R, :] * ups[c])
    west_own = dots(lambda c: t_down * weights[c, 0:1, :] * downs[c])
    west_up = dots(lambda c: tw_ups[c] * couple0[c, 0, R - 1 : R, :])
    east_down = dots(lambda c: tw_downs[c] * couple0[c, 0, 0:1, :])
    fields = []
    for k in range(6):
        up, down = take(par, 0, got1, got2, pl.ds(k * R, R))
        field = jnp.concatenate([own[pl.ds(k * R, R), :], up, down], axis=0)
        if k == CENTER:
            field = jnp.where(field == 0.0, 1.0, field)
        if k == EAST:
            field = jnp.where(rows == R - 1, east_own, jnp.where(rows == EX - 1, east_down, field))
        if k == WEST:
            field = jnp.where(rows == 0, west_own, jnp.where(rows == R, west_up, field))
        ext[k] = field
        fields.append(field)
    up, down = (unfold(v, 4 * NC, 8, 3, R) for v in take(par, 0, got1, got2, pl.ds(AX_COL, 16)))
    packed = jnp.concatenate([cols[...], up, down], axis=0)
    ext_cols[...] = packed
    to_right = [lane_roll(f, HALO * (k % 4) + HALO) for k, f in enumerate(fields)]
    to_left = [lane_roll(f, HALO * (k % 4)) for k, f in enumerate(fields)]
    group = lanes // HALO

    def quad(parts):
        result = parts[-1]
        for g in range(len(parts) - 2, -1, -1):
            result = jnp.where(group == g, parts[g], result)
        return result

    put(par, 1, msg1, msg2, pl.ds(0, EX), quad(to_right[:4]), quad(to_left[:4]))
    put(
        par,
        1,
        msg1,
        msg2,
        pl.ds(EX, EX),
        quad(to_right[4:] + [lane_roll(packed, 64 - 2 * NC)]),
        quad(to_left[4:] + [lane_roll(packed, 64)]),
    )


def lane_sum(product, start):
    lanes = iotas(product.shape)[1]
    keep = jnp.logical_and(lanes >= start, lanes < start + NC)
    return jnp.sum(jnp.where(keep, product, 0.0), axis=1, keepdims=True)


def lane_pairs(values, step):
    lanes = iotas(values.shape)[1]
    return values + jnp.where((lanes // step) % 2 == 0, lane_roll(values, -step), lane_roll(values, step))


def even_rows(ref, half):
    return ref.at[half][pl.ds(0, ref.shape[1] // 2, stride=2), :]


def odd_rows(ref, half):
    return ref.at[half][pl.ds(1, ref.shape[1] // 2, stride=2), :]


def restrict(values, temp, step):
    result = []
    for half in range(2):
        temp[half] = values[half]
        result.append(lane_pairs(even_rows(temp, half) + odd_rows(temp, half), step))
    return result


def prolong(values, temp):
    result = []
    for half in range(2):
        count = values[half].shape[0]
        temp.at[half][pl.ds(0, count, stride=2), :] = values[half]
        temp.at[half][pl.ds(1, count, stride=2), :] = values[half]
        result.append(temp[half])
    return result


def coarsen_into(fine, coarse, temp, level):
    step = 2**level
    for half in range(2):
        lane_even = (iotas(fine.shape[2:])[1] // step) % 2 == 0
        center, east, west, north, south = (fine[d, half] for d in range(5))
        temp[half] = center + jnp.where(lane_even, north, south)
        total = even_rows(temp, half) + odd_rows(temp, half)
        temp[half] = east
        total = total + even_rows(temp, half)
        coarse[EAST, half] = lane_pairs(odd_rows(temp, half), step)
        temp[half] = west
        total = total + odd_rows(temp, half)
        coarse[WEST, half] = lane_pairs(even_rows(temp, half), step)
        total = lane_pairs(total, step)
        coarse[CENTER, half] = total
        coarse[SCALE, half] = RELAX / total
        temp[half] = jnp.where(lane_even, 0.0, north)
        coarse[NORTH, half] = lane_pairs(even_rows(temp, half) + odd_rows(temp, half), step)
        temp[half] = jnp.where(lane_even, south, 0.0)
        coarse[SOUTH, half] = lane_pairs(even_rows(temp, half) + odd_rows(temp, half), step)


def level_apply(values, coeffs, guarded, level):
    step = 2**level
    count = values[0].shape[0]
    lanes = iotas(values[0].shape)[1]
    right = [lane_roll(v, -step) for v in values]
    left = [lane_roll(v, step) for v in values]
    result = []
    for half in range(2):
        v = values[half]
        guarded[half, pl.ds(8, count), :] = v
        guarded[half, pl.ds(7, 1), :] = v[count - 1 : count]
        guarded[half, pl.ds(8 + count, 1), :] = v[0:1]
        result.append(
            coeffs[CENTER, half] * v
            + (
                coeffs[EAST, half] * guarded[half, pl.ds(9, count), :]
                + coeffs[WEST, half] * guarded[half, pl.ds(7, count), :]
                + coeffs[NORTH, half] * jnp.where(lanes >= L - step, right[1 - half], right[half])
                + coeffs[SOUTH, half] * jnp.where(lanes < step, left[1 - half], left[half])
            )
        )
    return result


def sweep(values, source, coeffs, guarded, level):
    applied = level_apply(values, coeffs, guarded, level)
    return [v + coeffs[SCALE, h] * (f - a) for h, (v, f, a) in enumerate(zip(values, source, applied))]


def difference(source, applied):
    return [f - a for f, a in zip(source, applied)]


def scaled(source, coeffs):
    return [coeffs[SCALE, h] * f for h, f in enumerate(source)]


def vcycle(source, levels, guards, temps):
    values0 = scaled(source, levels[0])
    source1 = restrict(difference(source, level_apply(values0, levels[0], guards[0], 0)), temps[0], 1)
    values1 = scaled(source1, levels[1])
    source2 = restrict(difference(source1, level_apply(values1, levels[1], guards[1], 1)), temps[1], 2)
    values2 = scaled(source2, levels[2])
    for _ in range(COARSE_SWEEPS - 1):
        values2 = sweep(values2, source2, levels[2], guards[2], 2)
    values1 = [v + e for v, e in zip(values1, prolong(values2, temps[1]))]
    values1 = sweep(values1, source1, levels[1], guards[1], 1)
    values0 = [v + e for v, e in zip(values0, prolong(values1, temps[0]))]
    return sweep(values0, source, levels[0], guards[0], 0)


def ghost_column(packed, start, to_lane, lane):
    return lane_roll(packed, to_lane - (start + lane))


def neighbour_sum(values, trans, guarded, up_row, down_row, right_col, left_col):
    lanes = iotas((R, L))[1]
    guarded[pl.ds(8, R), :] = values
    guarded[pl.ds(7, 1), :] = down_row
    guarded[pl.ds(8 + R, 1), :] = up_row
    north = jnp.where(lanes == L - 1, right_col, shifted(values, 1, 1))
    south = jnp.where(lanes == 0, left_col, shifted(values, 1, -1))
    return trans[0] * guarded[pl.ds(9, R), :] + trans[1] * guarded[pl.ds(7, R), :] + trans[2] * north + trans[3] * south


def ghost_rows(trans, up_row, down_row):
    rows, _ = iotas((R, L))
    return jnp.where(rows == R - 1, trans[0] * up_row, 0.0) + jnp.where(rows == 0, trans[1] * down_row, 0.0)


def ghost_columns(trans, right_col, left_col):
    _, lanes = iotas((R, L))
    return jnp.where(lanes == L - 1, trans[2] * right_col, 0.0) + jnp.where(lanes == 0, trans[3] * left_col, 0.0)


def one_step(pressure, vector, edges, col_right, col_left, diag, inverse, couple, trans, boost, z_out, around_rows):
    p = pressure[0][0:R]
    up_row, down_row = (pressure[0][R : R + 1], pressure[0][EX - 1 : EX])
    far = pressure[1][0:R]
    right_p, left_p = (lane_roll(far, L - 1), lane_roll(far, 1))
    second = []
    for c in range(NC):
        own = diag[c, 0] * p
        if c == 0:
            own = own + boost * p
        around = neighbour_sum(
            couple[c, 0] * p,
            trans,
            around_rows.at[c],
            edges[pl.ds(c, 1), :] * up_row,
            edges[pl.ds(NC + c, 1), :] * down_row,
            ghost_column(col_right, 64, L - 1, c) * right_p,
            ghost_column(col_left, 64, 0, c) * left_p,
        )
        second.append(vector[c] - (own - around))
    rest = []
    for c in range(NC):
        total = inverse[c, 0] * second[0]
        for k in range(1, NC):
            total = total + inverse[c, k] * second[k]
        rest.append(total)
        z_out[c] = total + p if c == 0 else total
    products = []
    for c in range(NC):
        product = couple[c, 0] * rest[0]
        for k in range(1, NC):
            product = product + couple[c, k] * rest[k]
        products.append(product)
    return products


def first_step_kernel(
    par, got1, got2, ext, ext_cols, edges, rhs, trans, weights, wells, diag, inverse, couple, rows_up, rows_down,
    msg1, msg2, z_out, partial, product, level0, level1, level2, cols_right, cols_left, pressure_part, product_cols,
    guard0, guard1, guard2, temp0, temp1, around_rows,
):
    rows, lanes = iotas((EX, L))
    right, left = take(par, 1, got1, got2, pl.ds(EX, EX))
    cols_right[...] = right
    cols_left[...] = left
    packed = ext_cols[...]
    north_own = -lane_sum(lane_roll(packed, 64 - 3 * NC) * right, 64)
    south_right = -lane_sum(lane_roll(packed, 64 - NC) * right, 64 + NC)
    south_own = -lane_sum(lane_roll(packed, 64 - NC) * left, 64)
    north_left = -lane_sum(lane_roll(packed, 64 + NC) * left, 64 + NC)
    right_four, left_four = take(par, 1, got1, got2, pl.ds(0, EX))
    source = None
    for k in range(6):
        from_right = lane_roll(right_four if k < 4 else right, -HALO * (k % 4))
        from_left = lane_roll(left_four if k < 4 else left, L - HALO - HALO * (k % 4))
        near = ext[k]
        far = jnp.where(lanes < HALO, from_right, jnp.where(lanes >= L - HALO, from_left, 0.0))
        if k == CENTER:
            far = jnp.where(far == 0.0, 1.0, far)
        if k == NORTH:
            near = jnp.where(lanes == L - 1, north_own, near)
            far = jnp.where(lanes == L - 1, north_left, far)
        if k == SOUTH:
            near = jnp.where(lanes == 0, south_own, near)
            far = jnp.where(lanes == 0, south_right, far)
        if k == 5:
            source = [near, far]
        else:
            level0[k, 0] = near
            level0[k, 1] = far
        if k == CENTER:
            level0[SCALE, 0] = RELAX / near
            level0[SCALE, 1] = RELAX / far
    levels = (level0, level1, level2)
    coarsen_into(level0, level1, temp0, 0)
    coarsen_into(level1, level2, temp1, 1)
    pressure = vcycle(source, levels, (guard0, guard1, guard2), (temp0, temp1))
    boost = WELL_BOOST * wells[...].astype(jnp.float32)
    vector = [rhs[c] for c in range(NC)]
    products = one_step(
        pressure, vector, edges, right[0:R], left[0:R], diag, inverse, couple, trans, boost, z_out,
        around_rows,
    )
    put(par, 0, msg1, msg2, pl.ds(BX_RING, RING_STATIC), rows_up[...], rows_down[...])
    weighed = jnp.zeros((R, L), jnp.float32)
    zero = jnp.zeros((1, L), jnp.float32)
    parts = []
    for c in range(NC):
        product[c] = products[c]
        value = -neighbour_sum(products[c], trans, around_rows.at[c], zero, zero, 0.0, 0.0)
        partial[c] = value
        weighed = weighed + weights[c] * value
        last, first = (slice(R - 1, R), slice(0, 1))
        put(par, 0, msg1, msg2, pl.ds(BX_EDGE + c, 1), products[c][last], products[c][first])
        put(par, 0, msg1, msg2, pl.ds(BX_RING + RING_VECTOR + c, 1), value[last], value[first])
        parts += [(products[c], 0, c), (products[c], L - 1, NC + c)]
    blank = jnp.zeros((16 - NC, L), jnp.float32)
    columns = pack_columns(parts)
    pressure_part[...] = weighed
    product_cols[...] = columns
    for msg in (msg1, msg2):
        msg[pl.ds(0, R), :] = weighed
        msg[pl.ds(BX_EDGE + NC, 16 - NC), :] = blank
        msg[pl.ds(BX_COL, 8), :] = fold(columns, 2 * NC, 8, 4)


def between_kernel(
    par, got1, got2, pressure_part, product_cols, product, edges, trans, weights, partial, pack_left, pack_right,
    msg1, msg2, ext, ext_cols, rows_out, vector_out,
):
    rows, lanes = iotas((EX, L))
    t_up, t_down = (trans[0, R - 1 : R, :], trans[1, 0:1, :])
    own_up, own_down, far_up, far_down = (jnp.zeros((1, L), jnp.float32) for _ in range(4))
    to_right, to_left = ([], [])
    for c in range(NC):
        up, down = take(par, 0, got1, got2, pl.ds(BX_EDGE + c, 1))
        rows_out[pl.ds(c, 1), :] = up
        rows_out[pl.ds(NC + c, 1), :] = down
        own_up = own_up + t_up * weights[c, R - 1 : R, :] * up
        own_down = own_down + t_down * weights[c, 0:1, :] * down
        far_up = far_up + edges[pl.ds(2 * NC + c, 1), :] * product[c, R - 1 : R, :]
        far_down = far_down + edges[pl.ds(3 * NC + c, 1), :] * product[c, 0:1, :]
        value = partial[c] - ghost_rows(trans, up, down)
        vector_out[c] = value
        to_right.append((value, L - 1, RING_VECTOR + c))
        to_left.append((value, 0, RING_VECTOR + c))
    up, down = take(par, 0, got1, got2, pl.ds(0, R))
    field = jnp.concatenate([pressure_part[...], up, down], axis=0)
    edge = jnp.where(rows == R - 1, own_up, 0.0) + jnp.where(rows == 0, own_down, 0.0)
    edge = edge + jnp.where(rows == R, far_up, 0.0) + jnp.where(rows == EX - 1, far_down, 0.0)
    field = field - edge
    ext[...] = field
    up, down = (unfold(v, 2 * NC, 8, 4, R) for v in take(par, 0, got1, got2, pl.ds(BX_COL, 8)))
    packed = jnp.concatenate([product_cols[...], up, down], axis=0)
    ext_cols[...] = packed
    near = lanes < HALO
    put(
        par, 1, msg1, msg2, pl.ds(0, R),
        fold(jnp.where(near, lane_roll(field, HALO), lane_roll(packed, HALO - NC)), HALO + NC, R, 3),
        fold(jnp.where(near, field, lane_roll(packed, HALO)), HALO + NC, R, 3),
    )
    fixed = iotas((R, L))[1] < RING_VECTOR
    put(
        par, 1, msg1, msg2, pl.ds(R, R),
        jnp.where(fixed, pack_right[...], pack_columns(to_right)),
        jnp.where(fixed, pack_left[...], pack_columns(to_left)),
    )


def row_ring(ring, outward, inward, pressure, row, out_row, own_row, edge_cols, product_row, couple_row, corners, old_corners):
    lanes = iotas((1, L))[1]
    near, far = pressure
    p, beyond = (near[row : row + 1], far[row : row + 1])
    p_right, p_left = (beyond[:, 0:1], beyond[:, L - 1 : L])
    p_out, p_own = (near[out_row : out_row + 1], near[own_row : own_row + 1])
    t_out, t_in = (ring(RING_TRANS + outward), ring(RING_TRANS + inward))
    t_right, t_left = (ring(RING_TRANS + 2), ring(RING_TRANS + 3))
    second = []
    for c in range(NC):
        beside = edge_cols(c) * p
        old_right, old_left = (ghost_column(old_corners[0], 64, L - 1, c), ghost_column(old_corners[1], 64, 0, c))
        new_right, new_left = (ghost_column(corners[0], HALO, L - 1, c), ghost_column(corners[1], HALO, 0, c))
        north = jnp.where(lanes == L - 1, old_right * p_right, shifted(beside, 1, 1))
        south = jnp.where(lanes == 0, old_left * p_left, shifted(beside, 1, -1))
        value = ring(RING_VECTOR + c) - t_in * product_row(c)
        value = value - jnp.where(lanes == L - 1, t_right * new_right, 0.0)
        value = value - jnp.where(lanes == 0, t_left * new_left, 0.0)
        second.append(
            value
            - ring(RING_EFF + c) * p
            + t_out * (ring(RING_NEXT + c) * p_out)
            + t_in * (couple_row(c) * p_own)
            + t_right * north
            + t_left * south
        )
    return second


def column_ring(pack, outward, inward, p, p_out, p_own, p_up, p_down, own_couple, own_product, beside_up, beside_down):
    lanes = iotas((R, L))[1]

    def trans(d):
        return pack[:, RING_TRANS + d : RING_TRANS + d + 1]

    second = (
        lane_roll(pack, -RING_VECTOR)
        - trans(inward) * own_product
        - lane_roll(pack, -RING_EFF) * p
        + trans(outward) * (lane_roll(pack, -RING_NEXT) * p_out)
        + trans(inward) * (own_couple * p_own)
        + trans(0) * (beside_up * p_up)
        + trans(1) * (beside_down * p_down)
    )
    spread = jnp.zeros((R, L), jnp.float32)
    for k in range(NC):
        within = jnp.logical_and(lanes >= NC * k, lanes < NC * k + NC)
        spread = jnp.where(within, second[:, k : k + 1], spread)
    terms = pack * spread
    total = terms
    for k in range(1, NC):
        total = total + lane_roll(terms, -NC * k)
    return total


def second_step_kernel(
    par, got1, got2, gotx1, gotx2, ext, ext_cols, rows_in, setup_cols, cols_right, cols_left, edges,
    level0, level1, level2, partial,
    product, rhs, trans, wells, diag, inverse, couple,
    z_out, dots, ring_up, ring_down, guard0, guard1, guard2, temp0, temp1, around_rows,
):
    rows, lanes = iotas((EX, L))
    right, left = (unfold(v, HALO + NC, R, 3, EX) for v in take(par, 1, got1, got2, pl.ds(0, R)))
    packed, tw = (ext_cols[...], setup_cols[...])
    old_right, old_left = (cols_right[...], cols_left[...])
    own_right = lane_sum(lane_roll(tw, HALO - 3 * NC) * right, HALO)
    own_left = lane_sum(lane_roll(tw, HALO - NC) * left, HALO)
    far_right = lane_sum(old_right * lane_roll(packed, 64), 64 + NC)
    far_left = lane_sum(old_left * lane_roll(packed, 64 + NC), 64 + NC)
    near = ext[...] - jnp.where(lanes == L - 1, own_right, 0.0) - jnp.where(lanes == 0, own_left, 0.0)
    far = jnp.where(
        lanes < HALO, right, jnp.where(lanes >= L - HALO, lane_roll(left, L - HALO), 0.0)
    )
    far = far - jnp.where(lanes == 0, far_right, 0.0) - jnp.where(lanes == L - 1, far_left, 0.0)
    pressure = vcycle([near, far], (level0, level1, level2), (guard0, guard1, guard2), (temp0, temp1))
    vector = []
    for c in range(NC):
        columns = ghost_columns(
            trans, ghost_column(right[0:R], HALO, L - 1, c), ghost_column(left[0:R], HALO, 0, c)
        )
        vector.append(partial[c] - columns)
    boost = WELL_BOOST * wells[...].astype(jnp.float32)
    products = one_step(
        pressure, vector, edges, old_right[0:R], old_left[0:R], diag, inverse, couple, trans, boost, z_out,
        around_rows,
    )
    up, down = take(par, 0, gotx1, gotx2, pl.ds(BX_RING, 112))
    ring_up[...] = up
    ring_down[...] = down
    second_up = row_ring(
        lambda i: ring_up[pl.ds(i, 1), :], 0, 1, pressure, R, R + 1, R - 1,
        lambda c: edges[pl.ds(c, 1), :], lambda c: product[c, R - 1 : R, :], lambda c: couple[c, 0, R - 1 : R, :],
        (right[R : R + 1], left[R : R + 1]), (old_right[R : R + 1], old_left[R : R + 1]),
    )
    second_down = row_ring(
        lambda i: ring_down[pl.ds(i, 1), :], 1, 0, pressure, EX - 1, EX - 2, 0,
        lambda c: edges[pl.ds(NC + c, 1), :], lambda c: product[c, 0:1, :], lambda c: couple[c, 0, 0:1, :],
        (right[EX - 1 : EX], left[EX - 1 : EX]), (old_right[EX - 1 : EX], old_left[EX - 1 : EX]),
    )
    product_up = ring_up[pl.ds(0, NC), :] * second_up[0]
    product_down = ring_down[pl.ds(0, NC), :] * second_down[0]
    for k in range(1, NC):
        product_up = product_up + ring_up[pl.ds(NC * k, NC), :] * second_up[k]
        product_down = product_down + ring_down[pl.ds(NC * k, NC), :] * second_down[k]
    pack_right, pack_left = take(par, 1, got1, got2, pl.ds(R, R))
    far_p = pressure[1]
    far_up, far_down = (shifted(far_p, 0, 1)[0:R], shifted(far_p, 0, -1)[0:R])
    far_p, near_p = (far_p[0:R], pressure[0][0:R])
    right_cols = column_ring(
        pack_right, 2, 3, far_p[:, 0:1], far_p[:, 1:2], near_p[:, L - 1 : L], far_up[:, 0:1], far_down[:, 0:1],
        lane_roll(tw[0:R], -2 * NC), lane_roll(packed[0:R], -NC),
        lane_roll(shifted(old_right, 0, 1)[0:R], -64), lane_roll(shifted(old_right, 0, -1)[0:R], -64),
    )
    left_cols = column_ring(
        pack_left, 3, 2, far_p[:, L - 1 : L], far_p[:, L - 2 : L - 1], near_p[:, 0:1], far_up[:, L - 1 : L],
        far_down[:, L - 1 : L], tw[0:R], packed[0:R],
        lane_roll(shifted(old_left, 0, 1)[0:R], -64), lane_roll(shifted(old_left, 0, -1)[0:R], -64),
    )
    sums = [jnp.zeros((R, L), jnp.float32) for _ in range(6)]
    for c in range(NC):
        two = -neighbour_sum(
            products[c], trans, around_rows.at[c], product_up[c : c + 1], product_down[c : c + 1],
            ghost_column(right_cols, 0, L - 1, c), ghost_column(left_cols, 0, 0, c),
        )
        zero, one = (rhs[c], vector[c])
        for k, (a, b) in enumerate(((zero, zero), (zero, one), (one, one), (zero, two), (one, two), (two, two))):
            sums[k] = sums[k] + a * b
    lane = iotas((1, L))[1]
    row = jnp.zeros((1, L), jnp.float32)
    for k, total in enumerate(sums):
        row = jnp.where(lane == k, jnp.sum(total, keepdims=True), row)
    dots[...] = jnp.broadcast_to(row, dots.shape)


def finish_kernel(gathered, z_one, z_two, out, estimate):
    row = jnp.sum(gathered[...], axis=0, keepdims=True)
    lanes = iotas((1, L))[1]
    g00, g01, g11, g02, g12, g22 = (
        jnp.sum(jnp.where(lanes == k, row, 0.0), axis=1, keepdims=True) for k in range(6)
    )
    beta = jnp.sqrt(g00)
    shift = g01 / g00
    h00 = 1.0 + shift
    length2 = g11 - shift * g01
    length = jnp.sqrt(length2)
    h10 = length / beta
    h01 = (g02 - shift * g01) / (beta * length)
    above = (g12 - shift * g02 - shift * (g11 - shift * g01)) / length2
    h11 = 1.0 + above
    h21 = jnp.sqrt((g22 - 2.0 * shift * g12 + shift * shift * g11) / length2 - h01 * h01 - above * above)
    radius0 = jnp.sqrt(h00 * h00 + h10 * h10)
    cos0, sin0 = (h00 / radius0, h10 / radius0)
    r01 = cos0 * h01 + sin0 * h11
    mid = cos0 * h11 - sin0 * h01
    radius1 = jnp.sqrt(mid * mid + h21 * h21)
    cos1, sin1 = (mid / radius1, h21 / radius1)
    rhs0, rhs1 = (cos0 * beta, -sin0 * beta)
    estimate[...] = jnp.abs(sin1 * rhs1)
    y1 = cos1 * rhs1 / radius1
    y0 = (rhs0 - r01 * y1) / radius0
    weight1 = y1 / length
    weight0 = y0 / beta - weight1 * shift
    for c in range(NC):
        out[c] = weight0 * z_one[c] + weight1 * z_two[c]


VMEM = functools.partial(pl.BlockSpec, memory_space=pltpu.VMEM)
HBM = functools.partial(pl.BlockSpec, memory_space=pltpu.HBM)
ANY = functools.partial(pl.BlockSpec, memory_space=pl.ANY)


def shape(*dims):
    return jax.ShapeDtypeStruct(dims, jnp.float32)


def call(kernel, in_specs, outs, scratch=(), cost=20_000_000):
    return pl.pallas_call(
        kernel,
        in_specs=list(in_specs),
        out_specs=[VMEM()] * len(outs),
        out_shape=list(outs),
        scratch_shapes=list(scratch),
        cost_estimate=pl.CostEstimate(flops=cost, bytes_accessed=1_000_000, transcendentals=0),
        compiler_params=pltpu.CompilerParams(vmem_limit_bytes=30 * 1024 * 1024),
    )


def swap(first, second, axis):
    peers = lax.axis_size(axis)
    pairs = [(i, i ^ 1) for i in range(peers) if i ^ 1 < peers]
    others = [(i, ((i + 1) ^ 1) - 1) for i in range(1, peers) if ((i + 1) ^ 1) - 1 < peers]
    return (lax.ppermute(first, axis, others), lax.ppermute(second, axis, pairs))


def on_device(right_side, diag_blocks, couple_blocks, transmissibility, pressure_weights, well_mask):
    par = jnp.stack([1 - (lax.axis_index("gx") & 1), 1 - (lax.axis_index("gy") & 1)]).astype(jnp.int32)
    par = jnp.broadcast_to(par[:, None], (2, L))

    def whole(*dims):
        return pl.BlockSpec(dims, lambda i: (0,) * len(dims))

    msg_a1, msg_a2, own, cols, diag0, couple0 = call(
        setup_kernel,
        [VMEM()] + [HBM()] * 6,
        [
            shape(AX_ROWS, L), shape(AX_ROWS, L), shape(6 * R, L), shape(R, L), shape(NC, 1, R, L),
            shape(NC, 1, R, L),
        ],
        [
            pltpu.VMEM((NC, R, L), jnp.float32),
            pltpu.VMEM((4, R, L), jnp.float32),
            pltpu.VMEM((NC, R, L), jnp.float32),
            pltpu.VMEM((R, L), jnp.int32),
            pltpu.SemaphoreType.DMA((6,)),
        ],
    )(
        par,
        *(
            pltpu.with_memory_space_constraint(x, pltpu.HBM)
            for x in (right_side, diag_blocks, couple_blocks, transmissibility, pressure_weights, well_mask)
        ),
    )

    got_a1, got_a2 = swap(msg_a1, msg_a2, "gx")

    slab = pl.BlockSpec((NC, NC, 8, L), lambda i: (0, 0, i, 0))
    strip = pl.BlockSpec((8, L), lambda i: (i, 0))
    inverse = pl.pallas_call(
        inverse_kernel,
        grid=(R // 8,),
        in_specs=[slab, strip],
        out_specs=slab,
        out_shape=shape(NC, NC, R, L),
        cost_estimate=pl.CostEstimate(flops=20_000_000, bytes_accessed=2_700_000, transcendentals=0),
        compiler_params=pltpu.CompilerParams(vmem_limit_bytes=30 * 1024 * 1024),
    )(pltpu.with_memory_space_constraint(diag_blocks, pltpu.HBM), well_mask)
    pack_left, pack_right, rows_up, rows_down = pl.pallas_call(
        ring_kernel,
        grid=(R // 8,),
        in_specs=[
            slab, pl.BlockSpec((NC, 1, 8, L), lambda i: (0, 0, i, 0)), slab,
            pl.BlockSpec((4, 8, L), lambda i: (0, i, 0)), strip,
        ],
        out_specs=[strip, strip, whole(RING_STATIC, L), whole(RING_STATIC, L)],
        out_shape=[shape(R, L), shape(R, L), shape(RING_STATIC, L), shape(RING_STATIC, L)],
        cost_estimate=pl.CostEstimate(flops=20_000_000, bytes_accessed=2_700_000, transcendentals=0),
        compiler_params=pltpu.CompilerParams(vmem_limit_bytes=30 * 1024 * 1024),
    )(inverse, diag0, couple_blocks, transmissibility, well_mask)

    msg_y1, msg_y2, ext, ext_cols, edges = pl.pallas_call(
        setup_middle_kernel,
        grid=(1,),
        in_specs=[
            VMEM(), whole(AX_ROWS, L), whole(AX_ROWS, L), whole(6 * R, L), whole(R, L), whole(NC, 1, R, L),
            whole(4, R, L), whole(NC, R, L), ANY(),
        ],
        out_specs=[whole(AY_ROWS, L), whole(AY_ROWS, L), whole(6, EX, L), whole(EX, L), whole(4 * NC, L)],
        out_shape=[shape(AY_ROWS, L), shape(AY_ROWS, L), shape(6, EX, L), shape(EX, L), shape(4 * NC, L)],
        compiler_params=pltpu.CompilerParams(vmem_limit_bytes=30 * 1024 * 1024),
    )(par, got_a1, got_a2, own, cols, couple0, transmissibility, pressure_weights, inverse)

    got_y1, got_y2 = swap(msg_y1, msg_y2, "gy")

    fields = shape(NC, R, L)
    work = [
        pltpu.VMEM(dims, jnp.float32)
        for dims in (
            (2, EX + 16, L), (2, EX // 2 + 16, L), (2, EX // 4 + 16, L), (2, EX, L), (2, EX // 2, L), (NC, R + 16, L),
        )
    ]
    msg_b1, msg_b2, z_one, partial, product, level0, level1, level2, cols_right, cols_left, pressure_part, product_cols = call(
        first_step_kernel,
        [VMEM()] + [VMEM()] * 14,
        [
            shape(BX_ROWS, L), shape(BX_ROWS, L), fields, fields, fields, shape(6, 2, EX, L),
            shape(6, 2, EX // 2, L), shape(6, 2, EX // 4, L),
            shape(EX, L), shape(EX, L), shape(R, L), shape(R, L),
        ],
        work,
    )(
        par, got_y1, got_y2, ext, ext_cols, edges, right_side, transmissibility, pressure_weights, well_mask,
        diag0, inverse, couple_blocks, rows_up, rows_down,
    )

    got_b1, got_b2 = swap(msg_b1, msg_b2, "gx")
    msg_c1, msg_c2, ext_b, ext_cols_b, rows_b, vector_b = call(
        between_kernel,
        [VMEM()] + [VMEM()] * 11,
        [shape(2 * R, L), shape(2 * R, L), shape(EX, L), shape(EX, L), shape(2 * NC, L), fields],
    )(
        par, got_b1, got_b2, pressure_part, product_cols, product, edges, transmissibility, pressure_weights,
        partial, pack_left, pack_right,
    )
    got_c1, got_c2 = swap(msg_c1, msg_c2, "gy")

    devices = lax.axis_size("gx") * lax.axis_size("gy")
    z_two, local = call(
        second_step_kernel,
        [VMEM()] * 23,
        [fields, shape(devices, L)],
        [pltpu.VMEM((112, L), jnp.float32), pltpu.VMEM((112, L), jnp.float32)] + work,
    )(
        par, got_c1, got_c2, got_b1, got_b2, ext_b, ext_cols_b, rows_b, ext_cols, cols_right, cols_left, edges,
        level0, level1, level2, vector_b, product, right_side, transmissibility, well_mask, diag0, inverse, couple_blocks,
    )
    gathered = lax.all_to_all(local, ("gx", "gy"), 0, 0, tiled=True)
    answer, estimate = call(finish_kernel, [VMEM()] * 3, [fields, shape(1, 1)])(gathered, z_one, z_two)
    return (answer, estimate.reshape(()))


def solution(mesh):
    return jax.shard_map(
        on_device,
        mesh=mesh,
        in_specs=(
            P(None, "gx", "gy"),
            P(None, None, "gx", "gy"),
            P(None, None, "gx", "gy"),
            P(None, "gx", "gy"),
            P(None, "gx", "gy"),
            P("gx", "gy"),
        ),
        out_specs=(P(None, "gx", "gy"), P()),
        check_vma=False,
    )
```

```python
import functools

import jax
import jax.numpy as jnp
from jax import lax
from jax.experimental import pallas as pl
from jax.experimental.pallas import tpu as pltpu
from jax.sharding import PartitionSpec as P

NC = 9
COARSE_SWEEPS = 6
RELAX = 0.8
WELL_BOOST = 8.0

R, L = 32, 128
HALO = 32
EX, EY = 3 * R, 2 * L

AX_EDGE = 6 * R
AX_COL = AX_EDGE + 24
AX_ROWS = AX_COL + 16
AY_ROWS = 2 * EX
BX_EDGE = R
BX_COL = BX_EDGE + 16
BX_RING = BX_COL + 8
BX_ROWS = BX_RING + 112
RING_EFF, RING_NEXT, RING_TRANS, RING_VECTOR, RING_STATIC = 81, 90, 99, 103, 104

CENTER, EAST, WEST, NORTH, SOUTH, SCALE = range(6)


def iotas(shape):
    return (lax.broadcasted_iota(jnp.int32, shape, 0), lax.broadcasted_iota(jnp.int32, shape, 1))


def shifted(values, axis, step):
    return pltpu.roll(values, (-step) % values.shape[axis], axis)


def lane_roll(values, shift):
    shift = shift % values.shape[1]
    return values if shift == 0 else pltpu.roll(values, shift, 1)


def first_is_up(par_ref, which, shape):
    return jnp.broadcast_to(par_ref[which : which + 1, :], shape) == 0


def put(par_ref, which, first, second, rows, up, down):
    mask = first_is_up(par_ref, which, up.shape)
    first[rows, :] = jnp.where(mask, up, down)
    second[rows, :] = jnp.where(mask, down, up)


def take(par_ref, which, first, second, rows):
    one, two = (first[rows, :], second[rows, :])
    mask = first_is_up(par_ref, which, one.shape)
    return (jnp.where(mask, one, two), jnp.where(mask, two, one))


def pack_columns(parts):
    shape = parts[0][0].shape
    lanes = iotas(shape)[1]
    packed = jnp.zeros(shape, jnp.float32)
    for values, lane, target in parts:
        packed = jnp.where(lanes == target, lane_roll(values, target - lane), packed)
    return packed


def fold(values, width, rows, per_group):
    lanes = iotas((rows, L))[1]
    blocks = []
    for start in range(0, values.shape[0], rows * per_group):
        block = values[start : start + rows]
        for g in range(1, per_group):
            first = start + g * rows
            if first < values.shape[0]:
                block = jnp.where(lanes >= g * width, lane_roll(values[first : first + rows], g * width), block)
        blocks.append(block)
    return blocks[0] if len(blocks) == 1 else jnp.concatenate(blocks, axis=0)


def unfold(folded, width, rows, per_group, total):
    parts = []
    for g in range(total // rows):
        block = folded[g // per_group * rows : (g // per_group + 1) * rows]
        parts.append(lane_roll(block, -(g % per_group) * width))
    return jnp.concatenate(parts, axis=0)


def setup_kernel(
    par, rhs_hbm, diag_hbm, couple_hbm, trans_hbm, weights_hbm, wells_hbm, msg1, msg2, own, cols,
    rhs, diag0, couple0, trans, weights, wells, sems,
):
    pairs = (
        (weights_hbm, weights),
        (couple_hbm.at[:, 0:1], couple0),
        (trans_hbm, trans),
        (diag_hbm.at[:, 0:1], diag0),
        (rhs_hbm, rhs),
        (wells_hbm, wells),
    )
    copies = [pltpu.make_async_copy(a, b, sems.at[i]) for i, (a, b) in enumerate(pairs)]
    for copy in copies:
        copy.start()
    for copy in copies[:3]:
        copy.wait()
    rows, lanes = iotas((R, L))
    links = [jnp.zeros((R, L), jnp.float32) for _ in range(4)]
    for c in range(NC):
        w, col = (weights[c], couple0[c, 0])
        for d, (axis, step) in enumerate(((0, 1), (0, -1), (1, 1), (1, -1))):
            links[d] = links[d] + w * shifted(col, axis, step)
    inside = (rows != R - 1, rows != 0, lanes != L - 1, lanes != 0)
    fields = [None] + [jnp.where(inside[d], -trans[d] * links[d], 0.0) for d in range(4)] + [None]
    t_up, t_down = (trans[0, R - 1 : R, :], trans[1, 0:1, :])
    t_right, t_left = (trans[2], trans[3])
    for c in range(NC):
        put(par, 0, msg1, msg2, pl.ds(AX_EDGE + c, 1), couple0[c, 0, R - 1 : R, :], couple0[c, 0, 0:1, :])
        put(par, 0, msg1, msg2, pl.ds(AX_EDGE + NC + c, 1), t_up * weights[c, R - 1 : R, :], t_down * weights[c, 0:1, :])
    blank = jnp.zeros((24 - 2 * NC, L), jnp.float32)
    msg1[pl.ds(AX_EDGE + 2 * NC, 24 - 2 * NC), :] = blank
    msg2[pl.ds(AX_EDGE + 2 * NC, 24 - 2 * NC), :] = blank
    parts = []
    for c in range(NC):
        col, w = (couple0[c, 0], weights[c])
        parts += [(col, 0, c), (t_left * w, 0, NC + c), (col, L - 1, 2 * NC + c), (t_right * w, L - 1, 3 * NC + c)]
    packed = pack_columns(parts)
    cols[...] = packed
    folded = fold(packed, 4 * NC, 8, 3)
    msg1[pl.ds(AX_COL, 16), :] = folded
    msg2[pl.ds(AX_COL, 16), :] = folded
    for copy in copies[3:]:
        copy.wait()
    center = WELL_BOOST * wells[...].astype(jnp.float32) * weights[0]
    pressure = jnp.zeros((R, L), jnp.float32)
    for c in range(NC):
        center = center + weights[c] * diag0[c, 0]
        pressure = pressure + weights[c] * rhs[c]
    fields[0], fields[5] = (center, pressure)
    for k, field in enumerate(fields):
        span = pl.ds(k * R, R)
        own[span, :] = field
        msg1[span, :] = field
        msg2[span, :] = field


def inverse_kernel(diag, wells, out):
    boost = WELL_BOOST * wells[...].astype(jnp.float32)
    a = [[diag[i, j] + boost if i == j else diag[i, j] for j in range(NC)] for i in range(NC)]
    for k in range(NC):
        inv = 1.0 / a[k][k]
        a[k] = [inv if j == k else a[k][j] * inv for j in range(NC)]
        for i in range(NC):
            if i != k:
                factor = a[i][k]
                a[i] = [-factor * inv if j == k else a[i][j] - factor * a[k][j] for j in range(NC)]
    for i in range(NC):
        for j in range(NC):
            out[i, j] = a[i][j]


def ring_kernel(inverse, diag, couple, trans, wells, pack_left, pack_right, rows_up, rows_down):
    boost = WELL_BOOST * wells[...].astype(jnp.float32)
    entries = []
    for k in range(NC):
        for c in range(NC):
            total = couple[c, 0] * inverse[0, k]
            for m in range(1, NC):
                total = total + couple[c, m] * inverse[m, k]
            entries.append((total, 0, NC * k + c))
    for c in range(NC):
        entries.append((diag[c, 0] + boost if c == 0 else diag[c, 0], 0, RING_EFF + c))
        entries.append((couple[c, 0], 1, RING_NEXT + c))
    for d in range(4):
        entries.append((trans[d], 0, RING_TRANS + d))
    pack_left[...] = pack_columns([(v, inward, place) for v, inward, place in entries])
    pack_right[...] = pack_columns([(v, L - 1 - inward, place) for v, inward, place in entries])
    zero = jnp.zeros((1, L), jnp.float32)

    @pl.when(pl.program_id(0) == 0)
    def _():
        rows_down[pl.ds(RING_STATIC - 1, 1), :] = zero
        for v, inward, place in entries:
            rows_down[pl.ds(place, 1), :] = v[inward : inward + 1, :]

    @pl.when(pl.program_id(0) == R // 8 - 1)
    def _():
        rows_up[pl.ds(RING_STATIC - 1, 1), :] = zero
        for v, inward, place in entries:
            rows_up[pl.ds(place, 1), :] = v[7 - inward : 8 - inward, :]


def setup_middle_kernel(par, got1, got2, own, cols, couple0, trans, weights, _, msg1, msg2, ext, ext_cols, edges):
    rows, lanes = iotas((EX, L))

    def dots(span_of):
        total = jnp.zeros((1, L), jnp.float32)
        for c in range(NC):
            total = total + span_of(c)
        return -total

    ups, downs, tw_ups, tw_downs = ([], [], [], [])
    for c in range(NC):
        up, down = take(par, 0, got1, got2, pl.ds(AX_EDGE + c, 1))
        ups.append(up)
        downs.append(down)
        up, down = take(par, 0, got1, got2, pl.ds(AX_EDGE + NC + c, 1))
        tw_ups.append(up)
        tw_downs.append(down)
        edges[pl.ds(c, 1), :] = ups[c]
        edges[pl.ds(NC + c, 1), :] = downs[c]
        edges[pl.ds(2 * NC + c, 1), :] = tw_ups[c]
        edges[pl.ds(3 * NC + c, 1), :] = tw_downs[c]
    t_up, t_down = (trans[0, R - 1 : R, :], trans[1, 0:1, :])
    east_own = dots(lambda c: t_up * weights[c, R - 1 : R, :] * ups[c])
    west_own = dots(lambda c: t_down * weights[c, 0:1, :] * downs[c])
    west_up = dots(lambda c: tw_ups[c] * couple0[c, 0, R - 1 : R, :])
    east_down = dots(lambda c: tw_downs[c] * couple0[c, 0, 0:1, :])
    fields = []
    for k in range(6):
        up, down = take(par, 0, got1, got2, pl.ds(k * R, R))
        field = jnp.concatenate([own[pl.ds(k * R, R), :], up, down], axis=0)
        if k == CENTER:
            field = jnp.where(field == 0.0, 1.0, field)
        if k == EAST:
            field = jnp.where(rows == R - 1, east_own, jnp.where(rows == EX - 1, east_down, field))
        if k == WEST:
            field = jnp.where(rows == 0, west_own, jnp.where(rows == R, west_up, field))
        ext[k] = field
        fields.append(field)
    up, down = (unfold(v, 4 * NC, 8, 3, R) for v in take(par, 0, got1, got2, pl.ds(AX_COL, 16)))
    packed = jnp.concatenate([cols[...], up, down], axis=0)
    ext_cols[...] = packed
    to_right = [lane_roll(f, HALO * (k % 4) + HALO) for k, f in enumerate(fields)]
    to_left = [lane_roll(f, HALO * (k % 4)) for k, f in enumerate(fields)]
    group = lanes // HALO

    def quad(parts):
        result = parts[-1]
        for g in range(len(parts) - 2, -1, -1):
            result = jnp.where(group == g, parts[g], result)
        return result

    put(par, 1, msg1, msg2, pl.ds(0, EX), quad(to_right[:4]), quad(to_left[:4]))
    put(
        par,
        1,
        msg1,
        msg2,
        pl.ds(EX, EX),
        quad(to_right[4:] + [lane_roll(packed, 64 - 2 * NC)]),
        quad(to_left[4:] + [lane_roll(packed, 64)]),
    )


def lane_sum(product, start):
    lanes = iotas(product.shape)[1]
    keep = jnp.logical_and(lanes >= start, lanes < start + NC)
    return jnp.sum(jnp.where(keep, product, 0.0), axis=1, keepdims=True)


def lane_pairs(values, step):
    lanes = iotas(values.shape)[1]
    return values + jnp.where((lanes // step) % 2 == 0, lane_roll(values, -step), lane_roll(values, step))


def even_rows(ref, half):
    return ref.at[half][pl.ds(0, ref.shape[1] // 2, stride=2), :]


def odd_rows(ref, half):
    return ref.at[half][pl.ds(1, ref.shape[1] // 2, stride=2), :]


def restrict(values, temp, step):
    result = []
    for half in range(2):
        temp[half] = values[half]
        result.append(lane_pairs(even_rows(temp, half) + odd_rows(temp, half), step))
    return result


def prolong(values, temp):
    result = []
    for half in range(2):
        count = values[half].shape[0]
        temp.at[half][pl.ds(0, count, stride=2), :] = values[half]
        temp.at[half][pl.ds(1, count, stride=2), :] = values[half]
        result.append(temp[half])
    return result


def coarsen_into(fine, coarse, temp, level):
    step = 2**level
    for half in range(2):
        lane_even = (iotas(fine.shape[2:])[1] // step) % 2 == 0
        center, east, west, north, south = (fine[d, half] for d in range(5))
        temp[half] = center + jnp.where(lane_even, north, south)
        total = even_rows(temp, half) + odd_rows(temp, half)
        temp[half] = east
        total = total + even_rows(temp, half)
        coarse[EAST, half] = lane_pairs(odd_rows(temp, half), step)
        temp[half] = west
        total = total + odd_rows(temp, half)
        coarse[WEST, half] = lane_pairs(even_rows(temp, half), step)
        total = lane_pairs(total, step)
        coarse[CENTER, half] = total
        coarse[SCALE, half] = RELAX / total
        temp[half] = jnp.where(lane_even, 0.0, north)
        coarse[NORTH, half] = lane_pairs(even_rows(temp, half) + odd_rows(temp, half), step)
        temp[half] = jnp.where(lane_even, south, 0.0)
        coarse[SOUTH, half] = lane_pairs(even_rows(temp, half) + odd_rows(temp, half), step)


def level_apply(values, coeffs, guarded, level):
    step = 2**level
    count = values[0].shape[0]
    lanes = iotas(values[0].shape)[1]
    right = [lane_roll(v, -step) for v in values]
    left = [lane_roll(v, step) for v in values]
    result = []
    for half in range(2):
        v = values[half]
        guarded[half, pl.ds(8, count), :] = v
        guarded[half, pl.ds(7, 1), :] = v[count - 1 : count]
        guarded[half, pl.ds(8 + count, 1), :] = v[0:1]
        result.append(
            coeffs[CENTER, half] * v
            + (
                coeffs[EAST, half] * guarded[half, pl.ds(9, count), :]
                + coeffs[WEST, half] * guarded[half, pl.ds(7, count), :]
                + coeffs[NORTH, half] * jnp.where(lanes >= L - step, right[1 - half], right[half])
                + coeffs[SOUTH, half] * jnp.where(lanes < step, left[1 - half], left[half])
            )
        )
    return result


def sweep(values, source, coeffs, guarded, level):
    applied = level_apply(values, coeffs, guarded, level)
    return [v + coeffs[SCALE, h] * (f - a) for h, (v, f, a) in enumerate(zip(values, source, applied))]


def difference(source, applied):
    return [f - a for f, a in zip(source, applied)]


def scaled(source, coeffs):
    return [coeffs[SCALE, h] * f for h, f in enumerate(source)]


def vcycle(source, levels, guards, temps):
    values0 = scaled(source, levels[0])
    source1 = restrict(difference(source, level_apply(values0, levels[0], guards[0], 0)), temps[0], 1)
    values1 = scaled(source1, levels[1])
    source2 = restrict(difference(source1, level_apply(values1, levels[1], guards[1], 1)), temps[1], 2)
    values2 = scaled(source2, levels[2])
    for _ in range(COARSE_SWEEPS - 1):
        values2 = sweep(values2, source2, levels[2], guards[2], 2)
    values1 = [v + e for v, e in zip(values1, prolong(values2, temps[1]))]
    values1 = sweep(values1, source1, levels[1], guards[1], 1)
    values0 = [v + e for v, e in zip(values0, prolong(values1, temps[0]))]
    return sweep(values0, source, levels[0], guards[0], 0)


def ghost_column(packed, start, to_lane, lane):
    return lane_roll(packed, to_lane - (start + lane))


def neighbour_sum(values, trans, guarded, up_row, down_row, right_col, left_col):
    lanes = iotas((R, L))[1]
    guarded[pl.ds(8, R), :] = values
    guarded[pl.ds(7, 1), :] = down_row
    guarded[pl.ds(8 + R, 1), :] = up_row
    north = jnp.where(lanes == L - 1, right_col, shifted(values, 1, 1))
    south = jnp.where(lanes == 0, left_col, shifted(values, 1, -1))
    return trans[0] * guarded[pl.ds(9, R), :] + trans[1] * guarded[pl.ds(7, R), :] + trans[2] * north + trans[3] * south


def ghost_rows(trans, up_row, down_row):
    rows, _ = iotas((R, L))
    return jnp.where(rows == R - 1, trans[0] * up_row, 0.0) + jnp.where(rows == 0, trans[1] * down_row, 0.0)


def ghost_columns(trans, right_col, left_col):
    _, lanes = iotas((R, L))
    return jnp.where(lanes == L - 1, trans[2] * right_col, 0.0) + jnp.where(lanes == 0, trans[3] * left_col, 0.0)


def one_step(pressure, vector, edges, col_right, col_left, diag, inverse, couple, trans, boost, z_out, around_rows):
    p = pressure[0][0:R]
    up_row, down_row = (pressure[0][R : R + 1], pressure[0][EX - 1 : EX])
    far = pressure[1][0:R]
    right_p, left_p = (lane_roll(far, L - 1), lane_roll(far, 1))
    second = []
    for c in range(NC):
        own = diag[c, 0] * p
        if c == 0:
            own = own + boost * p
        around = neighbour_sum(
            couple[c, 0] * p,
            trans,
            around_rows.at[c],
            edges[pl.ds(c, 1), :] * up_row,
            edges[pl.ds(NC + c, 1), :] * down_row,
            ghost_column(col_right, 64, L - 1, c) * right_p,
            ghost_column(col_left, 64, 0, c) * left_p,
        )
        second.append(vector[c] - (own - around))
    rest = []
    for c in range(NC):
        total = inverse[c, 0] * second[0]
        for k in range(1, NC):
            total = total + inverse[c, k] * second[k]
        rest.append(total)
        z_out[c] = total + p if c == 0 else total
    products = []
    for c in range(NC):
        product = couple[c, 0] * rest[0]
        for k in range(1, NC):
            product = product + couple[c, k] * rest[k]
        products.append(product)
    return products


def first_step_kernel(
    par, got1, got2, ext, ext_cols, edges, rhs, trans, weights, wells, diag, inverse, couple, rows_up, rows_down,
    msg1, msg2, z_out, partial, product, level0, level1, level2, cols_right, cols_left, pressure_part, product_cols,
    guard0, guard1, guard2, temp0, temp1, around_rows,
):
    rows, lanes = iotas((EX, L))
    right, left = take(par, 1, got1, got2, pl.ds(EX, EX))
    cols_right[...] = right
    cols_left[...] = left
    packed = ext_cols[...]
    north_own = -lane_sum(lane_roll(packed, 64 - 3 * NC) * right, 64)
    south_right = -lane_sum(lane_roll(packed, 64 - NC) * right, 64 + NC)
    south_own = -lane_sum(lane_roll(packed, 64 - NC) * left, 64)
    north_left = -lane_sum(lane_roll(packed, 64 + NC) * left, 64 + NC)
    right_four, left_four = take(par, 1, got1, got2, pl.ds(0, EX))
    source = None
    for k in range(6):
        from_right = lane_roll(right_four if k < 4 else right, -HALO * (k % 4))
        from_left = lane_roll(left_four if k < 4 else left, L - HALO - HALO * (k % 4))
        near = ext[k]
        far = jnp.where(lanes < HALO, from_right, jnp.where(lanes >= L - HALO, from_left, 0.0))
        if k == CENTER:
            far = jnp.where(far == 0.0, 1.0, far)
        if k == NORTH:
            near = jnp.where(lanes == L - 1, north_own, near)
            far = jnp.where(lanes == L - 1, north_left, far)
        if k == SOUTH:
            near = jnp.where(lanes == 0, south_own, near)
            far = jnp.where(lanes == 0, south_right, far)
        if k == 5:
            source = [near, far]
        else:
            level0[k, 0] = near
            level0[k, 1] = far
        if k == CENTER:
            level0[SCALE, 0] = RELAX / near
            level0[SCALE, 1] = RELAX / far
    levels = (level0, level1, level2)
    coarsen_into(level0, level1, temp0, 0)
    coarsen_into(level1, level2, temp1, 1)
    pressure = vcycle(source, levels, (guard0, guard1, guard2), (temp0, temp1))
    boost = WELL_BOOST * wells[...].astype(jnp.float32)
    vector = [rhs[c] for c in range(NC)]
    products = one_step(
        pressure, vector, edges, right[0:R], left[0:R], diag, inverse, couple, trans, boost, z_out,
        around_rows,
    )
    put(par, 0, msg1, msg2, pl.ds(BX_RING, RING_STATIC), rows_up[...], rows_down[...])
    weighed = jnp.zeros((R, L), jnp.float32)
    zero = jnp.zeros((1, L), jnp.float32)
    parts = []
    for c in range(NC):
        product[c] = products[c]
        value = -neighbour_sum(products[c], trans, around_rows.at[c], zero, zero, 0.0, 0.0)
        partial[c] = value
        weighed = weighed + weights[c] * value
        last, first = (slice(R - 1, R), slice(0, 1))
        put(par, 0, msg1, msg2, pl.ds(BX_EDGE + c, 1), products[c][last], products[c][first])
        put(par, 0, msg1, msg2, pl.ds(BX_RING + RING_VECTOR + c, 1), value[last], value[first])
        parts += [(products[c], 0, c), (products[c], L - 1, NC + c)]
    blank = jnp.zeros((16 - NC, L), jnp.float32)
    columns = pack_columns(parts)
    pressure_part[...] = weighed
    product_cols[...] = columns
    for msg in (msg1, msg2):
        msg[pl.ds(0, R), :] = weighed
        msg[pl.ds(BX_EDGE + NC, 16 - NC), :] = blank
        msg[pl.ds(BX_COL, 8), :] = fold(columns, 2 * NC, 8, 4)


def between_kernel(
    par, got1, got2, pressure_part, product_cols, product, edges, trans, weights, partial, pack_left, pack_right,
    msg1, msg2, ext, ext_cols, rows_out, vector_out,
):
    rows, lanes = iotas((EX, L))
    t_up, t_down = (trans[0, R - 1 : R, :], trans[1, 0:1, :])
    own_up, own_down, far_up, far_down = (jnp.zeros((1, L), jnp.float32) for _ in range(4))
    to_right, to_left = ([], [])
    for c in range(NC):
        up, down = take(par, 0, got1, got2, pl.ds(BX_EDGE + c, 1))
        rows_out[pl.ds(c, 1), :] = up
        rows_out[pl.ds(NC + c, 1), :] = down
        own_up = own_up + t_up * weights[c, R - 1 : R, :] * up
        own_down = own_down + t_down * weights[c, 0:1, :] * down
        far_up = far_up + edges[pl.ds(2 * NC + c, 1), :] * product[c, R - 1 : R, :]
        far_down = far_down + edges[pl.ds(3 * NC + c, 1), :] * product[c, 0:1, :]
        value = partial[c] - ghost_rows(trans, up, down)
        vector_out[c] = value
        to_right.append((value, L - 1, RING_VECTOR + c))
        to_left.append((value, 0, RING_VECTOR + c))
    up, down = take(par, 0, got1, got2, pl.ds(0, R))
    field = jnp.concatenate([pressure_part[...], up, down], axis=0)
    edge = jnp.where(rows == R - 1, own_up, 0.0) + jnp.where(rows == 0, own_down, 0.0)
    edge = edge + jnp.where(rows == R, far_up, 0.0) + jnp.where(rows == EX - 1, far_down, 0.0)
    field = field - edge
    ext[...] = field
    up, down = (unfold(v, 2 * NC, 8, 4, R) for v in take(par, 0, got1, got2, pl.ds(BX_COL, 8)))
    packed = jnp.concatenate([product_cols[...], up, down], axis=0)
    ext_cols[...] = packed
    near = lanes < HALO
    put(
        par, 1, msg1, msg2, pl.ds(0, R),
        fold(jnp.where(near, lane_roll(field, HALO), lane_roll(packed, HALO - NC)), HALO + NC, R, 3),
        fold(jnp.where(near, field, lane_roll(packed, HALO)), HALO + NC, R, 3),
    )
    fixed = iotas((R, L))[1] < RING_VECTOR
    put(
        par, 1, msg1, msg2, pl.ds(R, R),
        jnp.where(fixed, pack_right[...], pack_columns(to_right)),
        jnp.where(fixed, pack_left[...], pack_columns(to_left)),
    )


def row_ring(ring, outward, inward, pressure, row, out_row, own_row, edge_cols, product_row, couple_row, corners, old_corners):
    lanes = iotas((1, L))[1]
    near, far = pressure
    p, beyond = (near[row : row + 1], far[row : row + 1])
    p_right, p_left = (beyond[:, 0:1], beyond[:, L - 1 : L])
    p_out, p_own = (near[out_row : out_row + 1], near[own_row : own_row + 1])
    t_out, t_in = (ring(RING_TRANS + outward), ring(RING_TRANS + inward))
    t_right, t_left = (ring(RING_TRANS + 2), ring(RING_TRANS + 3))
    second = []
    for c in range(NC):
        beside = edge_cols(c) * p
        old_right, old_left = (ghost_column(old_corners[0], 64, L - 1, c), ghost_column(old_corners[1], 64, 0, c))
        new_right, new_left = (ghost_column(corners[0], HALO, L - 1, c), ghost_column(corners[1], HALO, 0, c))
        north = jnp.where(lanes == L - 1, old_right * p_right, shifted(beside, 1, 1))
        south = jnp.where(lanes == 0, old_left * p_left, shifted(beside, 1, -1))
        value = ring(RING_VECTOR + c) - t_in * product_row(c)
        value = value - jnp.where(lanes == L - 1, t_right * new_right, 0.0)
        value = value - jnp.where(lanes == 0, t_left * new_left, 0.0)
        second.append(
            value
            - ring(RING_EFF + c) * p
            + t_out * (ring(RING_NEXT + c) * p_out)
            + t_in * (couple_row(c) * p_own)
            + t_right * north
            + t_left * south
        )
    return second


def column_ring(pack, outward, inward, p, p_out, p_own, p_up, p_down, own_couple, own_product, beside_up, beside_down):
    lanes = iotas((R, L))[1]

    def trans(d):
        return pack[:, RING_TRANS + d : RING_TRANS + d + 1]

    second = (
        lane_roll(pack, -RING_VECTOR)
        - trans(inward) * own_product
        - lane_roll(pack, -RING_EFF) * p
        + trans(outward) * (lane_roll(pack, -RING_NEXT) * p_out)
        + trans(inward) * (own_couple * p_own)
        + trans(0) * (beside_up * p_up)
        + trans(1) * (beside_down * p_down)
    )
    spread = jnp.zeros((R, L), jnp.float32)
    for k in range(NC):
        within = jnp.logical_and(lanes >= NC * k, lanes < NC * k + NC)
        spread = jnp.where(within, second[:, k : k + 1], spread)
    terms = pack * spread
    total = terms
    for k in range(1, NC):
        total = total + lane_roll(terms, -NC * k)
    return total


def second_step_kernel(
    par, got1, got2, gotx1, gotx2, ext, ext_cols, rows_in, setup_cols, cols_right, cols_left, edges,
    level0, level1, level2, partial,
    product, rhs, trans, wells, diag, inverse, couple,
    z_out, dots, ring_up, ring_down, guard0, guard1, guard2, temp0, temp1, around_rows,
):
    rows, lanes = iotas((EX, L))
    right, left = (unfold(v, HALO + NC, R, 3, EX) for v in take(par, 1, got1, got2, pl.ds(0, R)))
    packed, tw = (ext_cols[...], setup_cols[...])
    old_right, old_left = (cols_right[...], cols_left[...])
    own_right = lane_sum(lane_roll(tw, HALO - 3 * NC) * right, HALO)
    own_left = lane_sum(lane_roll(tw, HALO - NC) * left, HALO)
    far_right = lane_sum(old_right * lane_roll(packed, 64), 64 + NC)
    far_left = lane_sum(old_left * lane_roll(packed, 64 + NC), 64 + NC)
    near = ext[...] - jnp.where(lanes == L - 1, own_right, 0.0) - jnp.where(lanes == 0, own_left, 0.0)
    far = jnp.where(
        lanes < HALO, right, jnp.where(lanes >= L - HALO, lane_roll(left, L - HALO), 0.0)
    )
    far = far - jnp.where(lanes == 0, far_right, 0.0) - jnp.where(lanes == L - 1, far_left, 0.0)
    pressure = vcycle([near, far], (level0, level1, level2), (guard0, guard1, guard2), (temp0, temp1))
    vector = []
    for c in range(NC):
        columns = ghost_columns(
            trans, ghost_column(right[0:R], HALO, L - 1, c), ghost_column(left[0:R], HALO, 0, c)
        )
        vector.append(partial[c] - columns)
    boost = WELL_BOOST * wells[...].astype(jnp.float32)
    products = one_step(
        pressure, vector, edges, old_right[0:R], old_left[0:R], diag, inverse, couple, trans, boost, z_out,
        around_rows,
    )
    up, down = take(par, 0, gotx1, gotx2, pl.ds(BX_RING, 112))
    ring_up[...] = up
    ring_down[...] = down
    second_up = row_ring(
        lambda i: ring_up[pl.ds(i, 1), :], 0, 1, pressure, R, R + 1, R - 1,
        lambda c: edges[pl.ds(c, 1), :], lambda c: product[c, R - 1 : R, :], lambda c: couple[c, 0, R - 1 : R, :],
        (right[R : R + 1], left[R : R + 1]), (old_right[R : R + 1], old_left[R : R + 1]),
    )
    second_down = row_ring(
        lambda i: ring_down[pl.ds(i, 1), :], 1, 0, pressure, EX - 1, EX - 2, 0,
        lambda c: edges[pl.ds(NC + c, 1), :], lambda c: product[c, 0:1, :], lambda c: couple[c, 0, 0:1, :],
        (right[EX - 1 : EX], left[EX - 1 : EX]), (old_right[EX - 1 : EX], old_left[EX - 1 : EX]),
    )
    product_up = ring_up[pl.ds(0, NC), :] * second_up[0]
    product_down = ring_down[pl.ds(0, NC), :] * second_down[0]
    for k in range(1, NC):
        product_up = product_up + ring_up[pl.ds(NC * k, NC), :] * second_up[k]
        product_down = product_down + ring_down[pl.ds(NC * k, NC), :] * second_down[k]
    pack_right, pack_left = take(par, 1, got1, got2, pl.ds(R, R))
    far_p = pressure[1]
    far_up, far_down = (shifted(far_p, 0, 1)[0:R], shifted(far_p, 0, -1)[0:R])
    far_p, near_p = (far_p[0:R], pressure[0][0:R])
    right_cols = column_ring(
        pack_right, 2, 3, far_p[:, 0:1], far_p[:, 1:2], near_p[:, L - 1 : L], far_up[:, 0:1], far_down[:, 0:1],
        lane_roll(tw[0:R], -2 * NC), lane_roll(packed[0:R], -NC),
        lane_roll(shifted(old_right, 0, 1)[0:R], -64), lane_roll(shifted(old_right, 0, -1)[0:R], -64),
    )
    left_cols = column_ring(
        pack_left, 3, 2, far_p[:, L - 1 : L], far_p[:, L - 2 : L - 1], near_p[:, 0:1], far_up[:, L - 1 : L],
        far_down[:, L - 1 : L], tw[0:R], packed[0:R],
        lane_roll(shifted(old_left, 0, 1)[0:R], -64), lane_roll(shifted(old_left, 0, -1)[0:R], -64),
    )
    sums = [jnp.zeros((R, L), jnp.float32) for _ in range(6)]
    for c in range(NC):
        two = -neighbour_sum(
            products[c], trans, around_rows.at[c], product_up[c : c + 1], product_down[c : c + 1],
            ghost_column(right_cols, 0, L - 1, c), ghost_column(left_cols, 0, 0, c),
        )
        zero, one = (rhs[c], vector[c])
        for k, (a, b) in enumerate(((zero, zero), (zero, one), (one, one), (zero, two), (one, two), (two, two))):
            sums[k] = sums[k] + a * b
    lane = iotas((1, L))[1]
    row = jnp.zeros((1, L), jnp.float32)
    for k, total in enumerate(sums):
        row = jnp.where(lane == k, jnp.sum(total, keepdims=True), row)
    dots[...] = jnp.broadcast_to(row, dots.shape)


def finish_kernel(gathered, z_one, z_two, out, estimate):
    row = jnp.sum(gathered[...], axis=0, keepdims=True)
    lanes = iotas((1, L))[1]
    g00, g01, g11, g02, g12, g22 = (
        jnp.sum(jnp.where(lanes == k, row, 0.0), axis=1, keepdims=True) for k in range(6)
    )
    beta = jnp.sqrt(g00)
    shift = g01 / g00
    h00 = 1.0 + shift
    length2 = g11 - shift * g01
    length = jnp.sqrt(length2)
    h10 = length / beta
    h01 = (g02 - shift * g01) / (beta * length)
    above = (g12 - shift * g02 - shift * (g11 - shift * g01)) / length2
    h11 = 1.0 + above
    h21 = jnp.sqrt((g22 - 2.0 * shift * g12 + shift * shift * g11) / length2 - h01 * h01 - above * above)
    radius0 = jnp.sqrt(h00 * h00 + h10 * h10)
    cos0, sin0 = (h00 / radius0, h10 / radius0)
    r01 = cos0 * h01 + sin0 * h11
    mid = cos0 * h11 - sin0 * h01
    radius1 = jnp.sqrt(mid * mid + h21 * h21)
    cos1, sin1 = (mid / radius1, h21 / radius1)
    rhs0, rhs1 = (cos0 * beta, -sin0 * beta)
    estimate[...] = jnp.abs(sin1 * rhs1)
    y1 = cos1 * rhs1 / radius1
    y0 = (rhs0 - r01 * y1) / radius0
    weight1 = y1 / length
    weight0 = y0 / beta - weight1 * shift
    for c in range(NC):
        out[c] = weight0 * z_one[c] + weight1 * z_two[c]


VMEM = functools.partial(pl.BlockSpec, memory_space=pltpu.VMEM)
HBM = functools.partial(pl.BlockSpec, memory_space=pltpu.HBM)
ANY = functools.partial(pl.BlockSpec, memory_space=pl.ANY)


def shape(*dims):
    return jax.ShapeDtypeStruct(dims, jnp.float32)


def call(kernel, in_specs, outs, scratch=(), cost=20_000_000):
    return pl.pallas_call(
        kernel,
        in_specs=list(in_specs),
        out_specs=[VMEM()] * len(outs),
        out_shape=list(outs),
        scratch_shapes=list(scratch),
        cost_estimate=pl.CostEstimate(flops=cost, bytes_accessed=1_000_000, transcendentals=0),
        compiler_params=pltpu.CompilerParams(vmem_limit_bytes=30 * 1024 * 1024),
    )


def swap(first, second, axis):
    peers = lax.axis_size(axis)
    pairs = [(i, i ^ 1) for i in range(peers) if i ^ 1 < peers]
    others = [(i, ((i + 1) ^ 1) - 1) for i in range(1, peers) if ((i + 1) ^ 1) - 1 < peers]
    if axis == "gy":
        pairs, others = (others, pairs)
    return (lax.ppermute(first, axis, others), lax.ppermute(second, axis, pairs))


def on_device(right_side, diag_blocks, couple_blocks, transmissibility, pressure_weights, well_mask):
    par = jnp.stack([1 - (lax.axis_index("gx") & 1), lax.axis_index("gy") & 1]).astype(jnp.int32)
    par = jnp.broadcast_to(par[:, None], (2, L))
    column = pl.BlockSpec((NC, 1, R, L), lambda i: (0, 0, 0, 0))

    def whole(*dims):
        return pl.BlockSpec(dims, lambda i: (0,) * len(dims))

    msg_a1, msg_a2, own, cols = call(
        setup_kernel,
        [VMEM()] + [HBM()] * 6,
        [shape(AX_ROWS, L), shape(AX_ROWS, L), shape(6 * R, L), shape(R, L)],
        [
            pltpu.VMEM((NC, R, L), jnp.float32),
            pltpu.VMEM((NC, 1, R, L), jnp.float32),
            pltpu.VMEM((NC, 1, R, L), jnp.float32),
            pltpu.VMEM((4, R, L), jnp.float32),
            pltpu.VMEM((NC, R, L), jnp.float32),
            pltpu.VMEM((R, L), jnp.int32),
            pltpu.SemaphoreType.DMA((6,)),
        ],
    )(
        par,
        *(
            pltpu.with_memory_space_constraint(x, pltpu.HBM)
            for x in (right_side, diag_blocks, couple_blocks, transmissibility, pressure_weights, well_mask)
        ),
    )

    got_a1, got_a2 = swap(msg_a1, msg_a2, "gx")

    slab = pl.BlockSpec((NC, NC, 8, L), lambda i: (0, 0, i, 0))
    strip = pl.BlockSpec((8, L), lambda i: (i, 0))
    inverse = pl.pallas_call(
        inverse_kernel,
        grid=(R // 8,),
        in_specs=[slab, strip],
        out_specs=slab,
        out_shape=shape(NC, NC, R, L),
        cost_estimate=pl.CostEstimate(flops=20_000_000, bytes_accessed=2_700_000, transcendentals=0),
        compiler_params=pltpu.CompilerParams(vmem_limit_bytes=30 * 1024 * 1024),
    )(diag_blocks, well_mask)
    pack_left, pack_right, rows_up, rows_down = pl.pallas_call(
        ring_kernel,
        grid=(R // 8,),
        in_specs=[slab, slab, slab, pl.BlockSpec((4, 8, L), lambda i: (0, i, 0)), strip],
        out_specs=[strip, strip, whole(RING_STATIC, L), whole(RING_STATIC, L)],
        out_shape=[shape(R, L), shape(R, L), shape(RING_STATIC, L), shape(RING_STATIC, L)],
        cost_estimate=pl.CostEstimate(flops=20_000_000, bytes_accessed=2_700_000, transcendentals=0),
        compiler_params=pltpu.CompilerParams(vmem_limit_bytes=30 * 1024 * 1024),
    )(inverse, diag_blocks, couple_blocks, transmissibility, well_mask)

    msg_y1, msg_y2, ext, ext_cols, edges = pl.pallas_call(
        setup_middle_kernel,
        grid=(1,),
        in_specs=[
            VMEM(), whole(AX_ROWS, L), whole(AX_ROWS, L), whole(6 * R, L), whole(R, L), column,
            whole(4, R, L), whole(NC, R, L), ANY(),
        ],
        out_specs=[whole(AY_ROWS, L), whole(AY_ROWS, L), whole(6, EX, L), whole(EX, L), whole(4 * NC, L)],
        out_shape=[shape(AY_ROWS, L), shape(AY_ROWS, L), shape(6, EX, L), shape(EX, L), shape(4 * NC, L)],
        compiler_params=pltpu.CompilerParams(vmem_limit_bytes=30 * 1024 * 1024),
    )(par, got_a1, got_a2, own, cols, couple_blocks, transmissibility, pressure_weights, inverse)

    got_y1, got_y2 = swap(msg_y1, msg_y2, "gy")

    fields = shape(NC, R, L)
    work = [
        pltpu.VMEM(dims, jnp.float32)
        for dims in (
            (2, EX + 16, L), (2, EX // 2 + 16, L), (2, EX // 4 + 16, L), (2, EX, L), (2, EX // 2, L), (NC, R + 16, L),
        )
    ]
    msg_b1, msg_b2, z_one, partial, product, level0, level1, level2, cols_right, cols_left, pressure_part, product_cols = call(
        first_step_kernel,
        [VMEM()] + [VMEM()] * 14,
        [
            shape(BX_ROWS, L), shape(BX_ROWS, L), fields, fields, fields, shape(6, 2, EX, L),
            shape(6, 2, EX // 2, L), shape(6, 2, EX // 4, L),
            shape(EX, L), shape(EX, L), shape(R, L), shape(R, L),
        ],
        work,
    )(
        par, got_y1, got_y2, ext, ext_cols, edges, right_side, transmissibility, pressure_weights, well_mask,
        diag_blocks, inverse, couple_blocks, rows_up, rows_down,
    )

    got_b1, got_b2 = swap(msg_b1, msg_b2, "gx")
    msg_c1, msg_c2, ext_b, ext_cols_b, rows_b, vector_b = call(
        between_kernel,
        [VMEM()] + [VMEM()] * 11,
        [shape(2 * R, L), shape(2 * R, L), shape(EX, L), shape(EX, L), shape(2 * NC, L), fields],
    )(
        par, got_b1, got_b2, pressure_part, product_cols, product, edges, transmissibility, pressure_weights,
        partial, pack_left, pack_right,
    )
    got_c1, got_c2 = swap(msg_c1, msg_c2, "gy")

    devices = lax.axis_size("gx") * lax.axis_size("gy")
    z_two, local = call(
        second_step_kernel,
        [VMEM()] * 23,
        [fields, shape(devices, L)],
        [pltpu.VMEM((112, L), jnp.float32), pltpu.VMEM((112, L), jnp.float32)] + work,
    )(
        par, got_c1, got_c2, got_b1, got_b2, ext_b, ext_cols_b, rows_b, ext_cols, cols_right, cols_left, edges,
        level0, level1, level2, vector_b, product, right_side, transmissibility, well_mask, diag_blocks, inverse, couple_blocks,
    )
    gathered = lax.all_to_all(local, ("gx", "gy"), 0, 0, tiled=True)
    answer, estimate = call(finish_kernel, [VMEM()] * 3, [fields, shape(1, 1)])(gathered, z_one, z_two)
    return (answer, estimate.reshape(()))


def solution(mesh):
    return jax.shard_map(
        on_device,
        mesh=mesh,
        in_specs=(
            P(None, "gx", "gy"),
            P(None, None, "gx", "gy"),
            P(None, None, "gx", "gy"),
            P(None, "gx", "gy"),
            P(None, "gx", "gy"),
            P("gx", "gy"),
        ),
        out_specs=(P(None, "gx", "gy"), P()),
        check_vma=False,
    )
```
